32 devices in a mesh: shard: 4 (over z), context: 2 (over x), tensor: 4 (over y, core).
Axes of the slice: x: 2, y: 2, z: 4, core: 2. Of those that a mesh axis runs over, the one named last changes fastest.
Arguments:
- x_in: bfloat16 [1024, 4, 1152], P(('context', 'tensor'), 'shard'), may hold values from -6 to 6
- cond: float32 [4, 1152], replicated, may hold values from -6 to 6
- w_ada: bfloat16 [2, 1152, 6, 1152], P(None, None, None, 'shard'), may hold values from -0.1875 to 0.1875
- b_ada: bfloat16 [2, 6, 1152], P(None, None, 'shard'), may hold values from -3 to 3
- w_qkv: bfloat16 [2, 3, 1152, 1152], P(None, None, 'shard', 'tensor'), may hold values from -0.1875 to 0.1875
- b_qv: bfloat16 [2, 2, 1152], P(None, None, 'tensor'), may hold values from -3 to 3
- w_proj: bfloat16 [2, 1152, 1152], P(None, 'tensor', 'shard'), may hold values from -1.5 to 1.5
- b_proj: bfloat16 [2, 1152], replicated, may hold values from -2 to 2
- up_weight: bfloat16 [2, 1152, 4608], P(None, 'shard', 'tensor'), may hold values from -0.1875 to 0.1875
- up_bias_vector: bfloat16 [2, 4608], P(None, 'tensor'), may hold values from -3 to 3
- down_weight: bfloat16 [2, 4608, 1152], P(None, 'tensor', 'shard'), may hold values from -0.09375 to 0.09375
- down_bias_vector: bfloat16 [2, 1152], replicated, may hold values from -2 to 2
- cotangent: bfloat16 [1024, 4, 1152], P(('context', 'tensor'), 'shard'), may hold values from -6 to 6
Outputs:
- output: bfloat16 [1024, 4, 1152], P(('context', 'tensor'), 'shard')
- grad_input: float32 [1024, 4, 1152], P(('context', 'tensor'), 'shard')
- grad_cond: float32 [4, 1152], replicated
- grad_w_ada: float32 [2, 1152, 6, 1152], P(None, None, None, 'shard')
- grad_b_ada: float32 [2, 6, 1152], P(None, None, 'shard')
- grad_w_qkv: float32 [2, 3, 1152, 1152], P(None, None, 'shard', 'tensor')
- grad_b_qv: float32 [2, 2, 1152], P(None, None, 'tensor')
- grad_w_proj: float32 [2, 1152, 1152], P(None, 'tensor', 'shard')
- grad_b_proj: float32 [2, 1152], replicated
- grad_w_up: float32 [2, 1152, 4608], P(None, 'shard', 'tensor')
- grad_b_up: float32 [2, 4608], P(None, 'tensor')
- grad_w_down: float32 [2, 4608, 1152], P(None, 'tensor', 'shard')
- grad_b_down: float32 [2, 1152], replicated
The draws below stay inside these ranges and needn't reach their ends.
All inputs are finite; a program needn't handle non-finite values.
Results may differ from the reference program's by a relative error of at most 0.024.
The reference program's roundings to bfloat16 on the way count: a program that leaves them out, or rounds other values in their place, can miss the bound.
Values may be sent and summed in bfloat16 or wider, within the bound.
A program may use at most 192 MiB of HBM per device.

```python
import jax
import jax.numpy as jnp
from jax import lax

D = 1152
H = 16
HD = 72
FF = 4608
LAYERS = 2
SEQS = 4
SEQ_LEN = 1024


def steps_of(key, dims, split, low, largest):
    def one(dim, shards_of):
        heights = jax.random.uniform(jax.random.fold_in(jax.random.fold_in(key, 6), dim), (shards_of,), jnp.float32, low / len(split), largest / len(split))
        return jnp.repeat(jnp.exp(heights), dims[dim] // shards_of).reshape((-1,) + (1,) * (len(dims) - dim - 1))

    loudness = one(*split[0])
    for cut in split[1:]:
        loudness = loudness * one(*cut)
    return loudness


def scatter_about(key, extent, scale, most, shards=(), held_as=jnp.bfloat16):
    array = jax.random.normal(key, extent, jnp.float32) * scale
    if len(shards) > 0:
        array = steps_of(key, extent, shards, -0.22, 0.18) * array
    return jnp.clip(array, min=-most, max=most).astype(held_as)


def setup_inputs(seed: int = 0) -> dict:
    key_of = jax.random.split(jax.random.key(seed), 14)
    x_in = scatter_about(key_of[0], (SEQ_LEN, SEQS, D), 1.0, 6.0, ((0, 8), (1, 4)))
    cond = scatter_about(key_of[1], (SEQS, D), 1.0, 6.0, (), jnp.float32)
    w_ada = scatter_about(key_of[2], (LAYERS, D, 6, D), D ** -0.5, 0.1875, ((3, 4),))
    b_ada = scatter_about(key_of[3], (LAYERS, 6, D), 0.5, 3.0, ((2, 4),))
    w_qkv = scatter_about(key_of[4], (LAYERS, 3, D, D), D ** -0.5, 0.1875, ((2, 4), (3, 4)))
    b_qv = scatter_about(key_of[5], (LAYERS, 2, D), 0.5, 3.0, ((2, 4),))
    w_proj = scatter_about(key_of[6], (LAYERS, D, D), (D // 64) ** -0.5, 1.5, ((1, 4), (2, 4)))
    b_proj = scatter_about(key_of[7], (LAYERS, D), 0.3, 2.0)
    up_weight = scatter_about(key_of[8], (LAYERS, D, FF), D ** -0.5, 0.1875, ((1, 4), (2, 4)))
    up_bias_vector = scatter_about(key_of[9], (LAYERS, FF), 0.5, 3.0, ((1, 4),))
    down_weight = scatter_about(key_of[10], (LAYERS, FF, D), FF ** -0.5, 0.09375, ((1, 4), (2, 4)))
    down_bias_vector = scatter_about(key_of[11], (LAYERS, D), 0.3, 2.0)
    cotangent = scatter_about(key_of[12], (SEQ_LEN, SEQS, D), 1.0, 6.0, ((0, 8), (1, 4)))
    return dict(x_in=x_in, cond=cond, w_ada=w_ada, b_ada=b_ada, w_qkv=w_qkv, b_qv=b_qv, w_proj=w_proj, b_proj=b_proj, up_weight=up_weight, up_bias_vector=up_bias_vector, down_weight=down_weight, down_bias_vector=down_bias_vector, cotangent=cotangent)


epsilon = 1e-06
highest_precision = lax.Precision.HIGHEST

@jax.custom_vjp
def low(v):
    return lax.optimization_barrier(v.astype(jnp.bfloat16)).astype(jnp.float32)

@jax.custom_vjp
def reduced_backward(v):
    return v

def low_keep(v):
    return (low(v), None)

def low_pass(kept, grad):
    return (grad,)

def back_keep(v):
    return (v, None)

def back_low(kept, grad):
    return (low(grad),)
low.defvjp(low_keep, low_pass)
reduced_backward.defvjp(back_keep, back_low)

def layer_norm(values):
    center = values - lax.optimization_barrier(jnp.mean(values, axis=-1, keepdims=True))
    variance = lax.optimization_barrier(jnp.mean(center * center, axis=-1, keepdims=True))
    return center * lax.rsqrt(variance + epsilon)

def head_attention(head_parts):
    queries, keys, values = head_parts
    scores = reduced_backward(jnp.dot(queries, keys.T, precision=highest_precision) * HD ** (-0.5))
    shifted = scores - lax.optimization_barrier(jnp.max(scores, axis=-1, keepdims=True))
    exp_scores = jnp.exp(shifted)
    probs = exp_scores / lax.optimization_barrier(jnp.sum(exp_scores, axis=-1, keepdims=True))
    return jnp.dot(low(probs), values, precision=highest_precision)

def to_heads(tokens):
    return tokens.reshape(tokens.shape[0], H, HD).transpose(1, 0, 2)

def sequence_attention(seq_parts):
    queries, keys, values = seq_parts
    per_head = lax.map(jax.checkpoint(head_attention), (to_heads(queries), to_heads(keys), to_heads(values)))
    return per_head.transpose(1, 0, 2).reshape(queries.shape[0], D)

def diffusion_transformer_layer(hidden_state, condition_reduced, model_parameters):
    w_ada, b_ada, w_qkv, b_qv, w_proj, b_proj, up_weight, up_bias_vector, down_weight, down_bias_vector = model_parameters
    modulation = reduced_backward(low(jnp.einsum('sd,dkc->skc', condition_reduced, w_ada, precision=highest_precision) + b_ada))
    mix_in = low(layer_norm(hidden_state) * (1.0 + modulation[:, 1]) + modulation[:, 0])
    projected = jnp.einsum('lsd,kde->klse', mix_in, w_qkv, precision=highest_precision)
    queries = reduced_backward(low(projected[0] + b_qv[0]))
    keys = reduced_backward(low(projected[1]))
    values = reduced_backward(low(projected[2] + b_qv[1]))
    attended = lax.map(sequence_attention, (jnp.moveaxis(queries, 1, 0), jnp.moveaxis(keys, 1, 0), jnp.moveaxis(values, 1, 0)))
    attended = reduced_backward(low(jnp.moveaxis(attended, 0, 1)))
    branch = reduced_backward(jnp.einsum('lse,ed->lsd', attended, w_proj, precision=highest_precision) + b_proj)
    after_attn = hidden_state + modulation[:, 2] * branch
    feedforward_input = low(layer_norm(after_attn) * (1.0 + modulation[:, 4]) + modulation[:, 3])
    preactivation_value = reduced_backward(jnp.einsum('ect,ty->ecy', feedforward_input, up_weight, precision=highest_precision) + up_bias_vector)
    activation_value = low(jax.nn.gelu(preactivation_value, approximate=True))
    feedforward_output = reduced_backward(jnp.einsum('bcv,vh->bch', activation_value, down_weight, precision=highest_precision) + down_bias_vector)
    return after_attn + modulation[:, 5] * feedforward_output

def reference(x_in, cond, w_ada, b_ada, w_qkv, b_qv, w_proj, b_proj, up_weight, up_bias_vector, down_weight, down_bias_vector, cotangent):
    weights = tuple((member_entry.astype(jnp.float32) for member_entry in (w_ada, b_ada, w_qkv, b_qv, w_proj, b_proj, up_weight, up_bias_vector, down_weight, down_bias_vector)))

    def forward(x_value, cond_value, *layer_parameters):
        condition_reduced = low(jax.nn.silu(cond_value))
        hidden_state = x_value
        for layer_number_index in range(LAYERS):
            hidden_state = diffusion_transformer_layer(hidden_state, condition_reduced, tuple((member_entry[layer_number_index] for member_entry in layer_parameters)))
        return hidden_state
    result, pullback = jax.vjp(forward, x_in.astype(jnp.float32), cond.astype(jnp.float32), *weights)
    grads = pullback(cotangent.astype(jnp.float32))
    return (result.astype(jnp.bfloat16), grads[0], grads[1], grads[2], grads[3], grads[4], grads[5], grads[6], grads[7], grads[8], grads[9], grads[10], grads[11])
```

```python
import functools

import jax
import jax.numpy as jnp
from jax import lax
from jax.experimental import pallas as pl
from jax.experimental.pallas import tpu as pltpu
from jax.sharding import PartitionSpec as P

D = 1152
HD = 72
FF = 4608
LAYERS = 2


epsilon = 1e-06


def normalize(values):
    center = values - jnp.mean(values, axis=-1, keepdims=True)
    inverse = lax.rsqrt(jnp.mean(center * center, axis=-1, keepdims=True) + epsilon)
    return (center * inverse, inverse)


def normalize_back(grad_normed, normed, inverse):
    mean_grad = jnp.mean(grad_normed, axis=-1, keepdims=True)
    mean_proj = jnp.mean(grad_normed * normed, axis=-1, keepdims=True)
    return inverse * (grad_normed - mean_grad - normed * mean_proj)


def gelu_tanh(values):
    return jax.nn.gelu(values, approximate=True)


def to_heads(tokens):
    return tokens.reshape(tokens.shape[0], tokens.shape[1], -1, HD).transpose(1, 2, 0, 3)


def from_heads(blocks):
    return blocks.transpose(2, 0, 1, 3).reshape(blocks.shape[2], blocks.shape[0], -1)


def over_heads(head_fn, arrays):
    return lax.map(lambda seq_items: lax.map(head_fn, seq_items), arrays)


def score_block(query_head, key_head):
    return jnp.einsum(
        "qe,ke->qk", query_head, key_head, preferred_element_type=jnp.float32
    ) * HD ** (-0.5)


def forward_head(head_parts):
    query_head, key_head, value_head = head_parts
    scores = score_block(query_head, key_head)
    maxima = jnp.max(scores, axis=-1, keepdims=True)
    exp_scores = jnp.exp(scores - maxima)
    row_total = jnp.sum(exp_scores, axis=-1, keepdims=True)
    prob_low = (exp_scores / row_total).astype(jnp.bfloat16)
    result = jnp.dot(prob_low, value_head, preferred_element_type=jnp.float32).astype(jnp.bfloat16)
    return (result, (maxima + jnp.log(row_total))[:, 0])


def full_grads(head_parts):
    query_head, key_head, value_head, grad_head, log_head = head_parts
    prob_full = jnp.exp(score_block(query_head, key_head) - log_head[:, None])
    grad_prob = jnp.einsum("qe,ke->qk", grad_head, value_head, preferred_element_type=jnp.float32)
    row_delta = jnp.sum(prob_full * grad_prob, axis=-1, keepdims=True)
    grad_score = (prob_full * (grad_prob - row_delta)).astype(jnp.bfloat16)
    grad_query = jnp.dot(grad_score, key_head, preferred_element_type=jnp.float32) * HD ** (-0.5)
    grad_key = jnp.einsum(
        "qk,qe->ke", grad_score, query_head, preferred_element_type=jnp.float32
    ) * HD ** (-0.5)
    grad_value = jnp.einsum(
        "qk,qe->ke", prob_full.astype(jnp.bfloat16), grad_head, preferred_element_type=jnp.float32
    )
    return (grad_query, grad_key, grad_value)


def fetch_weights(qkv_part, proj_part, up_part, down_part, mod_part):
    return (
        lax.all_gather(qkv_part, "shard", axis=2, tiled=True),
        lax.all_gather(proj_part, "shard", axis=2, tiled=True),
        lax.all_gather(up_part, "shard", axis=1, tiled=True),
        lax.all_gather(down_part, "shard", axis=2, tiled=True),
        lax.all_gather(mod_part, "shard", axis=3, tiled=True),
    )


def layer_forward(hidden_state, weights, modulation, biases):
    full_qkv, full_proj, full_up, full_down, mod_unused = weights
    bias_qv, bias_proj, bias_up, bias_down = biases
    normed1, inverse1 = normalize(hidden_state)
    mix_in = (normed1 * (1.0 + modulation[:, 1]) + modulation[:, 0]).astype(jnp.bfloat16)
    mixed_all = lax.all_gather(mix_in, "tensor", axis=0, tiled=True)
    projected = jnp.einsum("tbd,kde->tbke", mixed_all, full_qkv, preferred_element_type=jnp.float32)
    queries = (projected[:, :, 0] + bias_qv[0]).astype(jnp.bfloat16)
    keys_own = projected[:, :, 1].astype(jnp.bfloat16)
    values_own = (projected[:, :, 2] + bias_qv[1]).astype(jnp.bfloat16)
    keys_all, values_all = (
        lax.all_gather(keys_own, "context", axis=0, tiled=True),
        lax.all_gather(values_own, "context", axis=0, tiled=True),
    )
    head_out, log_sums = over_heads(
        forward_head, (to_heads(queries), to_heads(keys_all), to_heads(values_all))
    )
    attended = from_heads(head_out)
    row_block = attended
    branch = (
        lax.psum_scatter(
            jnp.einsum("tbe,ed->tbd", row_block, full_proj, preferred_element_type=jnp.float32),
            "tensor",
            scatter_dimension=0,
            tiled=True,
        )
        + bias_proj
    )
    after_attn = hidden_state + modulation[:, 2] * branch
    normed2, inverse2 = normalize(after_attn)
    feedforward_input = (normed2 * (1.0 + modulation[:, 4]) + modulation[:, 3]).astype(jnp.bfloat16)
    ff_all = lax.all_gather(feedforward_input, "tensor", axis=0, tiled=True)
    preactivation_value = (
        jnp.einsum("tbd,df->tbf", ff_all, full_up, preferred_element_type=jnp.float32) + bias_up
    )
    activation_value = gelu_tanh(preactivation_value).astype(jnp.bfloat16)
    row_block = activation_value
    feedforward_output = (
        lax.psum_scatter(
            jnp.einsum(
                "tbf,fd->tbd", row_block, full_down, preferred_element_type=jnp.float32
            ).astype(jnp.bfloat16),
            "tensor",
            scatter_dimension=0,
            tiled=True,
        ).astype(jnp.float32)
        + bias_down
    )
    result = after_attn + modulation[:, 5] * feedforward_output
    stash = (
        normed1,
        inverse1,
        mixed_all,
        queries,
        keys_all,
        values_all,
        attended,
        log_sums,
        branch,
        normed2,
        inverse2,
        ff_all,
        preactivation_value,
        activation_value,
        feedforward_output,
    )
    return (result, stash)


def layer_backward(grad_hidden, weights, modulation, stash):
    full_qkv, full_proj, full_up, full_down, mod_unused = weights
    (
        normed1,
        inverse1,
        mixed_all,
        queries,
        keys_all,
        values_all,
        attended,
        log_sums,
        branch,
        normed2,
        inverse2,
        ff_all,
        preactivation_value,
        activation_value,
        feedforward_output,
    ) = stash
    grad_ff = (modulation[:, 5] * grad_hidden).astype(jnp.bfloat16)
    grad_gate2 = jnp.sum(grad_hidden * feedforward_output, axis=0)
    bias_down = jnp.sum(grad_ff.astype(jnp.float32), axis=(0, 1))
    grad_ff_all = lax.all_gather(grad_ff, "tensor", axis=0, tiled=True)
    grad_w_down = jnp.einsum(
        "tbf,tbd->fd", activation_value, grad_ff_all, preferred_element_type=jnp.float32
    )
    grad_activ = jnp.einsum(
        "tbd,fd->tbf", grad_ff_all, full_down, preferred_element_type=jnp.float32
    )
    gelu_value, gelu_back = jax.vjp(gelu_tanh, preactivation_value)
    grad_pre = gelu_back(grad_activ)[0].astype(jnp.bfloat16)
    bias_up = jnp.sum(grad_pre.astype(jnp.float32), axis=(0, 1))
    grad_w_up = jnp.einsum("tbd,tbf->df", ff_all, grad_pre, preferred_element_type=jnp.float32)
    row_block = grad_pre
    grad_ffin = lax.psum_scatter(
        jnp.einsum("tbf,df->tbd", row_block, full_up, preferred_element_type=jnp.float32).astype(
            jnp.bfloat16
        ),
        "tensor",
        scatter_dimension=0,
        tiled=True,
    ).astype(jnp.float32)
    grad_shift2 = jnp.sum(grad_ffin, axis=0)
    grad_scale2 = jnp.sum(grad_ffin * normed2, axis=0)
    grad_after = grad_hidden + normalize_back(
        grad_ffin * (1.0 + modulation[:, 4]), normed2, inverse2
    )
    grad_branch = (modulation[:, 2] * grad_after).astype(jnp.bfloat16)
    grad_gate1 = jnp.sum(grad_after * branch, axis=0)
    bias_proj = jnp.sum(grad_branch.astype(jnp.float32), axis=(0, 1))
    grad_branch_all = lax.all_gather(grad_branch, "tensor", axis=0, tiled=True)
    grad_w_proj = jnp.einsum(
        "tbe,tbd->ed", attended, grad_branch_all, preferred_element_type=jnp.float32
    )
    grad_attended = jnp.einsum(
        "tbd,ed->tbe", grad_branch_all, full_proj, preferred_element_type=jnp.float32
    ).astype(jnp.bfloat16)
    head_inputs = (
        to_heads(queries),
        to_heads(keys_all),
        to_heads(values_all),
        to_heads(grad_attended),
        log_sums,
    )
    grad_q_heads, grad_k_heads, grad_v_heads = over_heads(full_grads, head_inputs)
    grad_queries = from_heads(grad_q_heads).astype(jnp.bfloat16)
    grad_keys, grad_values = (
        lax.psum_scatter(
            from_heads(grad_k_heads).astype(jnp.bfloat16),
            "context",
            scatter_dimension=0,
            tiled=True,
        ).astype(jnp.float32),
        lax.psum_scatter(
            from_heads(grad_v_heads).astype(jnp.bfloat16),
            "context",
            scatter_dimension=0,
            tiled=True,
        ).astype(jnp.float32),
    )
    grad_keys = grad_keys.astype(jnp.bfloat16)
    grad_values = grad_values.astype(jnp.bfloat16)
    grad_qkv = jnp.stack((grad_queries, grad_keys, grad_values), axis=2)
    bias_qv = jnp.stack(
        (
            jnp.sum(grad_queries.astype(jnp.float32), axis=(0, 1)),
            jnp.sum(grad_values.astype(jnp.float32), axis=(0, 1)),
        )
    )
    grad_w_qkv = jnp.einsum(
        "tbd,tbke->kde", mixed_all, grad_qkv, preferred_element_type=jnp.float32
    )
    row_block = grad_qkv
    grad_mixin = lax.psum_scatter(
        jnp.einsum("tbke,kde->tbd", row_block, full_qkv, preferred_element_type=jnp.float32).astype(
            jnp.bfloat16
        ),
        "tensor",
        scatter_dimension=0,
        tiled=True,
    ).astype(jnp.float32)
    grad_shift1 = jnp.sum(grad_mixin, axis=0)
    grad_scale1 = jnp.sum(grad_mixin * normed1, axis=0)
    grad_input = grad_after + normalize_back(
        grad_mixin * (1.0 + modulation[:, 1]), normed1, inverse1
    )
    grad_mod_own = jnp.stack(
        (grad_shift1, grad_scale1, grad_gate1, grad_shift2, grad_scale2, grad_gate2), axis=1
    )
    return (
        grad_input,
        (grad_w_qkv, grad_w_proj, grad_w_up, grad_w_down),
        (grad_mod_own, bias_qv, bias_proj, bias_up, bias_down),
    )


def body(
    x_in,
    cond,
    w_ada,
    b_ada,
    w_qkv,
    b_qv,
    w_proj,
    b_proj,
    up_weight,
    up_bias_vector,
    down_weight,
    down_bias_vector,
    cotangent,
):
    shard_index = lax.axis_index("shard")
    tensor_index = lax.axis_index("tensor")
    context_index = lax.axis_index("context")
    own_latents = x_in.shape[1]
    all_latents = cond.shape[0]
    shard_cols = w_ada.shape[3]
    head_cols = w_qkv.shape[3]
    hidden_cols = up_weight.shape[2]
    condition_reduced = jax.nn.silu(cond).astype(jnp.bfloat16)
    mod_terms = (
        jnp.einsum("sd,ldkc->lskc", condition_reduced, w_ada, preferred_element_type=jnp.float32)
        + b_ada.astype(jnp.float32)[:, None]
    ).astype(jnp.bfloat16)
    hidden_state = x_in.astype(jnp.float32)
    layer_state = []
    for layer_number_index in range(LAYERS):
        sliced = fetch_weights(
            w_qkv[layer_number_index : layer_number_index + 1],
            w_proj[layer_number_index : layer_number_index + 1],
            up_weight[layer_number_index : layer_number_index + 1],
            down_weight[layer_number_index : layer_number_index + 1],
            mod_terms[layer_number_index : layer_number_index + 1],
        )
        weights = tuple((member_entry[0] for member_entry in sliced))
        modulation = lax.dynamic_slice_in_dim(
            weights[4], shard_index * own_latents, own_latents, 0
        ).astype(jnp.float32)
        biases = (
            b_qv[layer_number_index].astype(jnp.float32),
            b_proj[layer_number_index].astype(jnp.float32),
            up_bias_vector[layer_number_index].astype(jnp.float32),
            down_bias_vector[layer_number_index].astype(jnp.float32),
        )
        hidden_state, stash = layer_forward(hidden_state, weights, modulation, biases)
        layer_state.append((weights, modulation, stash))
    output = hidden_state.astype(jnp.bfloat16)
    grad_hidden = cotangent.astype(jnp.float32)
    cond_total = jnp.zeros(cond.shape, jnp.float32)
    results = [None] * LAYERS
    context_mask = (context_index == 0).astype(jnp.float32)
    for layer_number_index in reversed(range(LAYERS)):
        weights, modulation, stash = layer_state[layer_number_index]
        grad_hidden, matrix_grads, small_terms = layer_backward(
            grad_hidden, weights, modulation, stash
        )
        grad_mod_own, bias_qv, bias_proj, bias_up, bias_down = small_terms
        grad_mod_pad = lax.dynamic_update_slice_in_dim(
            jnp.zeros((all_latents, 6, D), jnp.float32), grad_mod_own, shard_index * own_latents, 0
        )
        bias_qv_pad = lax.dynamic_update_slice_in_dim(
            jnp.zeros((2, D), jnp.float32), bias_qv, tensor_index * head_cols, 1
        )
        bias_up_pad = lax.dynamic_update_slice_in_dim(
            jnp.zeros((FF,), jnp.float32), bias_up, tensor_index * hidden_cols, 0
        )
        mod_sum, proj_sum, down_sum, qv_sum, up_sum = lax.psum(
            (grad_mod_pad, bias_proj, bias_down, bias_qv_pad, bias_up_pad),
            ("shard", "context", "tensor"),
        )
        mod_cols = lax.dynamic_slice_in_dim(
            mod_sum.astype(jnp.bfloat16), shard_index * shard_cols, shard_cols, 2
        )
        grad_w_ada = jnp.einsum(
            "sd,skc->dkc", condition_reduced, mod_cols, preferred_element_type=jnp.float32
        )
        grad_b_ada = jnp.sum(mod_cols.astype(jnp.float32), axis=0)
        cond_part = (
            jnp.einsum(
                "skc,dkc->sd",
                mod_cols,
                w_ada[layer_number_index],
                preferred_element_type=jnp.float32,
            )
            * context_mask
        )
        grad_w_qkv, grad_w_proj, grad_w_up, grad_w_down = matrix_grads
        qkv_all, proj_all, up_all, down_all, cond_sum = (
            lax.psum(grad_w_qkv.astype(jnp.bfloat16), ("shard", "context")).astype(jnp.float32),
            lax.psum(grad_w_proj.astype(jnp.bfloat16), ("shard", "context")).astype(jnp.float32),
            lax.psum(grad_w_up.astype(jnp.bfloat16), ("shard", "context")).astype(jnp.float32),
            lax.psum(grad_w_down.astype(jnp.bfloat16), ("shard", "context")).astype(jnp.float32),
            lax.psum(cond_part.astype(jnp.bfloat16), ("shard", "context")).astype(jnp.float32),
        )
        qkv_own = lax.dynamic_slice_in_dim(qkv_all, shard_index * shard_cols, shard_cols, 1)
        proj_own = lax.dynamic_slice_in_dim(proj_all, shard_index * shard_cols, shard_cols, 1)
        up_own = lax.dynamic_slice_in_dim(up_all, shard_index * shard_cols, shard_cols, 0)
        down_own = lax.dynamic_slice_in_dim(down_all, shard_index * shard_cols, shard_cols, 1)
        cond_total = cond_total + cond_sum
        results[layer_number_index] = (
            grad_w_ada,
            grad_b_ada,
            qkv_own,
            lax.dynamic_slice_in_dim(qv_sum, tensor_index * head_cols, head_cols, 1),
            proj_own,
            proj_sum,
            up_own,
            lax.dynamic_slice_in_dim(up_sum, tensor_index * hidden_cols, hidden_cols, 0),
            down_own,
            down_sum,
        )
    silu_value, silu_back = jax.vjp(jax.nn.silu, cond)
    grad_cond = silu_back(cond_total)[0]
    stacked = tuple(
        (
            jnp.stack(
                [results[layer_number_index][member_entry] for layer_number_index in range(LAYERS)]
            )
            for member_entry in range(10)
        )
    )
    return (
        output,
        grad_hidden,
        grad_cond,
        stacked[0],
        stacked[1],
        stacked[2],
        stacked[3],
        stacked[4],
        stacked[5],
        stacked[6],
        stacked[7],
        stacked[8],
        stacked[9],
    )


MESH = pl.DeviceIdType.MESH
F32 = jnp.float32
BF16 = jnp.bfloat16


def nt(a, b):
    return lax.dot_general(a, b, (((1,), (1,)), ((), ())), preferred_element_type=F32)


def nn(a, b):
    return jnp.dot(a, b, preferred_element_type=F32)


def tn(a, b):
    return lax.dot_general(a, b, (((0,), (0,)), ((), ())), preferred_element_type=F32)


def fold(v):
    return jnp.sum(v.reshape(v.shape[0] // 8, 8, v.shape[1]), axis=0)


def rows_at(start, size, multiple=16):
    return pl.ds(pl.multiple_of(start, multiple), size)


def stage_kernel(
    zs_n,
    x_ref,
    cot_ref,
    modin_ref,
    bias_ref,
    s_ref,
    out_ref,
    gin_ref,
    gw_ref,
    small_ref,
    k_mixed,
    k_ff,
    k_pre,
    k_own,
    w,
    mixed,
    qkv,
    qa,
    att,
    ffall,
    pre,
    own,
    inv,
    lse,
    modr,
    modv,
    af,
    pool,
    ra,
    ysend,
    yrecv,
    xsend,
    xrecv,
    dsend,
    drecv,
    gff,
    gpre,
    gb,
    dqkv,
    dkv,
    pb,
    otw,
    ot,
    rx,
    rz,
    sm,
    smr,
    m_s,
    m_r,
    wz_s,
    wz_r,
    wx_s,
    wx_r,
    w_l,
    ap_s,
    ap_r,
    at_s,
    at_r,
    rt_s,
    rt_r,
    rp_s,
    rp_r,
    gx_s,
    gx_r,
    gz_s,
    gz_r,
    gf_s,
    gf_r,
    g_l,
    sm_s,
    sm_r,
    k_s,
):
    z = lax.axis_index("shard")
    c = lax.axis_index("context")
    t = lax.axis_index("tensor")
    y = t // 2
    k = t - 2 * y
    tp = t + 1 - 2 * k
    t_far = t + 2 - 4 * y
    tp_far = tp + 2 - 4 * y
    dev_p = (z, c, tp)
    dev_y = (z, c, t_far)
    dev_x = (z, 1 - c, t)
    zo = [lax.rem(z + d, zs_n) for d in range(1, zs_n)]
    scale = HD ** (-0.5)
    hb = gin_ref

    def rc(src, dst, ss, rs, dev):
        return pltpu.make_async_remote_copy(
            src_ref=src, dst_ref=dst, send_sem=ss, recv_sem=rs, device_id=dev, device_id_type=MESH
        )

    barrier = pltpu.get_barrier_semaphore()
    for dev in [dev_p, dev_y, dev_x] + [(zz, c, t) for zz in zo]:
        pl.semaphore_signal(barrier, inc=1, device_id=dev, device_id_type=MESH)
    pl.semaphore_wait(barrier, 2 + zs_n)

    def mod_copy(d, to, frm):
        return rc(modin_ref.at[to], modr.at[frm], m_s.at[d], m_r.at[frm], (to, c, t))

    for d, zz in enumerate(zo):
        mod_copy(d, zz, z).start()

    half = 144

    def w_rows(zz, cc):
        return rows_at(288 * zz + half * cc, half)

    def w0(i):
        pltpu.make_async_copy(s_ref.at[i], w.at[i, rows_at(288 * z, 288)], w_l.at[i]).start()
        for d, zz in enumerate(zo):
            rc(
                s_ref.at[i, rows_at(half * c, half)],
                w.at[i, w_rows(z, c)],
                wz_s.at[i, d],
                wz_r.at[i, z],
                (zz, c, t),
            ).start()

    def w1(i):
        for d, zz in enumerate(zo):
            part = w.at[i, w_rows(zz, c)]
            rc(part, part, wz_s.at[i, d], wz_r.at[i, zz], dev_x).wait_recv()
            rc(part, part, wx_s.at[i, d], wx_r.at[i, d], dev_x).start()

    def w2(i):
        for d, zz in enumerate(zo):
            part = w.at[i, w_rows(zz, 1 - c)]
            rc(part, part, wx_s.at[i, d], wx_r.at[i, d], dev_x).wait_recv()
        pltpu.make_async_copy(s_ref.at[i], w.at[i, rows_at(288 * z, 288)], w_l.at[i]).wait()

    def w_drain(i):
        for d, zz in enumerate(zo):
            part = w.at[i, w_rows(zz, c)]
            rc(part, part, wz_s.at[i, d], wz_r.at[i, zz], dev_x).wait_send()
            rc(part, part, wx_s.at[i, d], wx_r.at[i, d], dev_x).wait_send()

    for i in range(6):
        w0(i)

    modr[z] = modin_ref[z]
    for zz in zo:
        mod_copy(0, zz, zz).wait_recv()
    for d in range(zs_n - 1):
        mod_copy(d, zo[d], z).wait_send()
    for layer in range(LAYERS):
        for zz in range(zs_n):
            modv[layer, 0:6, 288 * zz : 288 * (zz + 1)] = modr[zz, 8 * layer : 8 * layer + 6, 0:288]

    def mrow(layer, kind):
        return modv[layer, kind : kind + 1, :]

    def ap_copy(layer, index, block, offset, size, dev):
        part = mixed.at[rows_at(128 * block + offset, size)]
        return rc(part, part, ap_s.at[layer, index], ap_r.at[layer, index], dev)

    def ap_parts(layer):
        b_own, b_p = 4 * c + t, 4 * c + tp
        b_y, b_yp = 4 * c + t_far, 4 * c + tp_far
        b_x, b_xp = 4 * (1 - c) + t, 4 * (1 - c) + tp
        b_d, b_dp = 4 * (1 - c) + t_far, 4 * (1 - c) + tp_far
        sends = [
            (0, b_own, 0, 128, dev_p),
            (1, b_own, 0, 64, dev_y),
            (4, b_own, 64, 64, dev_x),
            (2, b_own, 64, 64, dev_y),
            (3, b_own, 0, 64, dev_x),
            (5, b_y, 0, 64, dev_x),
            (6, b_x, 64, 64, dev_y),
            (7, b_y, 0, 64, dev_p),
            (8, b_y, 64, 64, dev_p),
            (9, b_x, 0, 64, dev_p),
            (10, b_x, 64, 64, dev_p),
            (11, b_d, 0, 64, dev_p),
            (12, b_d, 64, 64, dev_p),
        ]
        recvs = {
            0: (b_p, 0, 128),
            1: (b_y, 0, 64),
            2: (b_y, 64, 64),
            3: (b_x, 0, 64),
            4: (b_x, 64, 64),
            5: (b_d, 0, 64),
            6: (b_d, 64, 64),
            7: (b_yp, 0, 64),
            8: (b_yp, 64, 64),
            9: (b_xp, 0, 64),
            10: (b_xp, 64, 64),
            11: (b_dp, 0, 64),
            12: (b_dp, 64, 64),
        }

        def send(index):
            for entry in sends:
                if entry[0] == index:
                    ap_copy(layer, *entry).start()

        def wait(index):
            ap_copy(layer, index, *recvs[index], dev_p).wait_recv()

        def drain():
            for entry in sends:
                ap_copy(layer, *entry).wait_send()

        return send, wait, drain

    def gather_plane(layer, compute):
        send, wait, drain = ap_parts(layer)
        for index in (0, 1, 4, 2, 3):
            send(index)

        def step(i, carry):
            b0, b1, b2 = lax.rem(i, 2), lax.rem(i // 2, 2), i // 4

            @pl.when(i == 1)
            def _():
                wait(0)

            @pl.when(i == 2)
            def _():
                wait(1)
                send(5)
                send(7)
                wait(4)
                send(6)
                send(10)
                wait(2)
                send(8)
                wait(3)
                send(9)

            @pl.when(i == 3)
            def _():
                wait(7)
                wait(8)

            @pl.when(i == 5)
            def _():
                wait(9)
                wait(10)

            @pl.when(i == 6)
            def _():
                wait(5)
                send(11)
                wait(6)
                send(12)

            @pl.when(i == 7)
            def _():
                wait(11)
                wait(12)

            block = (
                4 * lax.rem(c + b2, 2) + 2 * lax.rem(y + b1, 2) + lax.rem(k + b0, 2)
            )
            compute(block)
            return carry

        lax.fori_loop(0, 8, step, 0)
        drain()

    def gather_tensor(buf, phase, layer, compute):
        def copy(index, block, offset, size, dev):
            part = buf.at[rows_at(128 * block + offset, size)]
            return rc(part, part, at_s.at[phase, layer, index], at_r.at[phase, layer, index], dev)

        copy(0, t, 0, 128, dev_p).start()
        copy(1, t, 0, 64, dev_y).start()
        copy(2, t, 64, 64, dev_y).start()

        def step(i, carry):
            b0, b1 = lax.rem(i, 2), i // 2

            @pl.when(i == 1)
            def _():
                copy(0, tp, 0, 128, dev_p).wait_recv()

            @pl.when(i == 2)
            def _():
                copy(1, t_far, 0, 64, dev_y).wait_recv()
                copy(3, t_far, 0, 64, dev_p).start()
                copy(2, t_far, 64, 64, dev_y).wait_recv()
                copy(4, t_far, 64, 64, dev_p).start()

            @pl.when(i == 3)
            def _():
                copy(3, tp_far, 0, 64, dev_p).wait_recv()
                copy(4, tp_far, 64, 64, dev_p).wait_recv()

            compute(2 * lax.rem(y + b1, 2) + lax.rem(k + b0, 2))
            return carry

        lax.fori_loop(0, 4, step, 0)
        copy(0, t, 0, 128, dev_p).wait_send()
        copy(1, t, 0, 64, dev_y).wait_send()
        copy(2, t, 64, 64, dev_y).wait_send()
        copy(3, t_far, 0, 64, dev_p).wait_send()
        copy(4, t_far, 64, 64, dev_p).wait_send()

    def pool_rows(i):
        return rows_at(128 * i, 128)

    def reduce_tensor(phase, layer, compute, beside):
        def to_p(i, slot):
            return rc(
                pool.at[pool_rows(i)],
                ra.at[slot],
                rt_s.at[phase, layer, slot],
                rt_r.at[phase, layer, slot],
                dev_p,
            )

        to_y = rc(ysend, yrecv, rt_s.at[phase, layer, 2], rt_r.at[phase, layer, 2], dev_y)

        def step(i, carry):
            b0, b1 = 1 - lax.rem(i, 2), 1 - i // 2
            pool[pool_rows(i), :] = compute(2 * lax.rem(y + b1, 2) + lax.rem(k + b0, 2))

            @pl.when(i == 0)
            def _():
                to_p(0, 0).start()

            @pl.when(i == 1)
            def _():
                to_p(0, 0).wait_recv()

                def add(r, inner):
                    rr = rows_at(16 * r, 16)
                    ysend[rr, :] = (pool[rows_at(128 + 16 * r, 16), :] + ra[0, rr, :]).astype(BF16)
                    return inner

                lax.fori_loop(0, 8, add, 0)
                to_y.start()

            @pl.when(i == 2)
            def _():
                to_p(2, 1).start()

            return carry

        lax.fori_loop(0, 4, step, 0)
        beside()
        to_p(2, 1).wait_recv()
        to_y.wait_recv()
        to_p(0, 0).wait_send()
        to_p(2, 1).wait_send()
        to_y.wait_send()

        def total(rr, r):
            return pool[rows_at(384 + 16 * r, 16), :] + ra[1, rr, :] + yrecv[rr, :].astype(F32)

        return total

    def reduce_plane(layer, compute, beside):
        def to_p(i, slot):
            return rc(
                pool.at[pool_rows(i)],
                ra.at[slot],
                rp_s.at[layer, slot],
                rp_r.at[layer, slot],
                dev_p,
            )

        d_x = rc(dsend.at[0:64], drecv.at[0:64], rp_s.at[layer, 4], rp_r.at[layer, 4], dev_x)
        d_y = rc(dsend.at[64:128], drecv.at[64:128], rp_s.at[layer, 5], rp_r.at[layer, 5], dev_y)
        to_x = rc(xsend, xrecv, rp_s.at[layer, 6], rp_r.at[layer, 6], dev_x)
        to_y = rc(ysend, yrecv, rp_s.at[layer, 7], rp_r.at[layer, 7], dev_y)

        def step(i, carry):
            q = i // 2
            b0, b1, b2 = 1 - lax.rem(i, 2), 1 - lax.rem(q, 2), 1 - q // 2
            block = (
                4 * lax.rem(c + b2, 2) + 2 * lax.rem(y + b1, 2) + lax.rem(k + b0, 2)
            )
            pool[pool_rows(i), :] = compute(block)

            @pl.when(b0 == 1)
            def _():
                to_p(i, q).start()

            @pl.when(i == 1)
            def _():
                to_p(0, 0).wait_recv()

                def add(r, inner):
                    rr = rows_at(16 * r, 16)
                    dsend[rr, :] = (pool[rows_at(128 + 16 * r, 16), :] + ra[0, rr, :]).astype(BF16)
                    return inner

                lax.fori_loop(0, 8, add, 0)
                d_x.start()
                d_y.start()

            @pl.when(i == 3)
            def _():
                to_p(2, 1).wait_recv()
                d_y.wait_recv()

                def add(r, inner):
                    rr = rows_at(16 * r, 16)
                    rh = rows_at(64 + 16 * r, 16)
                    xsend[rr, :] = (pool[rows_at(384 + 16 * r, 16), :] + ra[1, rr, :]).astype(BF16)
                    xsend[rh, :] = (
                        pool[rows_at(448 + 16 * r, 16), :] + ra[1, rh, :] + drecv[rh, :].astype(F32)
                    ).astype(BF16)
                    return inner

                lax.fori_loop(0, 4, add, 0)
                to_x.start()

            @pl.when(i == 5)
            def _():
                to_p(4, 2).wait_recv()
                d_x.wait_recv()

                def add(r, inner):
                    rr = rows_at(16 * r, 16)
                    rh = rows_at(64 + 16 * r, 16)
                    ysend[rr, :] = (
                        pool[rows_at(640 + 16 * r, 16), :] + ra[2, rr, :] + drecv[rr, :].astype(F32)
                    ).astype(BF16)
                    ysend[rh, :] = (pool[rows_at(704 + 16 * r, 16), :] + ra[2, rh, :]).astype(BF16)
                    return inner

                lax.fori_loop(0, 4, add, 0)
                to_y.start()

            return carry

        lax.fori_loop(0, 8, step, 0)
        beside()
        to_p(6, 3).wait_recv()
        to_x.wait_recv()
        to_y.wait_recv()
        for q in range(4):
            to_p(2 * q, q).wait_send()
        for copy in (d_x, d_y, to_x, to_y):
            copy.wait_send()

        def total(rr, r):
            return (
                pool[rows_at(896 + 16 * r, 16), :]
                + ra[3, rr, :]
                + xrecv[rr, :].astype(F32)
                + yrecv[rr, :].astype(F32)
            )

        return total

    def spread(column):
        return jnp.broadcast_to(column, (column.shape[0], 128))

    def layer_norm(v):
        center = v - jnp.mean(v, axis=-1, keepdims=True)
        r = lax.rsqrt(jnp.mean(center * center, axis=-1, keepdims=True) + epsilon)
        return center * r, r

    def keep(slot, src, dst):
        return pltpu.make_async_copy(src, dst, k_s.at[slot])

    def kept():
        return [(1, ffall, k_ff), (2, pre, k_pre), (3, own, k_own)]

    def head_mask(lo, rows):
        lane = lax.broadcasted_iota(jnp.int32, (rows, 256), 1)
        return (lane >= lo) & (lane < lo + HD)

    def forward(layer, carry):
        ia, iu, id_ = 3 * layer, 3 * layer + 1, 3 * layer + 2
        own_block = 4 * c + t

        def ln1(r, inner):
            rr = rows_at(16 * r, 16)
            n, iv = layer_norm(hb[rr, :])
            own[0, rr, :] = n
            inv[layer, 0, rr, :] = spread(iv)
            mixed[rows_at(128 * own_block + 16 * r, 16), :] = (
                n * (1.0 + mrow(layer, 1)) + mrow(layer, 0)
            ).astype(BF16)
            return inner

        lax.fori_loop(0, 8, ln1, 0)

        @pl.when(layer == 0)
        def _():
            w1(0)
            w2(0)

        @pl.when(layer == 1)
        def _():
            w1(4)
            w2(3)

        def project(block):
            rr = pool_rows(block)
            qkv[layer, rr, :] = (
                nn(mixed[rr, :], w[ia, :, 0:896]) + bias_ref[layer, 0:1, 0:896]
            ).astype(BF16)

        gather_plane(layer, project)

        @pl.when(layer == 0)
        def _():
            w1(1)

        keep(0, mixed, k_mixed.at[layer]).start()

        def take_q(b, inner):
            v = qkv[layer, rows_at(512 * c + 128 * b, 128), 512:896].astype(F32)
            qa[layer, rows_at(128 * b, 128), :] = pltpu.roll(v, 320, 1).astype(BF16)
            return inner

        lax.fori_loop(0, 4, take_q, 0)
        ot[...] = jnp.zeros_like(ot)

        def head(j, inner):
            p = j // 2
            h = j - 2 * p
            win = pl.ds(pl.multiple_of(128 * p, 128), 256)
            vwin = pl.ds(pl.multiple_of(256 + 128 * p, 128), 256)
            lo = 16 * p + 72 * h
            qm = jnp.where(head_mask(lo, 512), qa[layer, :, win].astype(F32), 0.0).astype(BF16)
            pb[0:512, 0:256] = qm

            def scores(kb, m8):
                rr = rows_at(256 * kb, 256)
                s = nt(qkv[layer, rr, win], pb[0:512, 0:256]) * scale
                pool[rr, 0:512] = s
                return jnp.maximum(m8, jnp.max(s.reshape(32, 8, 512), axis=0))

            m8 = lax.fori_loop(0, 4, scores, jnp.full((8, 512), -jnp.inf, F32))
            mx = jnp.max(m8, axis=0, keepdims=True)

            def exps(kb, l8):
                rr = rows_at(128 * kb, 128)
                e = jnp.exp(pool[rr, 0:512] - mx)
                pool[rr, 0:512] = e
                return l8 + fold(e)

            l8 = lax.fori_loop(0, 8, exps, jnp.zeros((8, 512), F32))
            row_sum = jnp.sum(l8, axis=0, keepdims=True)
            lse[layer, j, 0:1, :] = mx + jnp.log(row_sum)
            inverse = 1.0 / row_sum

            def probs(kb, inner2):
                rr = rows_at(128 * kb, 128)
                pb[rows_at(512 + 128 * kb, 128), :] = (pool[rr, 0:512] * inverse).astype(BF16)
                return inner2

            lax.fori_loop(0, 8, probs, 0)
            otw[...] = tn(qkv[layer, :, vwin], pb[512:1536, :])
            ot[pl.ds(pl.multiple_of(96 + 72 * j, 8), 72), :] = otw[
                pl.ds(pl.multiple_of(32 + lo, 8), 72), :
            ]
            return inner

        lax.fori_loop(0, 4, head, 0)

        def put_att(b, inner):
            cols = ot[:, pl.ds(pl.multiple_of(128 * b, 128), 128)]
            att[layer, rows_at(128 * b, 128), :] = cols.T.astype(BF16)
            return inner

        lax.fori_loop(0, 4, put_att, 0)

        @pl.when(layer == 0)
        def _():
            w1(2)

        @pl.when(layer == 1)
        def _():
            w1(5)

        def branch(b):
            return nt(att[layer, rows_at(128 * b, 128), :], w[ia, :, 768:1152])

        total1 = reduce_tensor(0, layer, branch, lambda: None)

        def ln2(r, inner):
            rr = rows_at(16 * r, 16)
            br = total1(rr, r) + bias_ref[layer, 1:2, :]
            own[2, rr, :] = br
            v = hb[rr, :] + mrow(layer, 2) * br
            af[rr, :] = v
            n, iv = layer_norm(v)
            own[1, rr, :] = n
            inv[layer, 1, rr, :] = spread(iv)
            ffall[rows_at(128 * t + 16 * r, 16), :] = (
                n * (1.0 + mrow(layer, 4)) + mrow(layer, 3)
            ).astype(BF16)
            return inner

        lax.fori_loop(0, 8, ln2, 0)
        w2(iu)

        def up(b):
            rr = rows_at(128 * b, 128)
            pre[rr, :] = nn(ffall[rr, :], w[iu]) + bias_ref[layer, 2:3, :]

            def gelu(r, inner):
                r2 = rows_at(128 * b + 16 * r, 16)
                gpre[r2, :] = jax.nn.gelu(pre[r2, :], approximate=True).astype(BF16)
                return inner

            lax.fori_loop(0, 8, gelu, 0)

        gather_tensor(ffall, 0, layer, up)
        w2(id_)

        @pl.when(layer == 0)
        def _():
            keep(1, ffall, k_ff).start()
            keep(2, pre, k_pre).start()

        def down(b):
            return nt(gpre[rows_at(128 * b, 128), :], w[id_])

        def beside():
            @pl.when(layer == 0)
            def _():
                w1(3)

        keep(0, mixed, k_mixed.at[layer]).wait()
        total2 = reduce_tensor(1, layer, down, beside)

        def finish(r, inner):
            rr = rows_at(16 * r, 16)
            fo = total2(rr, r) + bias_ref[layer, 3:4, :]
            own[3, rr, :] = fo
            hb[rr, :] = af[rr, :] + mrow(layer, 5) * fo
            return inner

        lax.fori_loop(0, 8, finish, 0)

        @pl.when(layer == 0)
        def _():
            keep(3, own, k_own).start()
            for slot, src, dst in kept():
                keep(slot, src, dst).wait()

        return carry

    hb[...] = x_ref[...].astype(F32)
    lax.fori_loop(0, LAYERS, forward, 0)
    out_ref[...] = hb[...].astype(BF16)
    for i in range(6):
        w_drain(i)
    hb[...] = cot_ref[...].astype(F32)

    def g_copy0(i, m, d, zz):
        return rc(w.at[i, w_rows(zz, 1 - c)], rx.at[m, zz], gx_s.at[i, d], gx_r.at[i, zz], dev_x)

    def g0(i, m):
        for d, zz in enumerate(zo + [z]):
            g_copy0(i, m, d, zz).start()

    def g_copy1(i, d, zz):
        return rc(w.at[i, w_rows(zz, c)], rz.at[i, d], gz_s.at[i, d], gz_r.at[i, d], (zz, c, t))

    def g1(i, m):
        for d, zz in enumerate(zo + [z]):
            g_copy0(i, m, d, zz).wait_recv()

            def add(r, inner):
                rr = rows_at(288 * zz + half * c + 16 * r, 16)
                w[i, rr, :] = (
                    w[i, rr, :].astype(F32) + rx[m, zz, rows_at(16 * r, 16), :].astype(F32)
                ).astype(BF16)
                return inner

            lax.fori_loop(0, 9, add, 0)
            if d < zs_n - 1:
                g_copy1(i, d, zz).start()

    def g_copy2(i):
        here = gw_ref.at[i, rows_at(half * c, half)]
        return rc(w.at[i, w_rows(z, c)], here, gf_s.at[i], gf_r.at[i], dev_x)

    def g_out(i):
        here = gw_ref.at[i, rows_at(half * c, half)]
        return pltpu.make_async_copy(w.at[i, w_rows(z, c)], here, g_l.at[i])

    def g2(i, m):
        for d in range(zs_n - 1):
            rc(rz.at[i, d], rz.at[i, d], gz_s.at[i, d], gz_r.at[i, d], dev_x).wait_recv()
        for d, zz in enumerate(zo + [z]):
            g_copy0(i, m, d, zz).wait_send()

        def add(r, inner):
            rr = rows_at(288 * z + half * c + 16 * r, 16)
            total = w[i, rr, :].astype(F32)
            for d in range(zs_n - 1):
                total = total + rz[i, d, rows_at(16 * r, 16), :].astype(F32)
            w[i, rr, :] = total.astype(BF16)
            return inner

        lax.fori_loop(0, 9, add, 0)
        g_copy2(i).start()
        g_out(i).start()

    def g3(i):
        other = gw_ref.at[i, rows_at(half * (1 - c), half)]
        rc(other, other, gf_s.at[i], gf_r.at[i], dev_x).wait_recv()
        g_copy2(i).wait_send()
        g_out(i).wait()
        for d, zz in enumerate(zo):
            g_copy1(i, d, zz).wait_send()

    def sm_copy(layer, index, size, dev):
        return rc(
            sm.at[layer, 0:size],
            smr.at[layer, index, 0:size],
            sm_s.at[layer, index],
            sm_r.at[layer, index],
            dev,
        )

    def small(layer):
        for index, size, dev in ((0, 8, dev_p), (1, 8, dev_y), (2, 16, dev_x)):
            step = sm_copy(layer, index, size, dev)
            step.start()
            step.wait_send()
            step.wait_recv()
            sm[layer, 0:size, :] = sm[layer, 0:size, :] + smr[layer, index, 0:size, :]
        small_ref[layer, z] = sm[layer]
        for d, zz in enumerate(zo):
            rc(
                sm.at[layer],
                small_ref.at[layer, z],
                sm_s.at[layer, 3 + d],
                sm_r.at[layer, 3 + z],
                (zz, c, t),
            ).start()

    def small_end(layer):
        for d, zz in enumerate(zo):
            end = rc(
                sm.at[layer],
                small_ref.at[layer, zz],
                sm_s.at[layer, 3 + d],
                sm_r.at[layer, 3 + zz],
                (zz, c, t),
            )
            end.wait_recv()
            end.wait_send()

    zero8 = jnp.zeros((8, D), F32)

    def put_sum(layer, row, v8):
        sm[layer, row : row + 1, 0 : v8.shape[1]] = jnp.sum(v8, axis=0, keepdims=True)

    def backward(step_index, carry):
        layer = LAYERS - 1 - step_index
        ia, iu, id_ = 3 * layer, 3 * layer + 1, 3 * layer + 2

        @pl.when(layer == 0)
        def _():
            keep(3, k_own, own).wait()

        def start(r, sums):
            rr = rows_at(16 * r, 16)
            g = hb[rr, :]
            gf = (mrow(layer, 5) * g).astype(BF16)
            gff[rows_at(128 * t + 16 * r, 16), :] = gf
            return (sums[0] + fold(g * own[3, rr, :]), sums[1] + fold(gf.astype(F32)))

        s_gate2, s_bdown = lax.fori_loop(0, 8, start, (zero8, zero8))
        put_sum(layer, 5, s_gate2)
        put_sum(layer, 7, s_bdown)

        @pl.when(layer == 0)
        def _():
            keep(2, k_pre, pre).wait()

        sm[layer, 9:10, :] = jnp.zeros((1, D), F32)

        def act_back(b):
            rr = rows_at(128 * b, 128)
            pool[rows_at(512, 128), :] = nn(gff[rr, :], w[id_])

            def one(r, total):
                r2 = rows_at(128 * b + 16 * r, 16)
                v = pre[r2, :]
                inner = 0.7978845608028654 * (v + 0.044715 * (v * v * v))
                th = jnp.tanh(inner)
                mixed[r2, :] = (0.5 * v * (1.0 + th)).astype(BF16)
                slope = 0.5 * (1.0 + th) + 0.5 * v * (1.0 - th * th) * (
                    0.7978845608028654 * (1.0 + 0.134145 * (v * v))
                )
                gp = (pool[rows_at(512 + 16 * r, 16), :] * slope).astype(BF16)
                gpre[r2, :] = gp
                return total + fold(gp.astype(F32))

            total = lax.fori_loop(0, 8, one, zero8)
            sm[layer, 9:10, :] = sm[layer, 9:10, :] + jnp.sum(total, axis=0, keepdims=True)

        gather_tensor(gff, 1, layer, act_back)

        @pl.when(layer == 1)
        def _():
            keep(2, k_pre, pre).start()

        @pl.when(layer == 0)
        def _():
            g2(5, 2)
            keep(1, k_ff, ffall).wait()

        def ffin_back(b):
            return nt(gpre[rows_at(128 * b, 128), :], w[iu])

        def beside1():
            def one_d(i, inner):
                cols = pl.ds(pl.multiple_of(128 * i, 128), 128)
                w[id_, rows_at(128 * i, 128), :] = tn(gff[:, cols], mixed[0:512, :]).astype(BF16)
                return inner

            lax.fori_loop(0, 9, one_d, 0)
            g0(id_, 2)
            keep(0, k_mixed.at[layer], mixed).start()

            def one_u(i, inner):
                cols = pl.ds(pl.multiple_of(128 * i, 128), 128)
                w[iu, rows_at(128 * i, 128), :] = tn(ffall[:, cols], gpre[...]).astype(BF16)
                return inner

            lax.fori_loop(0, 9, one_u, 0)
            g0(iu, 1 + 2 * layer)

            @pl.when(layer == 1)
            def _():
                keep(1, k_ff, ffall).start()

        total1 = reduce_tensor(2, layer, ffin_back, beside1)

        @pl.when(layer == 0)
        def _():
            g1(3, 0)

        def mid(r, sums):
            rr = rows_at(16 * r, 16)
            gf = total1(rr, r)
            n = own[1, rr, :]
            e = gf * (1.0 + mrow(layer, 4))
            iv = inv[layer, 1, rr, 0:1]
            ga = hb[rr, :] + iv * (
                e
                - jnp.mean(e, axis=-1, keepdims=True)
                - n * jnp.mean(e * n, axis=-1, keepdims=True)
            )
            hb[rr, :] = ga
            gbv = (mrow(layer, 2) * ga).astype(BF16)
            gb[rows_at(128 * t + 16 * r, 16), :] = gbv
            return (
                sums[0] + fold(gf),
                sums[1] + fold(gf * n),
                sums[2] + fold(ga * own[2, rr, :]),
                sums[3] + fold(gbv.astype(F32)),
            )

        s_shift2, s_scale2, s_gate1, s_bproj = lax.fori_loop(
            0, 8, mid, (zero8, zero8, zero8, zero8)
        )
        put_sum(layer, 3, s_shift2)
        put_sum(layer, 4, s_scale2)
        put_sum(layer, 2, s_gate1)
        put_sum(layer, 6, s_bproj)

        def att_back(b):
            rr = rows_at(128 * b, 128)
            v = nn(gb[rr, :], w[ia, :, 768:1152])
            dqkv[rr, 0:384] = pltpu.roll(v, 320, 1).astype(BF16)

        gather_tensor(gb, 2, layer, att_back)

        @pl.when(layer == 0)
        def _():
            g2(4, 3)

        dkv[...] = jnp.zeros_like(dkv)
        ot[...] = jnp.zeros_like(ot)

        def head(j, inner):
            p = j // 2
            h = j - 2 * p
            win = pl.ds(pl.multiple_of(128 * p, 128), 256)
            vwin = pl.ds(pl.multiple_of(256 + 128 * p, 128), 256)
            lo = 16 * p + 72 * h
            qm = jnp.where(head_mask(lo, 512), qa[layer, :, win].astype(F32), 0.0).astype(BF16)
            dm = jnp.where(head_mask(32 + lo, 512), dqkv[0:512, win].astype(F32), 0.0).astype(BF16)
            pb[0:512, 0:256] = qm
            pb[0:512, 256:512] = dm
            log_row = lse[layer, j, 0:1, :]

            def first(kb, d8):
                rr = rows_at(256 * kb, 256)
                s = nt(qkv[layer, rr, win], pb[0:512, 0:256]) * scale
                pr = jnp.exp(s - log_row)
                dp = nt(qkv[layer, rr, vwin], pb[0:512, 256:512])
                pool[rr, 0:512] = pr
                pool[rr, 512:1024] = dp
                dkv[rr, vwin] = dkv[rr, vwin] + nn(pr.astype(BF16), pb[0:512, 256:512])
                return d8 + fold(pr * dp)

            d8 = lax.fori_loop(0, 4, first, jnp.zeros((8, 512), F32))
            delta = jnp.sum(d8, axis=0, keepdims=True)

            def second(kb, inner2):
                rr = rows_at(256 * kb, 256)
                ds = (pool[rr, 0:512] * (pool[rr, 512:1024] - delta)).astype(BF16)
                pb[rows_at(512 + 256 * kb, 256), :] = ds
                dkv[rr, win] = dkv[rr, win] + nn(ds, pb[0:512, 0:256]) * scale
                return inner2

            lax.fori_loop(0, 4, second, 0)
            otw[...] = tn(qkv[layer, :, win], pb[512:1536, :]) * scale
            ot[pl.ds(pl.multiple_of(64 + 72 * j, 8), 72), :] = otw[
                pl.ds(pl.multiple_of(lo, 8), 72), :
            ]
            return inner

        lax.fori_loop(0, 4, head, 0)

        def put_kv(b, total):
            rr = rows_at(128 * b, 128)
            kv = dkv[rr, :].astype(BF16)
            dqkv[rr, 0:640] = kv
            dqkv[rr, 640:896] = jnp.zeros((128, 256), BF16)
            return total + fold(kv.astype(F32))

        s_kv = lax.fori_loop(0, 8, put_kv, jnp.zeros((8, 640), F32))

        def put_q(b, total):
            rr = rows_at(512 * c + 128 * b, 128)
            dq = ot[:, pl.ds(pl.multiple_of(128 * b, 128), 128)].T.astype(BF16).astype(F32)
            dqkv[rr, 512:640] = (dkv[rr, 512:640] + dq[:, 0:128]).astype(BF16)
            dqkv[rr, 640:896] = dq[:, 128:384].astype(BF16)
            return total + fold(dq)

        s_q = lax.fori_loop(0, 4, put_q, jnp.zeros((8, 384), F32))
        sm[layer, 8:9, :] = jnp.zeros((1, D), F32)
        sm[layer, 8:9, 0:640] = jnp.sum(s_kv, axis=0, keepdims=True)
        sm[layer, 8:9, 512:896] = sm[layer, 8:9, 512:896] + jnp.sum(s_q, axis=0, keepdims=True)
        g1(id_, 2)

        @pl.when(layer == 0)
        def _():
            g2(3, 0)

        def mix_back(block):
            return nt(dqkv[pool_rows(block), :], w[ia, :, 0:896])

        def beside2():
            keep(0, k_mixed.at[layer], mixed).wait()

            def one(i, inner):
                cols = pl.ds(pl.multiple_of(128 * i, 128), 128)
                rr = rows_at(128 * i, 128)
                w[ia, rr, 0:640] = tn(mixed[:, cols], dqkv[:, 0:640]).astype(BF16)
                here = rows_at(512 * c, 512)
                r2 = tn(mixed[here, cols], dqkv[here, 640:896])
                r3 = tn(gb[:, cols], att[layer])
                w[ia, rr, 640:768] = r2[:, 0:128].astype(BF16)
                w[ia, rr, 768:896] = (r2[:, 128:256] + r3[:, 0:128]).astype(BF16)
                w[ia, rr, 896:1152] = r3[:, 128:384].astype(BF16)
                return inner

            lax.fori_loop(0, 9, one, 0)
            g0(ia, 0)
            g1(iu, 1 + 2 * layer)


        total2 = reduce_plane(layer, mix_back, beside2)

        def last(r, sums):
            rr = rows_at(16 * r, 16)
            gm = total2(rr, r)
            n = own[0, rr, :]
            e = gm * (1.0 + mrow(layer, 1))
            iv = inv[layer, 0, rr, 0:1]
            hb[rr, :] = hb[rr, :] + iv * (
                e
                - jnp.mean(e, axis=-1, keepdims=True)
                - n * jnp.mean(e * n, axis=-1, keepdims=True)
            )
            return (sums[0] + fold(gm), sums[1] + fold(gm * n))

        s_shift1, s_scale1 = lax.fori_loop(0, 8, last, (zero8, zero8))
        put_sum(layer, 0, s_shift1)
        put_sum(layer, 1, s_scale1)

        @pl.when(layer == 1)
        def _():
            keep(3, k_own, own).start()

        return carry

    sm[...] = jnp.zeros_like(sm)
    lax.fori_loop(0, LAYERS, backward, 0)
    small(1)
    small(0)
    g2(2, 2)
    g1(0, 0)
    g2(1, 1)
    small_end(1)
    small_end(0)
    g2(0, 0)
    for i in range(6):
        g3(i)


def run_stage(zs_n, x_in, cot, modin, bias, blocks):
    vm = pl.BlockSpec(memory_space=pltpu.VMEM)
    anyspace = pl.BlockSpec(memory_space=pl.ANY)
    dma = pltpu.SemaphoreType.DMA
    sds = jax.ShapeDtypeStruct
    scratch = [
        pltpu.VMEM((6, D, D), BF16),
        pltpu.VMEM((1024, D), BF16),
        pltpu.VMEM((2, 1024, 896), BF16),
        pltpu.VMEM((2, 512, 384), BF16),
        pltpu.VMEM((2, 512, 384), BF16),
        pltpu.VMEM((512, D), BF16),
        pltpu.VMEM((512, D), F32),
        pltpu.VMEM((4, 128, D), F32),
        pltpu.VMEM((2, 2, 128, 128), F32),
        pltpu.VMEM((2, 4, 8, 512), F32),
        pltpu.VMEM((zs_n, 16, 384), F32),
        pltpu.VMEM((2, 8, D), F32),
        pltpu.VMEM((128, D), F32),
        pltpu.VMEM((1024, D), F32),
        pltpu.VMEM((4, 128, D), F32),
        pltpu.VMEM((128, D), BF16),
        pltpu.VMEM((128, D), BF16),
        pltpu.VMEM((128, D), BF16),
        pltpu.VMEM((128, D), BF16),
        pltpu.VMEM((128, D), BF16),
        pltpu.VMEM((128, D), BF16),
        pltpu.VMEM((512, D), BF16),
        pltpu.VMEM((512, D), BF16),
        pltpu.VMEM((512, D), BF16),
        pltpu.VMEM((1024, 896), BF16),
        pltpu.VMEM((1024, 640), F32),
        pltpu.VMEM((1536, 512), BF16),
        pltpu.VMEM((256, 512), F32),
        pltpu.VMEM((384, 512), F32),
        pltpu.VMEM((4, zs_n, 144, D), BF16),
        pltpu.VMEM((6, zs_n - 1, 144, D), BF16),
        pltpu.VMEM((2, 16, D), F32),
        pltpu.VMEM((2, 3, 16, D), F32),
        dma((zs_n - 1,)),
        dma((zs_n,)),
        dma((6, zs_n)),
        dma((6, zs_n)),
        dma((6, zs_n)),
        dma((6, zs_n)),
        dma((6,)),
        dma((2, 13)),
        dma((2, 13)),
        dma((3, 2, 5)),
        dma((3, 2, 5)),
        dma((3, 2, 3)),
        dma((3, 2, 3)),
        dma((2, 8)),
        dma((2, 8)),
        dma((6, zs_n)),
        dma((6, zs_n)),
        dma((6, zs_n)),
        dma((6, zs_n)),
        dma((6,)),
        dma((6,)),
        dma((6,)),
        dma((2, 3 + zs_n)),
        dma((2, 3 + zs_n)),
        dma((4,)),
    ]
    return pl.pallas_call(
        functools.partial(stage_kernel, zs_n),
        name="two_blocks",
        out_shape=(
            sds((128, D), BF16),
            sds((128, D), F32),
            sds((6, 288, D), BF16),
            sds((2, zs_n, 16, D), F32),
            sds((2, 1024, D), BF16),
            sds((512, D), BF16),
            sds((512, D), F32),
            sds((4, 128, D), F32),
        ),
        in_specs=[vm, vm, vm, vm, anyspace],
        out_specs=(vm, vm, anyspace, vm, anyspace, anyspace, anyspace, anyspace),
        scratch_shapes=scratch,
        compiler_params=pltpu.CompilerParams(
            collective_id=0, has_side_effects=True, vmem_limit_bytes=67043328
        ),
    )(x_in, cot, modin, bias, blocks)


def fast_body(
    zs_n,
    x_in,
    cond,
    w_ada,
    b_ada,
    w_qkv,
    b_qv,
    w_proj,
    b_proj,
    up_weight,
    up_bias_vector,
    down_weight,
    down_bias_vector,
    cotangent,
):
    z = lax.axis_index("shard")
    cols = w_ada.shape[3]
    heads = w_qkv.shape[3]
    cond_low = jax.nn.silu(cond).astype(BF16)
    mod_terms = (
        jnp.einsum("sd,ldkc->lskc", cond_low, w_ada, preferred_element_type=F32)
        + b_ada.astype(F32)[:, None]
    ).astype(BF16)
    modin = jnp.pad(
        mod_terms.astype(F32).transpose(1, 0, 2, 3), ((0, 0), (0, 0), (0, 2), (0, 384 - cols))
    ).reshape(zs_n, 16, 384)
    parts = []
    for layer in range(LAYERS):
        parts.append(
            jnp.concatenate(
                (
                    w_qkv[layer, 1],
                    w_qkv[layer, 2],
                    w_qkv[layer, 0],
                    w_proj[layer].T,
                ),
                axis=1,
            )
        )
        parts.append(up_weight[layer])
        parts.append(down_weight[layer].T)
    blocks = jnp.stack(parts)
    zero = jnp.zeros((LAYERS, heads), F32)
    b_qkv = jnp.concatenate(
        (zero, b_qv[:, 1].astype(F32), b_qv[:, 0].astype(F32), zero), axis=1
    )
    bias = jnp.stack(
        (b_qkv, b_proj.astype(F32), up_bias_vector.astype(F32), down_bias_vector.astype(F32)),
        axis=1,
    )
    out, grad_in, gw, small = run_stage(
        zs_n, x_in[:, 0], cotangent[:, 0], modin, bias, blocks
    )[:4]
    grad_mod = small[:, :, 0:6, :].astype(BF16)
    mod_cols = lax.dynamic_slice_in_dim(grad_mod, z * cols, cols, 3)
    grad_w_ada = jnp.einsum("sd,lskc->ldkc", cond_low, mod_cols, preferred_element_type=F32)
    grad_b_ada = jnp.sum(mod_cols.astype(F32), axis=1)
    cond_part = jnp.einsum("lskc,ldkc->sd", mod_cols, w_ada, preferred_element_type=F32)
    cond_total = lax.psum(cond_part, "shard")
    silu_value, silu_back = jax.vjp(jax.nn.silu, cond)
    grad_cond = silu_back(cond_total)[0]
    sums = jnp.sum(small[:, :, 6:10, :], axis=1)
    gw = gw.reshape(LAYERS, 3, cols, D).astype(F32)
    ga = gw[:, 0]
    return (
        out[:, None],
        grad_in[:, None],
        grad_cond,
        grad_w_ada,
        grad_b_ada,
        jnp.stack(
            (ga[:, :, 2 * heads : 3 * heads], ga[:, :, 0:heads], ga[:, :, heads : 2 * heads]),
            axis=1,
        ),
        jnp.stack((sums[:, 2, 2 * heads : 3 * heads], sums[:, 2, heads : 2 * heads]), axis=1),
        ga[:, :, 3 * heads :].transpose(0, 2, 1),
        sums[:, 0],
        gw[:, 1],
        sums[:, 3],
        gw[:, 2].transpose(0, 2, 1),
        sums[:, 1],
    )


def solution(mesh):
    shape = mesh.shape
    program = body
    if shape["context"] == 2 and shape["tensor"] == 4 and shape["shard"] == 4:
        program = functools.partial(fast_body, shape["shard"])
    return jax.shard_map(
        program,
        mesh=mesh,
        in_specs=(
            P(("context", "tensor"), "shard", None),
            P(),
            P(None, None, None, "shard"),
            P(None, None, "shard"),
            P(None, None, "shard", "tensor"),
            P(None, None, "tensor"),
            P(None, "tensor", "shard"),
            P(),
            P(None, "shard", "tensor"),
            P(None, "tensor"),
            P(None, "tensor", "shard"),
            P(),
            P(("context", "tensor"), "shard", None),
        ),
        out_specs=(
            P(("context", "tensor"), "shard", None),
            P(("context", "tensor"), "shard", None),
            P(),
            P(None, None, None, "shard"),
            P(None, None, "shard"),
            P(None, None, "shard", "tensor"),
            P(None, None, "tensor"),
            P(None, "tensor", "shard"),
            P(),
            P(None, "shard", "tensor"),
            P(None, "tensor"),
            P(None, "tensor", "shard"),
            P(),
        ),
        check_vma=False,
    )
```

```python
import functools

import jax
import jax.numpy as jnp
from jax import lax
from jax.experimental import pallas as pl
from jax.experimental.pallas import tpu as pltpu
from jax.sharding import PartitionSpec as P

D = 1152
HD = 72
FF = 4608
LAYERS = 2


epsilon = 1e-06


def normalize(values):
    center = values - jnp.mean(values, axis=-1, keepdims=True)
    inverse = lax.rsqrt(jnp.mean(center * center, axis=-1, keepdims=True) + epsilon)
    return (center * inverse, inverse)


def normalize_back(grad_normed, normed, inverse):
    mean_grad = jnp.mean(grad_normed, axis=-1, keepdims=True)
    mean_proj = jnp.mean(grad_normed * normed, axis=-1, keepdims=True)
    return inverse * (grad_normed - mean_grad - normed * mean_proj)


def gelu_tanh(values):
    return jax.nn.gelu(values, approximate=True)


def to_heads(tokens):
    return tokens.reshape(tokens.shape[0], tokens.shape[1], -1, HD).transpose(1, 2, 0, 3)


def from_heads(blocks):
    return blocks.transpose(2, 0, 1, 3).reshape(blocks.shape[2], blocks.shape[0], -1)


def over_heads(head_fn, arrays):
    return lax.map(lambda seq_items: lax.map(head_fn, seq_items), arrays)


def score_block(query_head, key_head):
    return jnp.einsum(
        "qe,ke->qk", query_head, key_head, preferred_element_type=jnp.float32
    ) * HD ** (-0.5)


def forward_head(head_parts):
    query_head, key_head, value_head = head_parts
    scores = score_block(query_head, key_head)
    maxima = jnp.max(scores, axis=-1, keepdims=True)
    exp_scores = jnp.exp(scores - maxima)
    row_total = jnp.sum(exp_scores, axis=-1, keepdims=True)
    prob_low = (exp_scores / row_total).astype(jnp.bfloat16)
    result = jnp.dot(prob_low, value_head, preferred_element_type=jnp.float32).astype(jnp.bfloat16)
    return (result, (maxima + jnp.log(row_total))[:, 0])


def full_grads(head_parts):
    query_head, key_head, value_head, grad_head, log_head = head_parts
    prob_full = jnp.exp(score_block(query_head, key_head) - log_head[:, None])
    grad_prob = jnp.einsum("qe,ke->qk", grad_head, value_head, preferred_element_type=jnp.float32)
    row_delta = jnp.sum(prob_full * grad_prob, axis=-1, keepdims=True)
    grad_score = (prob_full * (grad_prob - row_delta)).astype(jnp.bfloat16)
    grad_query = jnp.dot(grad_score, key_head, preferred_element_type=jnp.float32) * HD ** (-0.5)
    grad_key = jnp.einsum(
        "qk,qe->ke", grad_score, query_head, preferred_element_type=jnp.float32
    ) * HD ** (-0.5)
    grad_value = jnp.einsum(
        "qk,qe->ke", prob_full.astype(jnp.bfloat16), grad_head, preferred_element_type=jnp.float32
    )
    return (grad_query, grad_key, grad_value)


def fetch_weights(qkv_part, proj_part, up_part, down_part, mod_part):
    return (
        lax.all_gather(qkv_part, "shard", axis=2, tiled=True),
        lax.all_gather(proj_part, "shard", axis=2, tiled=True),
        lax.all_gather(up_part, "shard", axis=1, tiled=True),
        lax.all_gather(down_part, "shard", axis=2, tiled=True),
        lax.all_gather(mod_part, "shard", axis=3, tiled=True),
    )


def layer_forward(hidden_state, weights, modulation, biases):
    full_qkv, full_proj, full_up, full_down, mod_unused = weights
    bias_qv, bias_proj, bias_up, bias_down = biases
    normed1, inverse1 = normalize(hidden_state)
    mix_in = (normed1 * (1.0 + modulation[:, 1]) + modulation[:, 0]).astype(jnp.bfloat16)
    mixed_all = lax.all_gather(mix_in, "tensor", axis=0, tiled=True)
    projected = jnp.einsum("tbd,kde->tbke", mixed_all, full_qkv, preferred_element_type=jnp.float32)
    queries = (projected[:, :, 0] + bias_qv[0]).astype(jnp.bfloat16)
    keys_own = projected[:, :, 1].astype(jnp.bfloat16)
    values_own = (projected[:, :, 2] + bias_qv[1]).astype(jnp.bfloat16)
    keys_all, values_all = (
        lax.all_gather(keys_own, "context", axis=0, tiled=True),
        lax.all_gather(values_own, "context", axis=0, tiled=True),
    )
    head_out, log_sums = over_heads(
        forward_head, (to_heads(queries), to_heads(keys_all), to_heads(values_all))
    )
    attended = from_heads(head_out)
    row_block = attended
    branch = (
        lax.psum_scatter(
            jnp.einsum("tbe,ed->tbd", row_block, full_proj, preferred_element_type=jnp.float32),
            "tensor",
            scatter_dimension=0,
            tiled=True,
        )
        + bias_proj
    )
    after_attn = hidden_state + modulation[:, 2] * branch
    normed2, inverse2 = normalize(after_attn)
    feedforward_input = (normed2 * (1.0 + modulation[:, 4]) + modulation[:, 3]).astype(jnp.bfloat16)
    ff_all = lax.all_gather(feedforward_input, "tensor", axis=0, tiled=True)
    preactivation_value = (
        jnp.einsum("tbd,df->tbf", ff_all, full_up, preferred_element_type=jnp.float32) + bias_up
    )
    activation_value = gelu_tanh(preactivation_value).astype(jnp.bfloat16)
    row_block = activation_value
    feedforward_output = (
        lax.psum_scatter(
            jnp.einsum(
                "tbf,fd->tbd", row_block, full_down, preferred_element_type=jnp.float32
            ).astype(jnp.bfloat16),
            "tensor",
            scatter_dimension=0,
            tiled=True,
        ).astype(jnp.float32)
        + bias_down
    )
    result = after_attn + modulation[:, 5] * feedforward_output
    stash = (
        normed1,
        inverse1,
        mixed_all,
        queries,
        keys_all,
        values_all,
        attended,
        log_sums,
        branch,
        normed2,
        inverse2,
        ff_all,
        preactivation_value,
        activation_value,
        feedforward_output,
    )
    return (result, stash)


def layer_backward(grad_hidden, weights, modulation, stash):
    full_qkv, full_proj, full_up, full_down, mod_unused = weights
    (
        normed1,
        inverse1,
        mixed_all,
        queries,
        keys_all,
        values_all,
        attended,
        log_sums,
        branch,
        normed2,
        inverse2,
        ff_all,
        preactivation_value,
        activation_value,
        feedforward_output,
    ) = stash
    grad_ff = (modulation[:, 5] * grad_hidden).astype(jnp.bfloat16)
    grad_gate2 = jnp.sum(grad_hidden * feedforward_output, axis=0)
    bias_down = jnp.sum(grad_ff.astype(jnp.float32), axis=(0, 1))
    grad_ff_all = lax.all_gather(grad_ff, "tensor", axis=0, tiled=True)
    grad_w_down = jnp.einsum(
        "tbf,tbd->fd", activation_value, grad_ff_all, preferred_element_type=jnp.float32
    )
    grad_activ = jnp.einsum(
        "tbd,fd->tbf", grad_ff_all, full_down, preferred_element_type=jnp.float32
    )
    gelu_value, gelu_back = jax.vjp(gelu_tanh, preactivation_value)
    grad_pre = gelu_back(grad_activ)[0].astype(jnp.bfloat16)
    bias_up = jnp.sum(grad_pre.astype(jnp.float32), axis=(0, 1))
    grad_w_up = jnp.einsum("tbd,tbf->df", ff_all, grad_pre, preferred_element_type=jnp.float32)
    row_block = grad_pre
    grad_ffin = lax.psum_scatter(
        jnp.einsum("tbf,df->tbd", row_block, full_up, preferred_element_type=jnp.float32).astype(
            jnp.bfloat16
        ),
        "tensor",
        scatter_dimension=0,
        tiled=True,
    ).astype(jnp.float32)
    grad_shift2 = jnp.sum(grad_ffin, axis=0)
    grad_scale2 = jnp.sum(grad_ffin * normed2, axis=0)
    grad_after = grad_hidden + normalize_back(
        grad_ffin * (1.0 + modulation[:, 4]), normed2, inverse2
    )
    grad_branch = (modulation[:, 2] * grad_after).astype(jnp.bfloat16)
    grad_gate1 = jnp.sum(grad_after * branch, axis=0)
    bias_proj = jnp.sum(grad_branch.astype(jnp.float32), axis=(0, 1))
    grad_branch_all = lax.all_gather(grad_branch, "tensor", axis=0, tiled=True)
    grad_w_proj = jnp.einsum(
        "tbe,tbd->ed", attended, grad_branch_all, preferred_element_type=jnp.float32
    )
    grad_attended = jnp.einsum(
        "tbd,ed->tbe", grad_branch_all, full_proj, preferred_element_type=jnp.float32
    ).astype(jnp.bfloat16)
    head_inputs = (
        to_heads(queries),
        to_heads(keys_all),
        to_heads(values_all),
        to_heads(grad_attended),
        log_sums,
    )
    grad_q_heads, grad_k_heads, grad_v_heads = over_heads(full_grads, head_inputs)
    grad_queries = from_heads(grad_q_heads).astype(jnp.bfloat16)
    grad_keys, grad_values = (
        lax.psum_scatter(
            from_heads(grad_k_heads).astype(jnp.bfloat16),
            "context",
            scatter_dimension=0,
            tiled=True,
        ).astype(jnp.float32),
        lax.psum_scatter(
            from_heads(grad_v_heads).astype(jnp.bfloat16),
            "context",
            scatter_dimension=0,
            tiled=True,
        ).astype(jnp.float32),
    )
    grad_keys = grad_keys.astype(jnp.bfloat16)
    grad_values = grad_values.astype(jnp.bfloat16)
    grad_qkv = jnp.stack((grad_queries, grad_keys, grad_values), axis=2)
    bias_qv = jnp.stack(
        (
            jnp.sum(grad_queries.astype(jnp.float32), axis=(0, 1)),
            jnp.sum(grad_values.astype(jnp.float32), axis=(0, 1)),
        )
    )
    grad_w_qkv = jnp.einsum(
        "tbd,tbke->kde", mixed_all, grad_qkv, preferred_element_type=jnp.float32
    )
    row_block = grad_qkv
    grad_mixin = lax.psum_scatter(
        jnp.einsum("tbke,kde->tbd", row_block, full_qkv, preferred_element_type=jnp.float32).astype(
            jnp.bfloat16
        ),
        "tensor",
        scatter_dimension=0,
        tiled=True,
    ).astype(jnp.float32)
    grad_shift1 = jnp.sum(grad_mixin, axis=0)
    grad_scale1 = jnp.sum(grad_mixin * normed1, axis=0)
    grad_input = grad_after + normalize_back(
        grad_mixin * (1.0 + modulation[:, 1]), normed1, inverse1
    )
    grad_mod_own = jnp.stack(
        (grad_shift1, grad_scale1, grad_gate1, grad_shift2, grad_scale2, grad_gate2), axis=1
    )
    return (
        grad_input,
        (grad_w_qkv, grad_w_proj, grad_w_up, grad_w_down),
        (grad_mod_own, bias_qv, bias_proj, bias_up, bias_down),
    )


def body(
    x_in,
    cond,
    w_ada,
    b_ada,
    w_qkv,
    b_qv,
    w_proj,
    b_proj,
    up_weight,
    up_bias_vector,
    down_weight,
    down_bias_vector,
    cotangent,
):
    shard_index = lax.axis_index("shard")
    tensor_index = lax.axis_index("tensor")
    context_index = lax.axis_index("context")
    own_latents = x_in.shape[1]
    all_latents = cond.shape[0]
    shard_cols = w_ada.shape[3]
    head_cols = w_qkv.shape[3]
    hidden_cols = up_weight.shape[2]
    condition_reduced = jax.nn.silu(cond).astype(jnp.bfloat16)
    mod_terms = (
        jnp.einsum("sd,ldkc->lskc", condition_reduced, w_ada, preferred_element_type=jnp.float32)
        + b_ada.astype(jnp.float32)[:, None]
    ).astype(jnp.bfloat16)
    hidden_state = x_in.astype(jnp.float32)
    layer_state = []
    for layer_number_index in range(LAYERS):
        sliced = fetch_weights(
            w_qkv[layer_number_index : layer_number_index + 1],
            w_proj[layer_number_index : layer_number_index + 1],
            up_weight[layer_number_index : layer_number_index + 1],
            down_weight[layer_number_index : layer_number_index + 1],
            mod_terms[layer_number_index : layer_number_index + 1],
        )
        weights = tuple((member_entry[0] for member_entry in sliced))
        modulation = lax.dynamic_slice_in_dim(
            weights[4], shard_index * own_latents, own_latents, 0
        ).astype(jnp.float32)
        biases = (
            b_qv[layer_number_index].astype(jnp.float32),
            b_proj[layer_number_index].astype(jnp.float32),
            up_bias_vector[layer_number_index].astype(jnp.float32),
            down_bias_vector[layer_number_index].astype(jnp.float32),
        )
        hidden_state, stash = layer_forward(hidden_state, weights, modulation, biases)
        layer_state.append((weights, modulation, stash))
    output = hidden_state.astype(jnp.bfloat16)
    grad_hidden = cotangent.astype(jnp.float32)
    cond_total = jnp.zeros(cond.shape, jnp.float32)
    results = [None] * LAYERS
    context_mask = (context_index == 0).astype(jnp.float32)
    for layer_number_index in reversed(range(LAYERS)):
        weights, modulation, stash = layer_state[layer_number_index]
        grad_hidden, matrix_grads, small_terms = layer_backward(
            grad_hidden, weights, modulation, stash
        )
        grad_mod_own, bias_qv, bias_proj, bias_up, bias_down = small_terms
        grad_mod_pad = lax.dynamic_update_slice_in_dim(
            jnp.zeros((all_latents, 6, D), jnp.float32), grad_mod_own, shard_index * own_latents, 0
        )
        bias_qv_pad = lax.dynamic_update_slice_in_dim(
            jnp.zeros((2, D), jnp.float32), bias_qv, tensor_index * head_cols, 1
        )
        bias_up_pad = lax.dynamic_update_slice_in_dim(
            jnp.zeros((FF,), jnp.float32), bias_up, tensor_index * hidden_cols, 0
        )
        mod_sum, proj_sum, down_sum, qv_sum, up_sum = lax.psum(
            (grad_mod_pad, bias_proj, bias_down, bias_qv_pad, bias_up_pad),
            ("shard", "context", "tensor"),
        )
        mod_cols = lax.dynamic_slice_in_dim(
            mod_sum.astype(jnp.bfloat16), shard_index * shard_cols, shard_cols, 2
        )
        grad_w_ada = jnp.einsum(
            "sd,skc->dkc", condition_reduced, mod_cols, preferred_element_type=jnp.float32
        )
        grad_b_ada = jnp.sum(mod_cols.astype(jnp.float32), axis=0)
        cond_part = (
            jnp.einsum(
                "skc,dkc->sd",
                mod_cols,
                w_ada[layer_number_index],
                preferred_element_type=jnp.float32,
            )
            * context_mask
        )
        grad_w_qkv, grad_w_proj, grad_w_up, grad_w_down = matrix_grads
        qkv_all, proj_all, up_all, down_all, cond_sum = (
            lax.psum(grad_w_qkv.astype(jnp.bfloat16), ("shard", "context")).astype(jnp.float32),
            lax.psum(grad_w_proj.astype(jnp.bfloat16), ("shard", "context")).astype(jnp.float32),
            lax.psum(grad_w_up.astype(jnp.bfloat16), ("shard", "context")).astype(jnp.float32),
            lax.psum(grad_w_down.astype(jnp.bfloat16), ("shard", "context")).astype(jnp.float32),
            lax.psum(cond_part.astype(jnp.bfloat16), ("shard", "context")).astype(jnp.float32),
        )
        qkv_own = lax.dynamic_slice_in_dim(qkv_all, shard_index * shard_cols, shard_cols, 1)
        proj_own = lax.dynamic_slice_in_dim(proj_all, shard_index * shard_cols, shard_cols, 1)
        up_own = lax.dynamic_slice_in_dim(up_all, shard_index * shard_cols, shard_cols, 0)
        down_own = lax.dynamic_slice_in_dim(down_all, shard_index * shard_cols, shard_cols, 1)
        cond_total = cond_total + cond_sum
        results[layer_number_index] = (
            grad_w_ada,
            grad_b_ada,
            qkv_own,
            lax.dynamic_slice_in_dim(qv_sum, tensor_index * head_cols, head_cols, 1),
            proj_own,
            proj_sum,
            up_own,
            lax.dynamic_slice_in_dim(up_sum, tensor_index * hidden_cols, hidden_cols, 0),
            down_own,
            down_sum,
        )
    silu_value, silu_back = jax.vjp(jax.nn.silu, cond)
    grad_cond = silu_back(cond_total)[0]
    stacked = tuple(
        (
            jnp.stack(
                [results[layer_number_index][member_entry] for layer_number_index in range(LAYERS)]
            )
            for member_entry in range(10)
        )
    )
    return (
        output,
        grad_hidden,
        grad_cond,
        stacked[0],
        stacked[1],
        stacked[2],
        stacked[3],
        stacked[4],
        stacked[5],
        stacked[6],
        stacked[7],
        stacked[8],
        stacked[9],
    )


MESH = pl.DeviceIdType.MESH
F32 = jnp.float32
BF16 = jnp.bfloat16


def nt(a, b):
    return lax.dot_general(a, b, (((1,), (1,)), ((), ())), preferred_element_type=F32)


def nn(a, b):
    return jnp.dot(a, b, preferred_element_type=F32)


def tn(a, b):
    return lax.dot_general(a, b, (((0,), (0,)), ((), ())), preferred_element_type=F32)


def fold(v):
    return jnp.sum(v.reshape(v.shape[0] // 8, 8, v.shape[1]), axis=0)


def rows_at(start, size, multiple=16):
    return pl.ds(pl.multiple_of(start, multiple), size)


def stage_kernel(
    zs_n,
    x_ref,
    cot_ref,
    modin_ref,
    bias_ref,
    sa_ref,
    su_ref,
    sd_ref,
    out_ref,
    gin_ref,
    gw_ref,
    small_ref,
    w,
    mixed,
    qkv,
    qa,
    att,
    ffall,
    pre,
    act,
    own,
    inv,
    lse,
    modr,
    modv,
    af,
    pool,
    ra,
    ysend,
    yrecv,
    xsend,
    xrecv,
    dsend,
    drecv,
    gff,
    gpre,
    gb,
    doa,
    dqkv,
    dkv,
    pb,
    otw,
    ot,
    rz,
    sm,
    smr,
    m_s,
    m_r,
    wz_s,
    wz_r,
    w_l,
    ap_s,
    ap_r,
    rp_s,
    rp_r,
    gz_s,
    gz_r,
    gf_s,
    gf_r,
    g_l,
    sm_s,
    sm_r,
):
    z = lax.axis_index("shard")
    c = lax.axis_index("context")
    t = lax.axis_index("tensor")
    y = t // 2
    k = t - 2 * y
    tp = t + 1 - 2 * k
    t_far = t + 2 - 4 * y
    tp_far = tp + 2 - 4 * y
    dev_p = (z, c, tp)
    dev_y = (z, c, t_far)
    dev_x = (z, 1 - c, t)
    zo = [lax.rem(z + d, zs_n) for d in range(1, zs_n)]
    scale = HD ** (-0.5)
    hb = gin_ref

    def rc(src, dst, ss, rs, dev):
        return pltpu.make_async_remote_copy(
            src_ref=src, dst_ref=dst, send_sem=ss, recv_sem=rs, device_id=dev, device_id_type=MESH
        )

    barrier = pltpu.get_barrier_semaphore()
    for dev in [dev_p, dev_y, dev_x] + [(zz, c, t) for zz in zo]:
        pl.semaphore_signal(barrier, inc=1, device_id=dev, device_id_type=MESH)
    pl.semaphore_wait(barrier, 2 + zs_n)

    def mod_copy(d, to, frm):
        return rc(modin_ref.at[to], modr.at[frm], m_s.at[d], m_r.at[frm], (to, c, t))

    for d, zz in enumerate(zo):
        mod_copy(d, zz, z).start()

    shards = (sa_ref, su_ref, sd_ref)
    z_far = z + 2 - 4 * (z // 2)
    z_end = 3 * (z // 2)
    is_mid = (z == 1) | (z == 2)

    def w_rows(zz):
        return rows_at(288 * zz, 288)

    def w_send(layer, m, slot, zz):
        i = 3 * layer + m
        return rc(
            shards[m].at[layer], w.at[i, w_rows(z)], wz_s.at[i, slot], wz_r.at[i, z], (zz, c, t)
        )

    def w_local(layer, m):
        i = 3 * layer + m
        return pltpu.make_async_copy(shards[m].at[layer], w.at[i, w_rows(z)], w_l.at[i])

    def w0(layer, m):
        w_local(layer, m).start()
        w_send(layer, m, 0, z_far).start()

        @pl.when(z < zs_n - 1)
        def _():
            w_send(layer, m, 1, z + 1).start()

        @pl.when(z > 0)
        def _():
            w_send(layer, m, 2, z - 1).start()

    def w_take(i, zz):
        part = w.at[i, w_rows(zz)]
        return rc(part, part, wz_s.at[i, 3], wz_r.at[i, zz], (z_end, c, t))

    def relay(i):
        @pl.when(is_mid)
        def _():
            w_take(i, z_far).wait_recv()
            w_take(i, z_far).start()

    def w2(i):
        for zz in zo:

            @pl.when(jnp.logical_not(is_mid & (zz == z_far)))
            def _():
                w_take(i, zz).wait_recv()

        part = w.at[i, w_rows(z)]
        pltpu.make_async_copy(part, part, w_l.at[i]).wait()

    def w_drain(layer, m):
        w_send(layer, m, 0, z_far).wait_send()

        @pl.when(z < zs_n - 1)
        def _():
            w_send(layer, m, 1, z + 1).wait_send()

        @pl.when(z > 0)
        def _():
            w_send(layer, m, 2, z - 1).wait_send()

        @pl.when(is_mid)
        def _():
            w_take(3 * layer + m, z_far).wait_send()

    for layer in range(LAYERS):
        for m in range(3):
            w0(layer, m)

    modr[z] = modin_ref[z]
    for zz in zo:
        mod_copy(0, zz, zz).wait_recv()
    for d in range(zs_n - 1):
        mod_copy(d, zo[d], z).wait_send()
    for layer in range(LAYERS):
        for zz in range(zs_n):
            modv[layer, 0:6, 288 * zz : 288 * (zz + 1)] = modr[zz, 8 * layer : 8 * layer + 6, 0:288]

    def mrow(layer, kind):
        return modv[layer, kind : kind + 1, :]

    def ap_copy(buf, phase, layer, index, block, offset, size, dev):
        part = buf.at[rows_at(128 * block + offset, size)]
        return rc(part, part, ap_s.at[phase, layer, index], ap_r.at[phase, layer, index], dev)

    def ap_parts(buf, phase, layer):
        b_own, b_p = 4 * c + t, 4 * c + tp
        b_y, b_yp = 4 * c + t_far, 4 * c + tp_far
        b_x, b_xp = 4 * (1 - c) + t, 4 * (1 - c) + tp
        b_d, b_dp = 4 * (1 - c) + t_far, 4 * (1 - c) + tp_far
        sends = [
            (0, b_own, 0, 128, dev_p),
            (1, b_own, 0, 64, dev_y),
            (4, b_own, 64, 64, dev_x),
            (2, b_own, 64, 64, dev_y),
            (3, b_own, 0, 64, dev_x),
            (5, b_y, 0, 64, dev_x),
            (6, b_x, 64, 64, dev_y),
            (7, b_y, 0, 64, dev_p),
            (8, b_y, 64, 64, dev_p),
            (9, b_x, 0, 64, dev_p),
            (10, b_x, 64, 64, dev_p),
            (11, b_d, 0, 64, dev_p),
            (12, b_d, 64, 64, dev_p),
        ]
        recvs = {
            0: (b_p, 0, 128),
            1: (b_y, 0, 64),
            2: (b_y, 64, 64),
            3: (b_x, 0, 64),
            4: (b_x, 64, 64),
            5: (b_d, 0, 64),
            6: (b_d, 64, 64),
            7: (b_yp, 0, 64),
            8: (b_yp, 64, 64),
            9: (b_xp, 0, 64),
            10: (b_xp, 64, 64),
            11: (b_dp, 0, 64),
            12: (b_dp, 64, 64),
        }

        def send(index):
            for entry in sends:
                if entry[0] == index:
                    ap_copy(buf, phase, layer, *entry).start()

        def wait(index):
            ap_copy(buf, phase, layer, index, *recvs[index], dev_p).wait_recv()

        def drain():
            for entry in sends:
                ap_copy(buf, phase, layer, *entry).wait_send()

        return send, wait, drain

    def gather_plane(buf, phase, layer, compute):
        send, wait, drain = ap_parts(buf, phase, layer)
        for index in (0, 1, 4, 2, 3):
            send(index)

        def step(i, carry):
            b0, b1, b2 = lax.rem(i, 2), lax.rem(i // 2, 2), i // 4

            @pl.when(i == 1)
            def _():
                wait(0)

            @pl.when(i == 2)
            def _():
                wait(1)
                send(5)
                send(7)
                wait(4)
                send(6)
                send(10)
                wait(2)
                send(8)
                wait(3)
                send(9)

            @pl.when(i == 3)
            def _():
                wait(7)
                wait(8)

            @pl.when(i == 5)
            def _():
                wait(9)
                wait(10)

            @pl.when(i == 6)
            def _():
                wait(5)
                send(11)
                wait(6)
                send(12)

            @pl.when(i == 7)
            def _():
                wait(11)
                wait(12)

            block = (
                4 * lax.rem(c + b2, 2) + 2 * lax.rem(y + b1, 2) + lax.rem(k + b0, 2)
            )
            compute(block)
            return carry

        lax.fori_loop(0, 8, step, 0)
        drain()

    def pool_rows(i):
        return rows_at(128 * i, 128)

    def reduce_plane(phase, layer, compute, beside):
        def to_p(i, slot):
            return rc(
                pool.at[pool_rows(i)],
                ra.at[slot],
                rp_s.at[phase, layer, slot],
                rp_r.at[phase, layer, slot],
                dev_p,
            )

        d_x = rc(dsend.at[0:64], drecv.at[0:64], rp_s.at[phase, layer, 4], rp_r.at[phase, layer, 4], dev_x)
        d_y = rc(dsend.at[64:128], drecv.at[64:128], rp_s.at[phase, layer, 5], rp_r.at[phase, layer, 5], dev_y)
        to_x = rc(xsend, xrecv, rp_s.at[phase, layer, 6], rp_r.at[phase, layer, 6], dev_x)
        to_y = rc(ysend, yrecv, rp_s.at[phase, layer, 7], rp_r.at[phase, layer, 7], dev_y)

        def step(i, carry):
            q = i // 2
            b0, b1, b2 = 1 - lax.rem(i, 2), 1 - lax.rem(q, 2), 1 - q // 2
            block = (
                4 * lax.rem(c + b2, 2) + 2 * lax.rem(y + b1, 2) + lax.rem(k + b0, 2)
            )
            pool[pool_rows(i), :] = compute(block)

            @pl.when(b0 == 1)
            def _():
                to_p(i, q).start()

            @pl.when(i == 1)
            def _():
                to_p(0, 0).wait_recv()

                def add(r, inner):
                    rr = rows_at(16 * r, 16)
                    dsend[rr, :] = (pool[rows_at(128 + 16 * r, 16), :] + ra[0, rr, :]).astype(BF16)
                    return inner

                lax.fori_loop(0, 8, add, 0)
                d_x.start()
                d_y.start()

            @pl.when(i == 3)
            def _():
                to_p(2, 1).wait_recv()
                d_y.wait_recv()

                def add(r, inner):
                    rr = rows_at(16 * r, 16)
                    rh = rows_at(64 + 16 * r, 16)
                    xsend[rr, :] = (pool[rows_at(384 + 16 * r, 16), :] + ra[1, rr, :]).astype(BF16)
                    xsend[rh, :] = (
                        pool[rows_at(448 + 16 * r, 16), :] + ra[1, rh, :] + drecv[rh, :].astype(F32)
                    ).astype(BF16)
                    return inner

                lax.fori_loop(0, 4, add, 0)
                to_x.start()

            @pl.when(i == 5)
            def _():
                to_p(4, 2).wait_recv()
                d_x.wait_recv()

                def add(r, inner):
                    rr = rows_at(16 * r, 16)
                    rh = rows_at(64 + 16 * r, 16)
                    ysend[rr, :] = (
                        pool[rows_at(640 + 16 * r, 16), :] + ra[2, rr, :] + drecv[rr, :].astype(F32)
                    ).astype(BF16)
                    ysend[rh, :] = (pool[rows_at(704 + 16 * r, 16), :] + ra[2, rh, :]).astype(BF16)
                    return inner

                lax.fori_loop(0, 4, add, 0)
                to_y.start()

            return carry

        lax.fori_loop(0, 8, step, 0)
        beside()
        to_p(6, 3).wait_recv()
        to_x.wait_recv()
        to_y.wait_recv()
        for q in range(4):
            to_p(2 * q, q).wait_send()
        for copy in (d_x, d_y, to_x, to_y):
            copy.wait_send()

        def total(rr, r):
            return (
                pool[rows_at(896 + 16 * r, 16), :]
                + ra[3, rr, :]
                + xrecv[rr, :].astype(F32)
                + yrecv[rr, :].astype(F32)
            )

        return total

    def spread(column):
        return jnp.broadcast_to(column, (column.shape[0], 128))

    def layer_norm(v):
        center = v - jnp.mean(v, axis=-1, keepdims=True)
        r = lax.rsqrt(jnp.mean(center * center, axis=-1, keepdims=True) + epsilon)
        return center * r, r

    def head_mask(lo):
        lane = lax.broadcasted_iota(jnp.int32, (512, 256), 1)
        return (lane >= lo) & (lane < lo + HD)

    own_block = 4 * c + t

    def own_rows(r):
        return rows_at(128 * own_block + 16 * r, 16)

    def cols128(b):
        return pl.ds(pl.multiple_of(128 * b, 128), 128)

    def forward(layer, carry):
        ia, iu, id_ = 3 * layer, 3 * layer + 1, 3 * layer + 2

        def ln1(r, inner):
            rr = rows_at(16 * r, 16)
            n, iv = layer_norm(hb[rr, :])
            own[layer, 0, rr, :] = n
            inv[layer, 0, rr, :] = spread(iv)
            mixed[layer, own_rows(r), :] = (n * (1.0 + mrow(layer, 1)) + mrow(layer, 0)).astype(
                BF16
            )
            return inner

        lax.fori_loop(0, 8, ln1, 0)

        def project(block):
            rr = pool_rows(block)
            qkv[layer, rr, :] = (
                nn(mixed[layer, rr, :], w[ia, :, 0:512]) + bias_ref[layer, 0:1, 0:512]
            ).astype(BF16)

        @pl.when(layer == 0)
        def _():
            relay(0)
            gather_plane(mixed.at[layer], 0, layer, lambda block: None)
            w2(0)

            def one(block, inner):
                project(block)
                return inner

            lax.fori_loop(0, 8, one, 0)

        @pl.when(layer > 0)
        def _():
            w2(ia)
            gather_plane(mixed.at[layer], 0, layer, project)

        def take_q(b, inner):
            rr = pool_rows(b)
            v = qkv[layer, rr, 256:512].astype(F32)
            qa[layer, rr, :] = pltpu.roll(v, 224, 1).astype(BF16)
            return inner

        lax.fori_loop(0, 8, take_q, 0)
        ot[...] = jnp.zeros_like(ot)

        def head(j, inner):
            h = j // 2
            qh = j - 2 * h
            q_rows = rows_at(512 * qh, 512)
            q_cols = pl.ds(pl.multiple_of(512 * qh, 512), 512)
            qm = jnp.where(head_mask(72 * h), qa[layer, q_rows, :].astype(F32), 0.0)
            pb[0:512, 0:256] = qm.astype(BF16)

            def scores(kb, m8):
                rr = rows_at(256 * kb, 256)
                s = nt(qkv[layer, rr, 0:256], pb[0:512, 0:256]) * scale
                pool[rr, 0:512] = s
                return jnp.maximum(m8, jnp.max(s.reshape(32, 8, 512), axis=0))

            m8 = lax.fori_loop(0, 4, scores, jnp.full((8, 512), -jnp.inf, F32))
            mx = jnp.max(m8, axis=0, keepdims=True)

            def exps(kb, l8):
                rr = rows_at(128 * kb, 128)
                e = jnp.exp(pool[rr, 0:512] - mx)
                pool[rr, 0:512] = e
                return l8 + fold(e)

            l8 = lax.fori_loop(0, 8, exps, jnp.zeros((8, 512), F32))
            row_sum = jnp.sum(l8, axis=0, keepdims=True)
            lse[layer, j, 0:1, :] = mx + jnp.log(row_sum)
            inverse = 1.0 / row_sum

            def probs(kb, inner2):
                rr = rows_at(128 * kb, 128)
                pb[rows_at(512 + 128 * kb, 128), :] = (pool[rr, 0:512] * inverse).astype(BF16)
                return inner2

            lax.fori_loop(0, 8, probs, 0)
            otw[...] = tn(qkv[layer, :, 128:384], pb[512:1536, :])
            ot[pl.ds(pl.multiple_of(48 + 72 * h, 8), 72), q_cols] = otw[
                pl.ds(pl.multiple_of(16 + 72 * h, 8), 72), :
            ]
            return inner

        lax.fori_loop(0, 4, head, 0)

        def put_att(b, inner):
            att[layer, pool_rows(b), :] = ot[:, cols128(b)].T.astype(BF16)
            return inner

        lax.fori_loop(0, 8, put_att, 0)
        relay(iu)

        def branch(b):
            return nt(att[layer, pool_rows(b), :], w[ia, :, 384:640])

        total1 = reduce_plane(0, layer, branch, lambda: relay(id_))

        def ln2(r, inner):
            rr = rows_at(16 * r, 16)
            br = total1(rr, r) + bias_ref[layer, 1:2, :]
            own[layer, 2, rr, :] = br
            v = hb[rr, :] + mrow(layer, 2) * br
            af[rr, :] = v
            n, iv = layer_norm(v)
            own[layer, 1, rr, :] = n
            inv[layer, 1, rr, :] = spread(iv)
            ffall[layer, own_rows(r), :] = (n * (1.0 + mrow(layer, 4)) + mrow(layer, 3)).astype(
                BF16
            )
            return inner

        lax.fori_loop(0, 8, ln2, 0)
        w2(iu)

        def up(b):
            rr = pool_rows(b)
            pre[layer, rr, :] = nn(ffall[layer, rr, :], w[iu]) + bias_ref[layer, 2:3, 0:640]

            def gelu(r, inner):
                r2 = rows_at(128 * b + 16 * r, 16)
                act[r2, :] = jax.nn.gelu(pre[layer, r2, :], approximate=True).astype(BF16)
                return inner

            lax.fori_loop(0, 8, gelu, 0)

        gather_plane(ffall.at[layer], 1, layer, up)
        w2(id_)

        def down(b):
            return nt(act[pool_rows(b), :], w[id_])

        def beside():
            @pl.when(layer < LAYERS - 1)
            def _():
                relay(id_ + 1)

        total2 = reduce_plane(1, layer, down, beside)

        def finish(r, inner):
            rr = rows_at(16 * r, 16)
            fo = total2(rr, r) + bias_ref[layer, 3:4, :]
            own[layer, 3, rr, :] = fo
            hb[rr, :] = af[rr, :] + mrow(layer, 5) * fo
            return inner

        lax.fori_loop(0, 8, finish, 0)
        return carry

    hb[...] = x_ref[...].astype(F32)
    lax.fori_loop(0, LAYERS, forward, 0)
    out_ref[...] = hb[...].astype(BF16)
    for layer in range(LAYERS):
        for m in range(3):
            w_drain(layer, m)
    hb[...] = cot_ref[...].astype(F32)

    def g_copy(i, d, zz):
        return rc(w.at[i, w_rows(zz)], rz.at[i, d], gz_s.at[i, d], gz_r.at[i, d], (zz, c, t))

    def g0(i):
        for d, zz in enumerate(zo):
            g_copy(i, d, zz).start()

    def g_send(i):
        return rc(w.at[i, w_rows(z)], gw_ref.at[i, c], gf_s.at[i], gf_r.at[i], dev_x)

    def g_keep(i):
        return pltpu.make_async_copy(w.at[i, w_rows(z)], gw_ref.at[i, c], g_l.at[i])

    def g2(i):
        for d, zz in enumerate(zo):
            rc(rz.at[i, d], rz.at[i, d], gz_s.at[i, d], gz_r.at[i, d], dev_x).wait_recv()

        def add(r, inner):
            rr = rows_at(288 * z + 16 * r, 16)
            total = w[i, rr, :].astype(F32)
            for d in range(zs_n - 1):
                total = total + rz[i, d, rows_at(16 * r, 16), :].astype(F32)
            w[i, rr, :] = total.astype(BF16)
            return inner

        lax.fori_loop(0, 18, add, 0)
        g_send(i).start()
        g_keep(i).start()

    def g3(i):
        other = gw_ref.at[i, 1 - c]
        rc(other, other, gf_s.at[i], gf_r.at[i], dev_x).wait_recv()
        g_send(i).wait_send()
        g_keep(i).wait()
        for d, zz in enumerate(zo):
            g_copy(i, d, zz).wait_send()

    def small():
        for index, size, dev in ((0, 8, dev_p), (1, 8, dev_y), (2, 16, dev_x)):
            step = rc(
                sm.at[:, 0:size],
                smr.at[index, :, 0:size],
                sm_s.at[index],
                sm_r.at[index],
                dev,
            )
            step.start()
            step.wait_send()
            step.wait_recv()
            sm[:, 0:size, :] = sm[:, 0:size, :] + smr[index, :, 0:size, :]
        small_ref[z] = sm[...]
        for d, zz in enumerate(zo):
            rc(sm, small_ref.at[z], sm_s.at[3 + d], sm_r.at[3 + z], (zz, c, t)).start()

    def small_end():
        for d, zz in enumerate(zo):
            end = rc(sm, small_ref.at[zz], sm_s.at[3 + d], sm_r.at[3 + zz], (zz, c, t))
            end.wait_recv()
            end.wait_send()

    zero8 = jnp.zeros((8, D), F32)

    def put_sum(layer, row, v8):
        sm[layer, row : row + 1, 0 : v8.shape[1]] = jnp.sum(v8, axis=0, keepdims=True)

    def add_sum(layer, row, v8):
        here = (layer, pl.ds(row, 1), slice(0, v8.shape[1]))
        sm[here] = sm[here] + jnp.sum(v8, axis=0, keepdims=True)

    def backward(step_index, carry):
        layer = LAYERS - 1 - step_index
        ia, iu, id_ = 3 * layer, 3 * layer + 1, 3 * layer + 2

        def start(r, sums):
            rr = rows_at(16 * r, 16)
            g = hb[rr, :]
            gf = (mrow(layer, 5) * g).astype(BF16)
            gff[own_rows(r), :] = gf
            return (sums[0] + fold(g * own[layer, 3, rr, :]), sums[1] + fold(gf.astype(F32)))

        s_gate2, s_bdown = lax.fori_loop(0, 8, start, (zero8, zero8))
        put_sum(layer, 5, s_gate2)
        put_sum(layer, 7, s_bdown)

        def act_back(b):
            rr = pool_rows(b)
            pool[rows_at(512, 128), 0:640] = nn(gff[rr, :], w[id_])

            def one(r, total):
                r2 = rows_at(128 * b + 16 * r, 16)
                v = pre[layer, r2, :]
                th = jnp.tanh(0.7978845608028654 * (v + 0.044715 * (v * v * v)))
                act[r2, :] = (0.5 * v * (1.0 + th)).astype(BF16)
                slope = 0.5 * (1.0 + th) + 0.5 * v * (1.0 - th * th) * (
                    0.7978845608028654 * (1.0 + 0.134145 * (v * v))
                )
                gp = (pool[rows_at(512 + 16 * r, 16), 0:640] * slope).astype(BF16)
                gpre[r2, :] = gp
                return total + fold(gp.astype(F32))

            add_sum(layer, 10 + c, lax.fori_loop(0, 8, one, jnp.zeros((8, 640), F32)))

        gather_plane(gff, 2, layer, act_back)

        def ffin_back(b):
            return nt(gpre[pool_rows(b), :], w[iu])

        def beside1():
            def one_d(i, inner):
                w[id_, rows_at(128 * i, 128), :] = tn(gff[:, cols128(i)], act[...]).astype(BF16)
                return inner

            lax.fori_loop(0, 9, one_d, 0)
            g0(id_)

            def one_u(i, inner):
                w[iu, rows_at(128 * i, 128), :] = tn(ffall[layer, :, cols128(i)], gpre[...]).astype(
                    BF16
                )
                return inner

            lax.fori_loop(0, 9, one_u, 0)
            g0(iu)

        total1 = reduce_plane(2, layer, ffin_back, beside1)

        def mid(r, sums):
            rr = rows_at(16 * r, 16)
            gf = total1(rr, r)
            n = own[layer, 1, rr, :]
            e = gf * (1.0 + mrow(layer, 4))
            iv = inv[layer, 1, rr, 0:1]
            ga = hb[rr, :] + iv * (
                e
                - jnp.mean(e, axis=-1, keepdims=True)
                - n * jnp.mean(e * n, axis=-1, keepdims=True)
            )
            hb[rr, :] = ga
            gbv = (mrow(layer, 2) * ga).astype(BF16)
            gb[own_rows(r), :] = gbv
            return (
                sums[0] + fold(gf),
                sums[1] + fold(gf * n),
                sums[2] + fold(ga * own[layer, 2, rr, :]),
                sums[3] + fold(gbv.astype(F32)),
            )

        s_shift2, s_scale2, s_gate1, s_bproj = lax.fori_loop(
            0, 8, mid, (zero8, zero8, zero8, zero8)
        )
        put_sum(layer, 3, s_shift2)
        put_sum(layer, 4, s_scale2)
        put_sum(layer, 2, s_gate1)
        put_sum(layer, 6, s_bproj)

        def att_back(b):
            rr = pool_rows(b)
            doa[rr, :] = pltpu.roll(nn(gb[rr, :], w[ia, :, 384:640]), 224, 1).astype(BF16)

        gather_plane(gb, 3, layer, att_back)
        dkv[...] = jnp.zeros_like(dkv)
        ot[...] = jnp.zeros_like(ot)

        def head(j, inner):
            h = j // 2
            qh = j - 2 * h
            q_rows = rows_at(512 * qh, 512)
            q_cols = pl.ds(pl.multiple_of(512 * qh, 512), 512)
            qm = jnp.where(head_mask(72 * h), qa[layer, q_rows, :].astype(F32), 0.0)
            dm = jnp.where(head_mask(16 + 72 * h), doa[q_rows, :].astype(F32), 0.0)
            pb[0:512, 0:256] = qm.astype(BF16)
            pb[0:512, 256:512] = dm.astype(BF16)
            log_row = lse[layer, j, 0:1, :]

            def first(kb, d8):
                rr = rows_at(256 * kb, 256)
                s = nt(qkv[layer, rr, 0:256], pb[0:512, 0:256]) * scale
                pr = jnp.exp(s - log_row)
                dp = nt(qkv[layer, rr, 128:384], pb[0:512, 256:512])
                pool[rr, 0:512] = pr
                pool[rr, 512:1024] = dp
                dkv[rr, 128:384] = dkv[rr, 128:384] + nn(pr.astype(BF16), pb[0:512, 256:512])
                return d8 + fold(pr * dp)

            d8 = lax.fori_loop(0, 4, first, jnp.zeros((8, 512), F32))
            delta = jnp.sum(d8, axis=0, keepdims=True)

            def second(kb, inner2):
                rr = rows_at(256 * kb, 256)
                ds = (pool[rr, 0:512] * (pool[rr, 512:1024] - delta)).astype(BF16)
                pb[rows_at(512 + 256 * kb, 256), :] = ds
                dkv[rr, 0:256] = dkv[rr, 0:256] + nn(ds, pb[0:512, 0:256]) * scale
                return inner2

            lax.fori_loop(0, 4, second, 0)
            otw[...] = tn(qkv[layer, :, 0:256], pb[512:1536, :]) * scale
            ot[pl.ds(pl.multiple_of(32 + 72 * h, 8), 72), q_cols] = otw[
                pl.ds(pl.multiple_of(72 * h, 8), 72), :
            ]
            return inner

        lax.fori_loop(0, 4, head, 0)

        def put(b, total):
            rr = pool_rows(b)
            dq = ot[:, cols128(b)].T
            kv = dkv[rr, :]
            both = jnp.concatenate(
                (kv[:, 0:256], kv[:, 256:384] + dq[:, 0:128], dq[:, 128:256]), axis=1
            ).astype(BF16)
            dqkv[rr, :] = both
            return total + fold(both.astype(F32))

        add_sum(layer, 8 + c, lax.fori_loop(0, 8, put, jnp.zeros((8, 512), F32)))

        @pl.when(layer == 0)
        def _():
            g2(5)
            g2(4)

        def mix_back(block):
            return nt(dqkv[pool_rows(block), :], w[ia, :, 0:512])

        def beside2():
            def one(i, inner):
                rr = rows_at(128 * i, 128)
                r1 = tn(mixed[layer, :, cols128(i)], dqkv[...])
                r3 = tn(gb[:, cols128(i)], att[layer])
                w[ia, rr, 0:384] = r1[:, 0:384].astype(BF16)
                w[ia, rr, 384:512] = (r1[:, 384:512] + r3[:, 0:128]).astype(BF16)
                w[ia, rr, 512:640] = r3[:, 128:256].astype(BF16)
                return inner

            lax.fori_loop(0, 9, one, 0)
            g0(ia)

        total2 = reduce_plane(3, layer, mix_back, beside2)

        def last(r, sums):
            rr = rows_at(16 * r, 16)
            gm = total2(rr, r)
            n = own[layer, 0, rr, :]
            e = gm * (1.0 + mrow(layer, 1))
            iv = inv[layer, 0, rr, 0:1]
            hb[rr, :] = hb[rr, :] + iv * (
                e
                - jnp.mean(e, axis=-1, keepdims=True)
                - n * jnp.mean(e * n, axis=-1, keepdims=True)
            )
            return (sums[0] + fold(gm), sums[1] + fold(gm * n))

        s_shift1, s_scale1 = lax.fori_loop(0, 8, last, (zero8, zero8))
        put_sum(layer, 0, s_shift1)
        put_sum(layer, 1, s_scale1)
        return carry

    sm[...] = jnp.zeros_like(sm)
    lax.fori_loop(0, LAYERS, backward, 0)
    small()
    g2(3)
    g2(2)
    g2(1)
    small_end()
    g2(0)
    for i in range(6):
        g3(i)


def sum_kernel(zs_n, part_ref, out_ref, got, send_sem, recv_sem):
    z = lax.axis_index("shard")
    c = lax.axis_index("context")
    t = lax.axis_index("tensor")
    others = [lax.rem(z + d, zs_n) for d in range(1, zs_n)]
    barrier = pltpu.get_barrier_semaphore()
    for zz in others:
        pl.semaphore_signal(barrier, inc=1, device_id=(zz, c, t), device_id_type=MESH)
    pl.semaphore_wait(barrier, zs_n - 1)

    def copy(d, slot, zz):
        return pltpu.make_async_remote_copy(
            src_ref=part_ref,
            dst_ref=got.at[slot],
            send_sem=send_sem.at[d],
            recv_sem=recv_sem.at[slot],
            device_id=(zz, c, t),
            device_id_type=MESH,
        )

    for d, zz in enumerate(others):
        copy(d, z, zz).start()
    got[z] = part_ref[...]
    for d, zz in enumerate(others):
        copy(d, zz, zz).wait_recv()
        copy(d, z, zz).wait_send()
    total = got[0]
    for zz in range(1, zs_n):
        total = total + got[zz]
    out_ref[...] = total


def sum_shards(zs_n, part):
    vm = pl.BlockSpec(memory_space=pltpu.VMEM)
    dma = pltpu.SemaphoreType.DMA
    return pl.pallas_call(
        functools.partial(sum_kernel, zs_n),
        name="sum_shards",
        out_shape=jax.ShapeDtypeStruct(part.shape, F32),
        in_specs=[vm],
        out_specs=vm,
        scratch_shapes=[
            pltpu.VMEM((zs_n,) + part.shape, F32),
            dma((zs_n - 1,)),
            dma((zs_n,)),
        ],
        compiler_params=pltpu.CompilerParams(collective_id=1, has_side_effects=True),
    )(part)


def run_stage(zs_n, x_in, cot, modin, bias, block_a, block_u, block_d):
    vm = pl.BlockSpec(memory_space=pltpu.VMEM)
    anyspace = pl.BlockSpec(memory_space=pl.ANY)
    dma = pltpu.SemaphoreType.DMA
    sds = jax.ShapeDtypeStruct
    scratch = [
        pltpu.VMEM((6, D, 640), BF16),
        pltpu.VMEM((2, 1024, D), BF16),
        pltpu.VMEM((2, 1024, 512), BF16),
        pltpu.VMEM((2, 1024, 256), BF16),
        pltpu.VMEM((2, 1024, 256), BF16),
        pltpu.VMEM((2, 1024, D), BF16),
        pltpu.VMEM((2, 1024, 640), F32),
        pltpu.VMEM((1024, 640), BF16),
        pltpu.VMEM((2, 4, 128, D), F32),
        pltpu.VMEM((2, 2, 128, 128), F32),
        pltpu.VMEM((2, 4, 8, 512), F32),
        pltpu.VMEM((zs_n, 16, 384), F32),
        pltpu.VMEM((2, 8, D), F32),
        pltpu.VMEM((128, D), F32),
        pltpu.VMEM((1024, D), F32),
        pltpu.VMEM((4, 128, D), F32),
        pltpu.VMEM((128, D), BF16),
        pltpu.VMEM((128, D), BF16),
        pltpu.VMEM((128, D), BF16),
        pltpu.VMEM((128, D), BF16),
        pltpu.VMEM((128, D), BF16),
        pltpu.VMEM((128, D), BF16),
        pltpu.VMEM((1024, D), BF16),
        pltpu.VMEM((1024, 640), BF16),
        pltpu.VMEM((1024, D), BF16),
        pltpu.VMEM((1024, 256), BF16),
        pltpu.VMEM((1024, 512), BF16),
        pltpu.VMEM((1024, 384), F32),
        pltpu.VMEM((1536, 512), BF16),
        pltpu.VMEM((256, 512), F32),
        pltpu.VMEM((256, 1024), F32),
        pltpu.VMEM((6, zs_n - 1, 288, 640), BF16),
        pltpu.VMEM((2, 16, D), F32),
        pltpu.VMEM((3, 2, 16, D), F32),
        dma((zs_n - 1,)),
        dma((zs_n,)),
        dma((6, 4)),
        dma((6, zs_n)),
        dma((6,)),
        dma((4, 2, 13)),
        dma((4, 2, 13)),
        dma((4, 2, 8)),
        dma((4, 2, 8)),
        dma((6, zs_n)),
        dma((6, zs_n)),
        dma((6,)),
        dma((6,)),
        dma((6,)),
        dma((3 + zs_n,)),
        dma((3 + zs_n,)),
    ]
    return pl.pallas_call(
        functools.partial(stage_kernel, zs_n),
        name="two_blocks",
        out_shape=(
            sds((128, D), BF16),
            sds((128, D), F32),
            sds((6, 2, 288, 640), BF16),
            sds((zs_n, 2, 16, D), F32),
        ),
        in_specs=[vm, vm, vm, vm, anyspace, anyspace, anyspace],
        out_specs=(vm, vm, anyspace, vm),
        scratch_shapes=scratch,
        compiler_params=pltpu.CompilerParams(
            collective_id=0, has_side_effects=True, vmem_limit_bytes=67043328
        ),
    )(x_in, cot, modin, bias, block_a, block_u, block_d)


def fast_body(
    zs_n,
    x_in,
    cond,
    w_ada,
    b_ada,
    w_qkv,
    b_qv,
    w_proj,
    b_proj,
    up_weight,
    up_bias_vector,
    down_weight,
    down_bias_vector,
    cotangent,
):
    z = lax.axis_index("shard")
    c = lax.axis_index("context")
    cols = w_ada.shape[3]
    part = w_qkv.shape[3] // 2
    units = up_weight.shape[2] // 2
    cond_low = jax.nn.silu(cond).astype(BF16)
    mod_terms = (
        jnp.einsum("sd,ldkc->lskc", cond_low, w_ada, preferred_element_type=F32)
        + b_ada.astype(F32)[:, None]
    ).astype(BF16)
    modin = jnp.pad(
        mod_terms.astype(F32).transpose(1, 0, 2, 3), ((0, 0), (0, 0), (0, 2), (0, 384 - cols))
    ).reshape(zs_n, 16, 384)

    def mine(array, size, axis):
        return lax.dynamic_slice_in_dim(array, c * size, size, axis)

    def wide(array, size):
        return jnp.pad(array, ((0, 0),) * (array.ndim - 1) + ((0, size - array.shape[-1]),))

    heads = mine(w_qkv, part, 3)
    block_a = wide(
        jnp.concatenate(
            (
                heads[:, 1],
                heads[:, 2],
                heads[:, 0],
                mine(w_proj, part, 1).transpose(0, 2, 1),
            ),
            axis=2,
        ),
        640,
    )
    block_u = wide(mine(up_weight, units, 2), 640)
    block_d = wide(mine(down_weight, units, 1).transpose(0, 2, 1), 640)
    b_heads = mine(b_qv, part, 2).astype(F32)
    b_qkv = jnp.concatenate((jnp.zeros((LAYERS, part), F32), b_heads[:, 1], b_heads[:, 0]), axis=1)
    bias = jnp.stack(
        (
            wide(b_qkv, D),
            b_proj.astype(F32),
            wide(mine(up_bias_vector, units, 1).astype(F32), D),
            down_bias_vector.astype(F32),
        ),
        axis=1,
    )
    out, grad_in, gw, small = run_stage(
        zs_n, x_in[:, 0], cotangent[:, 0], modin, bias, block_a, block_u, block_d
    )
    grad_mod = small[:, :, 0:6, :].astype(BF16)
    mod_cols = lax.dynamic_slice_in_dim(grad_mod, z * cols, cols, 3)
    grad_w_ada = jnp.einsum("sd,slkc->ldkc", cond_low, mod_cols, preferred_element_type=F32)
    grad_b_ada = jnp.sum(mod_cols.astype(F32), axis=0)
    cond_part = jnp.einsum("slkc,ldkc->sd", mod_cols, w_ada, preferred_element_type=F32)
    cond_total = sum_shards(zs_n, cond_part)
    silu_value, silu_back = jax.vjp(jax.nn.silu, cond)
    grad_cond = silu_back(cond_total)[0]
    sums = jnp.sum(small[:, :, 6:12, :], axis=0)

    def halves(row, start, size):
        return jnp.concatenate(
            (sums[:, row, start : start + size], sums[:, row + 1, start : start + size]), axis=1
        )

    gw = gw.reshape(LAYERS, 3, 2, cols, 640)

    def both(m, start, size):
        return jnp.concatenate(
            (gw[:, m, 0, :, start : start + size], gw[:, m, 1, :, start : start + size]), axis=2
        ).astype(F32)

    return (
        out[:, None],
        grad_in[:, None],
        grad_cond,
        grad_w_ada,
        grad_b_ada,
        jnp.stack((both(0, 2 * part, part), both(0, 0, part), both(0, part, part)), axis=1),
        jnp.stack((halves(2, 2 * part, part), halves(2, part, part)), axis=1),
        both(0, 3 * part, part).transpose(0, 2, 1),
        sums[:, 0],
        both(1, 0, units),
        halves(4, 0, units),
        both(2, 0, units).transpose(0, 2, 1),
        sums[:, 1],
    )


def solution(mesh):
    shape = mesh.shape
    program = body
    if shape["context"] == 2 and shape["tensor"] == 4 and shape["shard"] == 4:
        program = functools.partial(fast_body, shape["shard"])
    return jax.shard_map(
        program,
        mesh=mesh,
        in_specs=(
            P(("context", "tensor"), "shard", None),
            P(),
            P(None, None, None, "shard"),
            P(None, None, "shard"),
            P(None, None, "shard", "tensor"),
            P(None, None, "tensor"),
            P(None, "tensor", "shard"),
            P(),
            P(None, "shard", "tensor"),
            P(None, "tensor"),
            P(None, "tensor", "shard"),
            P(),
            P(("context", "tensor"), "shard", None),
        ),
        out_specs=(
            P(("context", "tensor"), "shard", None),
            P(("context", "tensor"), "shard", None),
            P(),
            P(None, None, None, "shard"),
            P(None, None, "shard"),
            P(None, None, "shard", "tensor"),
            P(None, None, "tensor"),
            P(None, "tensor", "shard"),
            P(),
            P(None, "shard", "tensor"),
            P(None, "tensor"),
            P(None, "tensor", "shard"),
            P(),
        ),
        check_vma=False,
    )
```

```python
import functools

import jax
import jax.numpy as jnp
from jax import lax
from jax.experimental import pallas as pl
from jax.experimental.pallas import tpu as pltpu
from jax.sharding import PartitionSpec as P

D = 1152
HD = 72
FF = 4608
LAYERS = 2


epsilon = 1e-06


def normalize(values):
    center = values - jnp.mean(values, axis=-1, keepdims=True)
    inverse = lax.rsqrt(jnp.mean(center * center, axis=-1, keepdims=True) + epsilon)
    return (center * inverse, inverse)


def normalize_back(grad_normed, normed, inverse):
    mean_grad = jnp.mean(grad_normed, axis=-1, keepdims=True)
    mean_proj = jnp.mean(grad_normed * normed, axis=-1, keepdims=True)
    return inverse * (grad_normed - mean_grad - normed * mean_proj)


def gelu_tanh(values):
    return jax.nn.gelu(values, approximate=True)


def to_heads(tokens):
    return tokens.reshape(tokens.shape[0], tokens.shape[1], -1, HD).transpose(1, 2, 0, 3)


def from_heads(blocks):
    return blocks.transpose(2, 0, 1, 3).reshape(blocks.shape[2], blocks.shape[0], -1)


def over_heads(head_fn, arrays):
    return lax.map(lambda seq_items: lax.map(head_fn, seq_items), arrays)


def score_block(query_head, key_head):
    return jnp.einsum(
        "qe,ke->qk", query_head, key_head, preferred_element_type=jnp.float32
    ) * HD ** (-0.5)


def forward_head(head_parts):
    query_head, key_head, value_head = head_parts
    scores = score_block(query_head, key_head)
    maxima = jnp.max(scores, axis=-1, keepdims=True)
    exp_scores = jnp.exp(scores - maxima)
    row_total = jnp.sum(exp_scores, axis=-1, keepdims=True)
    prob_low = (exp_scores / row_total).astype(jnp.bfloat16)
    result = jnp.dot(prob_low, value_head, preferred_element_type=jnp.float32).astype(jnp.bfloat16)
    return (result, (maxima + jnp.log(row_total))[:, 0])


def full_grads(head_parts):
    query_head, key_head, value_head, grad_head, log_head = head_parts
    prob_full = jnp.exp(score_block(query_head, key_head) - log_head[:, None])
    grad_prob = jnp.einsum("qe,ke->qk", grad_head, value_head, preferred_element_type=jnp.float32)
    row_delta = jnp.sum(prob_full * grad_prob, axis=-1, keepdims=True)
    grad_score = (prob_full * (grad_prob - row_delta)).astype(jnp.bfloat16)
    grad_query = jnp.dot(grad_score, key_head, preferred_element_type=jnp.float32) * HD ** (-0.5)
    grad_key = jnp.einsum(
        "qk,qe->ke", grad_score, query_head, preferred_element_type=jnp.float32
    ) * HD ** (-0.5)
    grad_value = jnp.einsum(
        "qk,qe->ke", prob_full.astype(jnp.bfloat16), grad_head, preferred_element_type=jnp.float32
    )
    return (grad_query, grad_key, grad_value)


def fetch_weights(qkv_part, proj_part, up_part, down_part, mod_part):
    return (
        lax.all_gather(qkv_part, "shard", axis=2, tiled=True),
        lax.all_gather(proj_part, "shard", axis=2, tiled=True),
        lax.all_gather(up_part, "shard", axis=1, tiled=True),
        lax.all_gather(down_part, "shard", axis=2, tiled=True),
        lax.all_gather(mod_part, "shard", axis=3, tiled=True),
    )


def layer_forward(hidden_state, weights, modulation, biases):
    full_qkv, full_proj, full_up, full_down, mod_unused = weights
    bias_qv, bias_proj, bias_up, bias_down = biases
    normed1, inverse1 = normalize(hidden_state)
    mix_in = (normed1 * (1.0 + modulation[:, 1]) + modulation[:, 0]).astype(jnp.bfloat16)
    mixed_all = lax.all_gather(mix_in, "tensor", axis=0, tiled=True)
    projected = jnp.einsum("tbd,kde->tbke", mixed_all, full_qkv, preferred_element_type=jnp.float32)
    queries = (projected[:, :, 0] + bias_qv[0]).astype(jnp.bfloat16)
    keys_own = projected[:, :, 1].astype(jnp.bfloat16)
    values_own = (projected[:, :, 2] + bias_qv[1]).astype(jnp.bfloat16)
    keys_all, values_all = (
        lax.all_gather(keys_own, "context", axis=0, tiled=True),
        lax.all_gather(values_own, "context", axis=0, tiled=True),
    )
    head_out, log_sums = over_heads(
        forward_head, (to_heads(queries), to_heads(keys_all), to_heads(values_all))
    )
    attended = from_heads(head_out)
    row_block = attended
    branch = (
        lax.psum_scatter(
            jnp.einsum("tbe,ed->tbd", row_block, full_proj, preferred_element_type=jnp.float32),
            "tensor",
            scatter_dimension=0,
            tiled=True,
        )
        + bias_proj
    )
    after_attn = hidden_state + modulation[:, 2] * branch
    normed2, inverse2 = normalize(after_attn)
    feedforward_input = (normed2 * (1.0 + modulation[:, 4]) + modulation[:, 3]).astype(jnp.bfloat16)
    ff_all = lax.all_gather(feedforward_input, "tensor", axis=0, tiled=True)
    preactivation_value = (
        jnp.einsum("tbd,df->tbf", ff_all, full_up, preferred_element_type=jnp.float32) + bias_up
    )
    activation_value = gelu_tanh(preactivation_value).astype(jnp.bfloat16)
    row_block = activation_value
    feedforward_output = (
        lax.psum_scatter(
            jnp.einsum(
                "tbf,fd->tbd", row_block, full_down, preferred_element_type=jnp.float32
            ).astype(jnp.bfloat16),
            "tensor",
            scatter_dimension=0,
            tiled=True,
        ).astype(jnp.float32)
        + bias_down
    )
    result = after_attn + modulation[:, 5] * feedforward_output
    stash = (
        normed1,
        inverse1,
        mixed_all,
        queries,
        keys_all,
        values_all,
        attended,
        log_sums,
        branch,
        normed2,
        inverse2,
        ff_all,
        preactivation_value,
        activation_value,
        feedforward_output,
    )
    return (result, stash)


def layer_backward(grad_hidden, weights, modulation, stash):
    full_qkv, full_proj, full_up, full_down, mod_unused = weights
    (
        normed1,
        inverse1,
        mixed_all,
        queries,
        keys_all,
        values_all,
        attended,
        log_sums,
        branch,
        normed2,
        inverse2,
        ff_all,
        preactivation_value,
        activation_value,
        feedforward_output,
    ) = stash
    grad_ff = (modulation[:, 5] * grad_hidden).astype(jnp.bfloat16)
    grad_gate2 = jnp.sum(grad_hidden * feedforward_output, axis=0)
    bias_down = jnp.sum(grad_ff.astype(jnp.float32), axis=(0, 1))
    grad_ff_all = lax.all_gather(grad_ff, "tensor", axis=0, tiled=True)
    grad_w_down = jnp.einsum(
        "tbf,tbd->fd", activation_value, grad_ff_all, preferred_element_type=jnp.float32
    )
    grad_activ = jnp.einsum(
        "tbd,fd->tbf", grad_ff_all, full_down, preferred_element_type=jnp.float32
    )
    gelu_value, gelu_back = jax.vjp(gelu_tanh, preactivation_value)
    grad_pre = gelu_back(grad_activ)[0].astype(jnp.bfloat16)
    bias_up = jnp.sum(grad_pre.astype(jnp.float32), axis=(0, 1))
    grad_w_up = jnp.einsum("tbd,tbf->df", ff_all, grad_pre, preferred_element_type=jnp.float32)
    row_block = grad_pre
    grad_ffin = lax.psum_scatter(
        jnp.einsum("tbf,df->tbd", row_block, full_up, preferred_element_type=jnp.float32).astype(
            jnp.bfloat16
        ),
        "tensor",
        scatter_dimension=0,
        tiled=True,
    ).astype(jnp.float32)
    grad_shift2 = jnp.sum(grad_ffin, axis=0)
    grad_scale2 = jnp.sum(grad_ffin * normed2, axis=0)
    grad_after = grad_hidden + normalize_back(
        grad_ffin * (1.0 + modulation[:, 4]), normed2, inverse2
    )
    grad_branch = (modulation[:, 2] * grad_after).astype(jnp.bfloat16)
    grad_gate1 = jnp.sum(grad_after * branch, axis=0)
    bias_proj = jnp.sum(grad_branch.astype(jnp.float32), axis=(0, 1))
    grad_branch_all = lax.all_gather(grad_branch, "tensor", axis=0, tiled=True)
    grad_w_proj = jnp.einsum(
        "tbe,tbd->ed", attended, grad_branch_all, preferred_element_type=jnp.float32
    )
    grad_attended = jnp.einsum(
        "tbd,ed->tbe", grad_branch_all, full_proj, preferred_element_type=jnp.float32
    ).astype(jnp.bfloat16)
    head_inputs = (
        to_heads(queries),
        to_heads(keys_all),
        to_heads(values_all),
        to_heads(grad_attended),
        log_sums,
    )
    grad_q_heads, grad_k_heads, grad_v_heads = over_heads(full_grads, head_inputs)
    grad_queries = from_heads(grad_q_heads).astype(jnp.bfloat16)
    grad_keys, grad_values = (
        lax.psum_scatter(
            from_heads(grad_k_heads).astype(jnp.bfloat16),
            "context",
            scatter_dimension=0,
            tiled=True,
        ).astype(jnp.float32),
        lax.psum_scatter(
            from_heads(grad_v_heads).astype(jnp.bfloat16),
            "context",
            scatter_dimension=0,
            tiled=True,
        ).astype(jnp.float32),
    )
    grad_keys = grad_keys.astype(jnp.bfloat16)
    grad_values = grad_values.astype(jnp.bfloat16)
    grad_qkv = jnp.stack((grad_queries, grad_keys, grad_values), axis=2)
    bias_qv = jnp.stack(
        (
            jnp.sum(grad_queries.astype(jnp.float32), axis=(0, 1)),
            jnp.sum(grad_values.astype(jnp.float32), axis=(0, 1)),
        )
    )
    grad_w_qkv = jnp.einsum(
        "tbd,tbke->kde", mixed_all, grad_qkv, preferred_element_type=jnp.float32
    )
    row_block = grad_qkv
    grad_mixin = lax.psum_scatter(
        jnp.einsum("tbke,kde->tbd", row_block, full_qkv, preferred_element_type=jnp.float32).astype(
            jnp.bfloat16
        ),
        "tensor",
        scatter_dimension=0,
        tiled=True,
    ).astype(jnp.float32)
    grad_shift1 = jnp.sum(grad_mixin, axis=0)
    grad_scale1 = jnp.sum(grad_mixin * normed1, axis=0)
    grad_input = grad_after + normalize_back(
        grad_mixin * (1.0 + modulation[:, 1]), normed1, inverse1
    )
    grad_mod_own = jnp.stack(
        (grad_shift1, grad_scale1, grad_gate1, grad_shift2, grad_scale2, grad_gate2), axis=1
    )
    return (
        grad_input,
        (grad_w_qkv, grad_w_proj, grad_w_up, grad_w_down),
        (grad_mod_own, bias_qv, bias_proj, bias_up, bias_down),
    )


def body(
    x_in,
    cond,
    w_ada,
    b_ada,
    w_qkv,
    b_qv,
    w_proj,
    b_proj,
    up_weight,
    up_bias_vector,
    down_weight,
    down_bias_vector,
    cotangent,
):
    shard_index = lax.axis_index("shard")
    tensor_index = lax.axis_index("tensor")
    context_index = lax.axis_index("context")
    own_latents = x_in.shape[1]
    all_latents = cond.shape[0]
    shard_cols = w_ada.shape[3]
    head_cols = w_qkv.shape[3]
    hidden_cols = up_weight.shape[2]
    condition_reduced = jax.nn.silu(cond).astype(jnp.bfloat16)
    mod_terms = (
        jnp.einsum("sd,ldkc->lskc", condition_reduced, w_ada, preferred_element_type=jnp.float32)
        + b_ada.astype(jnp.float32)[:, None]
    ).astype(jnp.bfloat16)
    hidden_state = x_in.astype(jnp.float32)
    layer_state = []
    for layer_number_index in range(LAYERS):
        sliced = fetch_weights(
            w_qkv[layer_number_index : layer_number_index + 1],
            w_proj[layer_number_index : layer_number_index + 1],
            up_weight[layer_number_index : layer_number_index + 1],
            down_weight[layer_number_index : layer_number_index + 1],
            mod_terms[layer_number_index : layer_number_index + 1],
        )
        weights = tuple((member_entry[0] for member_entry in sliced))
        modulation = lax.dynamic_slice_in_dim(
            weights[4], shard_index * own_latents, own_latents, 0
        ).astype(jnp.float32)
        biases = (
            b_qv[layer_number_index].astype(jnp.float32),
            b_proj[layer_number_index].astype(jnp.float32),
            up_bias_vector[layer_number_index].astype(jnp.float32),
            down_bias_vector[layer_number_index].astype(jnp.float32),
        )
        hidden_state, stash = layer_forward(hidden_state, weights, modulation, biases)
        layer_state.append((weights, modulation, stash))
    output = hidden_state.astype(jnp.bfloat16)
    grad_hidden = cotangent.astype(jnp.float32)
    cond_total = jnp.zeros(cond.shape, jnp.float32)
    results = [None] * LAYERS
    context_mask = (context_index == 0).astype(jnp.float32)
    for layer_number_index in reversed(range(LAYERS)):
        weights, modulation, stash = layer_state[layer_number_index]
        grad_hidden, matrix_grads, small_terms = layer_backward(
            grad_hidden, weights, modulation, stash
        )
        grad_mod_own, bias_qv, bias_proj, bias_up, bias_down = small_terms
        grad_mod_pad = lax.dynamic_update_slice_in_dim(
            jnp.zeros((all_latents, 6, D), jnp.float32), grad_mod_own, shard_index * own_latents, 0
        )
        bias_qv_pad = lax.dynamic_update_slice_in_dim(
            jnp.zeros((2, D), jnp.float32), bias_qv, tensor_index * head_cols, 1
        )
        bias_up_pad = lax.dynamic_update_slice_in_dim(
            jnp.zeros((FF,), jnp.float32), bias_up, tensor_index * hidden_cols, 0
        )
        mod_sum, proj_sum, down_sum, qv_sum, up_sum = lax.psum(
            (grad_mod_pad, bias_proj, bias_down, bias_qv_pad, bias_up_pad),
            ("shard", "context", "tensor"),
        )
        mod_cols = lax.dynamic_slice_in_dim(
            mod_sum.astype(jnp.bfloat16), shard_index * shard_cols, shard_cols, 2
        )
        grad_w_ada = jnp.einsum(
            "sd,skc->dkc", condition_reduced, mod_cols, preferred_element_type=jnp.float32
        )
        grad_b_ada = jnp.sum(mod_cols.astype(jnp.float32), axis=0)
        cond_part = (
            jnp.einsum(
                "skc,dkc->sd",
                mod_cols,
                w_ada[layer_number_index],
                preferred_element_type=jnp.float32,
            )
            * context_mask
        )
        grad_w_qkv, grad_w_proj, grad_w_up, grad_w_down = matrix_grads
        qkv_all, proj_all, up_all, down_all, cond_sum = (
            lax.psum(grad_w_qkv.astype(jnp.bfloat16), ("shard", "context")).astype(jnp.float32),
            lax.psum(grad_w_proj.astype(jnp.bfloat16), ("shard", "context")).astype(jnp.float32),
            lax.psum(grad_w_up.astype(jnp.bfloat16), ("shard", "context")).astype(jnp.float32),
            lax.psum(grad_w_down.astype(jnp.bfloat16), ("shard", "context")).astype(jnp.float32),
            lax.psum(cond_part.astype(jnp.bfloat16), ("shard", "context")).astype(jnp.float32),
        )
        qkv_own = lax.dynamic_slice_in_dim(qkv_all, shard_index * shard_cols, shard_cols, 1)
        proj_own = lax.dynamic_slice_in_dim(proj_all, shard_index * shard_cols, shard_cols, 1)
        up_own = lax.dynamic_slice_in_dim(up_all, shard_index * shard_cols, shard_cols, 0)
        down_own = lax.dynamic_slice_in_dim(down_all, shard_index * shard_cols, shard_cols, 1)
        cond_total = cond_total + cond_sum
        results[layer_number_index] = (
            grad_w_ada,
            grad_b_ada,
            qkv_own,
            lax.dynamic_slice_in_dim(qv_sum, tensor_index * head_cols, head_cols, 1),
            proj_own,
            proj_sum,
            up_own,
            lax.dynamic_slice_in_dim(up_sum, tensor_index * hidden_cols, hidden_cols, 0),
            down_own,
            down_sum,
        )
    silu_value, silu_back = jax.vjp(jax.nn.silu, cond)
    grad_cond = silu_back(cond_total)[0]
    stacked = tuple(
        (
            jnp.stack(
                [results[layer_number_index][member_entry] for layer_number_index in range(LAYERS)]
            )
            for member_entry in range(10)
        )
    )
    return (
        output,
        grad_hidden,
        grad_cond,
        stacked[0],
        stacked[1],
        stacked[2],
        stacked[3],
        stacked[4],
        stacked[5],
        stacked[6],
        stacked[7],
        stacked[8],
        stacked[9],
    )


MESH = pl.DeviceIdType.MESH
F32 = jnp.float32
BF16 = jnp.bfloat16


def nt(a, b):
    return lax.dot_general(a, b, (((1,), (1,)), ((), ())), preferred_element_type=F32)


def nn(a, b):
    return jnp.dot(a, b, preferred_element_type=F32)


def tn(a, b):
    return lax.dot_general(a, b, (((0,), (0,)), ((), ())), preferred_element_type=F32)


def fold(v):
    return jnp.sum(v.reshape(v.shape[0] // 8, 8, v.shape[1]), axis=0)


def rows_at(start, size, multiple=16):
    return pl.ds(pl.multiple_of(start, multiple), size)


def stage_kernel(
    zs_n,
    x_ref,
    cot_ref,
    modin_ref,
    bias_ref,
    sa_ref,
    su_ref,
    sd_ref,
    out_ref,
    gin_ref,
    gw_ref,
    small_ref,
    w,
    mixed,
    qkv,
    qa,
    att,
    ffall,
    pre,
    act,
    own,
    inv,
    lse,
    modr,
    modv,
    af,
    pool,
    ra,
    ysend,
    yrecv,
    xsend,
    xrecv,
    dsend,
    drecv,
    gff,
    gpre,
    gb,
    doa,
    dqkv,
    dkv,
    pb,
    otw,
    ot,
    rz,
    rzr,
    sm,
    smr,
    m_s,
    m_r,
    wz_s,
    wz_r,
    w_l,
    ap_s,
    ap_r,
    rp_s,
    rp_r,
    gz_s,
    gz_r,
    gf_s,
    gf_r,
    g_l,
    g_c,
    r_c,
    sm_s,
    sm_r,
):
    z = lax.axis_index("shard")
    c = lax.axis_index("context")
    t = lax.axis_index("tensor")
    y = t // 2
    k = t - 2 * y
    tp = t + 1 - 2 * k
    t_far = t + 2 - 4 * y
    tp_far = tp + 2 - 4 * y
    dev_p = (z, c, tp)
    dev_y = (z, c, t_far)
    dev_x = (z, 1 - c, t)
    zo = [lax.rem(z + d, zs_n) for d in range(1, zs_n)]
    scale = HD ** (-0.5)
    hb = gin_ref

    def rc(src, dst, ss, rs, dev):
        return pltpu.make_async_remote_copy(
            src_ref=src, dst_ref=dst, send_sem=ss, recv_sem=rs, device_id=dev, device_id_type=MESH
        )

    barrier = pltpu.get_barrier_semaphore()
    for dev in [dev_p, dev_y, dev_x] + [(zz, c, t) for zz in zo]:
        pl.semaphore_signal(barrier, inc=1, device_id=dev, device_id_type=MESH)
    pl.semaphore_wait(barrier, 2 + zs_n)

    def mod_copy(d, to, frm):
        return rc(modin_ref.at[to], modr.at[frm], m_s.at[d], m_r.at[frm], (to, c, t))

    for d, zz in enumerate(zo):
        mod_copy(d, zz, z).start()

    shards = (sa_ref, su_ref, sd_ref)
    z_far = z + 2 - 4 * (z // 2)
    z_end = 3 * (z // 2)
    is_mid = (z == 1) | (z == 2)

    def w_rows(zz):
        return rows_at(288 * zz, 288)

    def w_send(layer, m, slot, zz):
        i = 3 * layer + m
        return rc(
            shards[m].at[layer], w.at[i, w_rows(z)], wz_s.at[i, slot], wz_r.at[i, z], (zz, c, t)
        )

    def w_local(layer, m):
        i = 3 * layer + m
        return pltpu.make_async_copy(shards[m].at[layer], w.at[i, w_rows(z)], w_l.at[i])

    def w0(layer, m):
        w_local(layer, m).start()
        w_send(layer, m, 0, z_far).start()

        @pl.when(z < zs_n - 1)
        def _():
            w_send(layer, m, 1, z + 1).start()

        @pl.when(z > 0)
        def _():
            w_send(layer, m, 2, z - 1).start()

    def w_take(i, zz):
        part = w.at[i, w_rows(zz)]
        return rc(part, part, wz_s.at[i, 3], wz_r.at[i, zz], (z_end, c, t))

    def relay(i):
        @pl.when(is_mid)
        def _():
            w_take(i, z_far).wait_recv()
            w_take(i, z_far).start()

    def w2(i):
        for zz in zo:

            @pl.when(jnp.logical_not(is_mid & (zz == z_far)))
            def _():
                w_take(i, zz).wait_recv()

        part = w.at[i, w_rows(z)]
        pltpu.make_async_copy(part, part, w_l.at[i]).wait()

    def w_drain(layer, m):
        w_send(layer, m, 0, z_far).wait_send()

        @pl.when(z < zs_n - 1)
        def _():
            w_send(layer, m, 1, z + 1).wait_send()

        @pl.when(z > 0)
        def _():
            w_send(layer, m, 2, z - 1).wait_send()

        @pl.when(is_mid)
        def _():
            w_take(3 * layer + m, z_far).wait_send()

    w0(0, 0)
    w0(0, 1)


    modr[z] = modin_ref[z]
    for zz in zo:
        mod_copy(0, zz, zz).wait_recv()
    for d in range(zs_n - 1):
        mod_copy(d, zo[d], z).wait_send()
    for layer in range(LAYERS):
        for zz in range(zs_n):
            modv[layer, 0:6, 288 * zz : 288 * (zz + 1)] = modr[zz, 8 * layer : 8 * layer + 6, 0:288]

    def mrow(layer, kind):
        return modv[layer, kind : kind + 1, :]

    def when(condition, action):
        @pl.when(condition)
        def _():
            action()

    def rows_of(s, block, offset=0, size=64):
        return rows_at(512 * s + 64 * block + offset, size)

    b_own, b_p = 4 * c + t, 4 * c + tp
    b_y, b_yp = 4 * c + t_far, 4 * c + tp_far
    b_x, b_xp = 4 * (1 - c) + t, 4 * (1 - c) + tp
    b_d, b_dp = 4 * (1 - c) + t_far, 4 * (1 - c) + tp_far
    sends = {
        0: (b_own, 0, 64, dev_p),
        1: (b_own, 0, 64, dev_y),
        2: (b_own, 0, 64, dev_x),
        3: (b_y, 0, 32, dev_x),
        4: (b_x, 32, 32, dev_y),
        5: (b_y, 0, 64, dev_p),
        6: (b_x, 0, 64, dev_p),
        7: (b_d, 0, 32, dev_p),
        8: (b_d, 32, 32, dev_p),
    }
    recvs = {
        0: (b_p, 0, 64),
        1: (b_y, 0, 64),
        2: (b_x, 0, 64),
        3: (b_d, 0, 32),
        4: (b_d, 32, 32),
        5: (b_yp, 0, 64),
        6: (b_xp, 0, 64),
        7: (b_dp, 0, 32),
        8: (b_dp, 32, 32),
    }

    class Gather:
        def __init__(self, buf, phase, layer):
            self.buf, self.phase, self.layer = buf, phase, layer

        def copy(self, s, index, block, offset, size, dev):
            part = self.buf.at[rows_of(s, block, offset, size)]
            at = (self.phase, self.layer, s, index)
            return rc(part, part, ap_s.at[at], ap_r.at[at], dev)

        def send(self, s, *indices):
            for index in indices:
                self.copy(s, index, *sends[index]).start()

        def wait(self, s, *indices):
            for index in indices:
                self.copy(s, index, *recvs[index], dev_p).wait_recv()

        def begin(self, s):
            self.send(s, 1, 2, 0)

        def hand_on(self, s):
            self.wait(s, 1)
            self.send(s, 3, 5)
            self.wait(s, 2)
            self.send(s, 4, 6)

        def hand_last(self, s):
            self.wait(s, 3)
            self.send(s, 7)
            self.wait(s, 4)
            self.send(s, 8)

        def drain(self):
            for s in range(2):
                for index, entry in sends.items():
                    self.copy(s, index, *entry).wait_send()

        def alone(self):
            for s in range(2):
                self.hand_on(s)
            for s in range(2):
                self.hand_last(s)
            for s in range(2):
                self.wait(s, 0, 5, 6, 7, 8)

        def run(self, compute, live=True):
            def step(n, carry):
                s, f = lax.rem(n, 2), n // 2

                def comm(*a):
                    first = a[0]
                    when((n == first) & live, lambda: a[1]())

                comm(0, lambda: self.wait(0, 0))
                comm(1, lambda: self.wait(1, 0))
                comm(2, lambda: (self.hand_on(0), self.wait(0, 5)))
                comm(3, lambda: (self.hand_on(1), self.wait(1, 5)))
                comm(4, lambda: self.wait(0, 6))
                comm(5, lambda: (self.wait(1, 6), self.hand_last(0)))
                comm(6, lambda: (self.wait(0, 7, 8), self.hand_last(1)))
                comm(7, lambda: self.wait(1, 7, 8))
                chip = 2 * lax.rem(c + f // 2, 2) + lax.rem(y + lax.rem(f, 2), 2)
                compute(s, 512 * s + 128 * chip)
                return carry

            lax.fori_loop(0, 8, step, 0)
            when(jnp.logical_and(live, True), self.drain)

    def pool_rows(i):
        return rows_at(128 * i, 128)

    def add_rows(count, fn):
        def one(r, inner):
            fn(16 * r)
            return inner

        lax.fori_loop(0, count // 16, one, 0)

    class Reduce:
        def __init__(self, phase, layer, compute):
            self.phase, self.layer, self.compute = phase, layer, compute

        def sem(self, s, index):
            at = (self.phase, self.layer, s, index)
            return rp_s.at[at], rp_r.at[at]

        def to_p(self, s, q):
            there = pool.at[rows_at(512 * s + 128 * q + 64 * (1 - k), 64)]
            return rc(there, ra.at[s, q], *self.sem(s, q), dev_p)

        def part(self, s, index, src, dst, offset, dev):
            return rc(
                src.at[s, pl.ds(offset, 32)],
                dst.at[s, pl.ds(offset, 32)],
                *self.sem(s, index),
                dev,
            )

        def leg(self, s, index):
            src, dst, offset, dev = {
                4: (dsend, drecv, 0, dev_x),
                5: (dsend, drecv, 32, dev_y),
                6: (xsend, xrecv, 0, dev_x),
                7: (ysend, yrecv, 32, dev_y),
                8: (xsend, xrecv, 32, dev_x),
                9: (ysend, yrecv, 0, dev_y),
            }[index]
            return self.part(s, index, src, dst, offset, dev)

        def pair(self, s, q, row):
            mine = pool[rows_at(512 * s + 128 * q + 64 * k + row, 16), :]
            return mine + ra[s, q, rows_at(row, 16), :]

        def step(self, s, q):
            chip = 2 * lax.rem(c + 1 - q // 2, 2) + lax.rem(y + 1 - lax.rem(q, 2), 2)
            pool[rows_at(512 * s + 128 * q, 128), :] = self.compute(512 * s + 128 * chip)
            self.to_p(s, q).start()
            def diagonal():
                self.to_p(s, 0).wait_recv()

                def fn(row):
                    dsend[s, rows_at(row, 16), :] = self.pair(s, 0, row).astype(BF16)

                add_rows(64, fn)
                self.leg(s, 4).start()
                self.leg(s, 5).start()

            def across_x():
                self.to_p(s, 1).wait_recv()

                def fn(row):
                    xsend[s, rows_at(row, 16), :] = self.pair(s, 1, row).astype(BF16)

                add_rows(32, fn)
                self.leg(s, 6).start()

            def across_y():
                self.to_p(s, 2).wait_recv()

                def fn(row):
                    ysend[s, rows_at(32 + row, 16), :] = self.pair(s, 2, 32 + row).astype(BF16)

                add_rows(32, fn)
                self.leg(s, 7).start()

            when(q == 1, diagonal)
            when(q == 2, across_x)
            when(q == 3, across_y)

        def hand_on(self, s):
            self.leg(s, 5).wait_recv()

            def fx(row):
                rr = rows_at(32 + row, 16)
                xsend[s, rr, :] = (
                    self.pair(s, 1, 32 + row) + drecv[s, rr, :].astype(F32)
                ).astype(BF16)

            add_rows(32, fx)
            self.leg(s, 8).start()
            self.leg(s, 4).wait_recv()

            def fy(row):
                rr = rows_at(row, 16)
                ysend[s, rr, :] = (self.pair(s, 2, row) + drecv[s, rr, :].astype(F32)).astype(BF16)

            add_rows(32, fy)
            self.leg(s, 9).start()

        def run(self):
            def one(n, carry):
                s, q = n // 4, lax.rem(n, 4)
                self.step(s, q)
                when(n == 5, lambda: self.hand_on(0))
                return carry

            lax.fori_loop(0, 8, one, 0)
            self.hand_on(1)

        def finish(self, s):
            self.to_p(s, 3).wait_recv()
            for index in (6, 7, 8, 9):
                self.leg(s, index).wait_recv()
            for q in range(4):
                self.to_p(s, q).wait_send()
            for index in range(4, 10):
                self.leg(s, index).wait_send()

        def total(self, s, row):
            rr = rows_at(row, 16)
            return (
                self.pair(s, 3, row) + xrecv[s, rr, :].astype(F32) + yrecv[s, rr, :].astype(F32)
            )

    def spread(column):
        return jnp.broadcast_to(column, (column.shape[0], 128))

    def layer_norm(v):
        center = v - jnp.mean(v, axis=-1, keepdims=True)
        r = lax.rsqrt(jnp.mean(center * center, axis=-1, keepdims=True) + epsilon)
        return center * r, r

    def head_mask(lo):
        lane = lax.broadcasted_iota(jnp.int32, (512, 256), 1)
        return (lane >= lo) & (lane < lo + HD)

    def own_rows(s, row):
        return rows_at(512 * s + 64 * b_own + row, 16)

    def cols128(b):
        return pl.ds(pl.multiple_of(128 * b, 128), 128)

    def piece(start):
        return rows_at(start, 128)

    def norm_in(layer, s):
        def ln1(r, inner):
            rr = rows_at(64 * s + 16 * r, 16)
            n, iv = layer_norm(hb[rr, :])
            own[layer, 0, rr, :] = n
            inv[layer, 0, rr, :] = spread(iv)
            mixed[layer, own_rows(s, 16 * r), :] = (
                n * (1.0 + mrow(layer, 1)) + mrow(layer, 0)
            ).astype(BF16)
            return inner

        lax.fori_loop(0, 4, ln1, 0)
        Gather(mixed.at[layer], 0, layer).begin(s)

    def forward(layer, carry):
        ia, iu, id_ = 3 * layer, 3 * layer + 1, 3 * layer + 2
        more = layer < LAYERS - 1

        def project(start):
            rr = piece(start)
            qkv[layer, rr, :] = (
                nn(mixed[layer, rr, :], w[ia, :, 0:512]) + bias_ref[layer, 0:1, 0:512]
            ).astype(BF16)
            v = qkv[layer, rr, 256:512].astype(F32)
            qa[layer, rr, :] = pltpu.roll(v, 224, 1).astype(BF16)

        w2(ia)
        Gather(mixed.at[layer], 0, layer).run(lambda s, start: project(start), layer > 0)
        relay(iu)
        when(more, lambda: w0(layer + 1, 0))
        ot[...] = jnp.zeros_like(ot)
        sum1 = Reduce(
            0, layer, lambda start: nt(att[layer, piece(start), :], w[ia, :, 384:640])
        )

        def half(qh, carry1):
            q_rows = rows_at(512 * qh, 512)
            q_cols = pl.ds(pl.multiple_of(512 * qh, 512), 512)

            def head(h, inner):
                when((qh == 1) & (h == 1), lambda: sum1.hand_on(0))
                qm = jnp.where(head_mask(72 * h), qa[layer, q_rows, :].astype(F32), 0.0)
                pb[0:512, 0:256] = qm.astype(BF16)

                def scores(kb, m8):
                    rr = rows_at(256 * kb, 256)
                    v = nt(qkv[layer, rr, 0:256], pb[0:512, 0:256]) * scale
                    pre[layer, rr, 0:512] = v
                    return jnp.maximum(m8, jnp.max(v.reshape(32, 8, 512), axis=0))

                m8 = lax.fori_loop(0, 4, scores, jnp.full((8, 512), -jnp.inf, F32))
                mx = jnp.max(m8, axis=0, keepdims=True)

                def exps(kb, l8):
                    rr = rows_at(128 * kb, 128)
                    e = jnp.exp(pre[layer, rr, 0:512] - mx)
                    pre[layer, rr, 0:512] = e
                    return l8 + fold(e)

                l8 = lax.fori_loop(0, 8, exps, jnp.zeros((8, 512), F32))
                row_sum = jnp.sum(l8, axis=0, keepdims=True)
                lse[layer, 2 * qh + h, 0:1, :] = mx + jnp.log(row_sum)
                inverse = 1.0 / row_sum

                def probs(kb, inner2):
                    rr = rows_at(128 * kb, 128)
                    pb[rows_at(512 + 128 * kb, 128), :] = (pre[layer, rr, 0:512] * inverse).astype(BF16)
                    return inner2

                lax.fori_loop(0, 8, probs, 0)
                otw[...] = tn(qkv[layer, :, 128:384], pb[512:1536, :])
                ot[pl.ds(pl.multiple_of(48 + 72 * h, 8), 72), q_cols] = otw[
                    pl.ds(pl.multiple_of(16 + 72 * h, 8), 72), :
                ]
                return inner

            lax.fori_loop(0, 2, head, 0)

            def put_att(b, inner):
                here = 4 * qh + b
                att[layer, pool_rows(here), :] = ot[:, cols128(here)].T.astype(BF16)
                return inner

            lax.fori_loop(0, 4, put_att, 0)

            def reduce_step(q, inner):
                sum1.step(qh, q)
                return inner

            lax.fori_loop(0, 4, reduce_step, 0)
            return carry1

        lax.fori_loop(0, 2, half, 0)
        sum1.hand_on(1)
        gather2 = Gather(ffall.at[layer], 1, layer)

        def norm_mid(s, carry1):
            sum1.finish(s)

            def ln2(r, inner):
                rr = rows_at(64 * s + 16 * r, 16)
                br = sum1.total(s, 16 * r) + bias_ref[layer, 1:2, :]
                own[layer, 2, rr, :] = br
                v = hb[rr, :] + mrow(layer, 2) * br
                af[rr, :] = v
                n, iv = layer_norm(v)
                own[layer, 1, rr, :] = n
                inv[layer, 1, rr, :] = spread(iv)
                ffall[layer, own_rows(s, 16 * r), :] = (
                    n * (1.0 + mrow(layer, 4)) + mrow(layer, 3)
                ).astype(BF16)
                return inner

            lax.fori_loop(0, 4, ln2, 0)
            gather2.begin(s)
            return carry1

        lax.fori_loop(0, 2, norm_mid, 0)
        relay(id_)
        when(more, lambda: w0(layer + 1, 1))
        w2(iu)

        def up(s, start):
            rr = piece(start)
            pre[layer, rr, :] = nn(ffall[layer, rr, :], w[iu]) + bias_ref[layer, 2:3, 0:640]

            def gelu(r, inner):
                r2 = rows_at(start + 16 * r, 16)
                act[r2, :] = jax.nn.gelu(pre[layer, r2, :], approximate=True).astype(BF16)
                return inner

            lax.fori_loop(0, 8, gelu, 0)

        gather2.run(up)
        w2(id_)
        sum2 = Reduce(1, layer, lambda start: nt(act[piece(start), :], w[id_]))
        sum2.run()

        def hand():
            relay(id_ + 1)
            w0(layer + 1, 2)

        when(more, hand)

        def finish(s, carry1):
            sum2.finish(s)

            def one(r, inner):
                rr = rows_at(64 * s + 16 * r, 16)
                fo = sum2.total(s, 16 * r) + bias_ref[layer, 3:4, :]
                own[layer, 3, rr, :] = fo
                hb[rr, :] = af[rr, :] + mrow(layer, 5) * fo
                return inner

            lax.fori_loop(0, 4, one, 0)
            when(more, lambda: norm_in(layer + 1, s))
            return carry1

        lax.fori_loop(0, 2, finish, 0)
        return carry

    hb[...] = x_ref[...].astype(F32)
    for s in range(2):
        norm_in(0, s)
    first_gather = Gather(mixed.at[0], 0, 0)
    last_gather = Gather(gff, 2, LAYERS - 1)
    for s in range(2):
        for r in range(4):
            g_in = cot_ref[64 * s + 16 * r : 64 * s + 16 * r + 16, :].astype(F32)
            gff[own_rows(s, 16 * r), :] = (mrow(LAYERS - 1, 5) * g_in).astype(BF16)
        last_gather.begin(s)
    first_gather.alone()
    relay(0)
    w0(0, 2)
    last_gather.alone()
    first_gather.drain()
    last_gather.drain()
    lax.fori_loop(0, LAYERS, forward, 0)

    for dev in (dev_p, dev_y, dev_x):
        pl.semaphore_signal(r_c, inc=1, device_id=dev, device_id_type=MESH)
    out_ref[...] = hb[...].astype(BF16)
    for layer in range(LAYERS):
        for m in range(3):
            w_drain(layer, m)
    hb[...] = cot_ref[...].astype(F32)

    def clear(d):
        rz[:, d] = jnp.zeros((6, 288, 640), BF16)

    when(z == 0, lambda: clear(0))
    when(z == 3, lambda: clear(2))

    def g_copy(i, d, zz):
        return rc(w.at[i, w_rows(zz)], rz.at[i, d], gz_s.at[i, d], gz_r.at[i, d], (zz, c, t))

    def g_relay(i):
        return rc(w.at[i, w_rows(3 - z)], rzr, gz_s.at[i, 3], gz_r.at[i, 3], (1 + z // 2, c, t))

    def g_end_copies(i):
        return (
            (z == 0, lambda: g_copy(i, 0, 1)),
            (z == 3, lambda: g_copy(i, 2, 2)),
            (jnp.logical_not(is_mid), lambda: g_copy(i, 1, z_far)),
        )

    def g0(i, credit):
        def from_mid():
            g_copy(i, 0, z + 1).start()
            g_copy(i, 2, z - 1).start()

        def from_end():
            when(jnp.logical_and(credit, True), lambda: pl.semaphore_wait(g_c, 1))
            g_relay(i).start()

        when(is_mid, from_mid)
        when(jnp.logical_not(is_mid), from_end)
        for condition, copy in g_end_copies(i):
            when(condition, lambda copy=copy: copy().start())

    def g1(i):
        def at_mid():
            g_relay(i).wait_recv()

            def add(row):
                rr = rows_at(288 * z_far + row, 16)
                w[i, rr, :] = (
                    w[i, rr, :].astype(F32) + rzr[rows_at(row, 16), :].astype(F32)
                ).astype(BF16)

            add_rows(288, add)
            g_copy(i, 1, z_far).start()
            pl.semaphore_signal(g_c, inc=1, device_id=(z_end, c, t), device_id_type=MESH)

        when(is_mid, at_mid)

    def g_send(i):
        return rc(w.at[i, w_rows(z)], gw_ref.at[i, c], gf_s.at[i], gf_r.at[i], dev_x)

    def g_keep(i):
        return pltpu.make_async_copy(w.at[i, w_rows(z)], gw_ref.at[i, c], g_l.at[i])

    def g2(i):
        def got(d):
            return rc(rz.at[i, d], rz.at[i, d], gz_s.at[i, d], gz_r.at[i, d], dev_x)

        when(z != 0, lambda: got(0).wait_recv())
        when(z != 3, lambda: got(2).wait_recv())
        got(1).wait_recv()

        def add(row):
            rr = rows_at(288 * z + row, 16)
            total = w[i, rr, :].astype(F32)
            for d in range(3):
                total = total + rz[i, d, rows_at(row, 16), :].astype(F32)
            w[i, rr, :] = total.astype(BF16)

        add_rows(288, add)
        g_send(i).start()
        g_keep(i).start()

    def g3(i):
        other = gw_ref.at[i, 1 - c]
        rc(other, other, gf_s.at[i], gf_r.at[i], dev_x).wait_recv()
        g_send(i).wait_send()
        g_keep(i).wait()

        def from_mid():
            for d, zz in ((0, z + 1), (1, z_far), (2, z - 1)):
                g_copy(i, d, zz).wait_send()

        when(is_mid, from_mid)
        when(jnp.logical_not(is_mid), lambda: g_relay(i).wait_send())
        for condition, copy in g_end_copies(i):
            when(condition, lambda copy=copy: copy().wait_send())

    def small():
        for index, size, dev in ((0, 8, dev_p), (1, 8, dev_y), (2, 16, dev_x)):
            step = rc(
                sm.at[:, 0:size],
                smr.at[index, :, 0:size],
                sm_s.at[index],
                sm_r.at[index],
                dev,
            )
            step.start()
            step.wait_send()
            step.wait_recv()
            sm[:, 0:size, :] = sm[:, 0:size, :] + smr[index, :, 0:size, :]
        small_ref[z] = sm[...]
        for d, zz in enumerate(zo):
            rc(sm, small_ref.at[z], sm_s.at[3 + d], sm_r.at[3 + z], (zz, c, t)).start()

    def small_end():
        for d, zz in enumerate(zo):
            end = rc(sm, small_ref.at[zz], sm_s.at[3 + d], sm_r.at[3 + zz], (zz, c, t))
            end.wait_recv()
            end.wait_send()

    zero8 = jnp.zeros((8, D), F32)

    def add_sum(layer, row, v8):
        here = (layer, pl.ds(row, 1), slice(0, v8.shape[1]))
        sm[here] = sm[here] + jnp.sum(v8, axis=0, keepdims=True)

    def grad_in_ff(layer, s, live):
        def start(r, sums):
            rr = rows_at(64 * s + 16 * r, 16)
            g = hb[rr, :]
            gf = (mrow(layer, 5) * g).astype(BF16)
            gff[own_rows(s, 16 * r), :] = gf
            return (sums[0] + fold(g * own[layer, 3, rr, :]), sums[1] + fold(gf.astype(F32)))

        s_gate2, s_bdown = lax.fori_loop(0, 4, start, (zero8, zero8))
        add_sum(layer, 5, s_gate2)
        add_sum(layer, 7, s_bdown)
        if live:
            Gather(gff, 2, layer).begin(s)

    def backward(step_index, carry):
        layer = LAYERS - 1 - step_index
        ia, iu, id_ = 3 * layer, 3 * layer + 1, 3 * layer + 2
        more = layer > 0

        def act_back(s, start):
            rr = piece(start)
            temp = rows_at(512 * s, 128)
            pool[temp, 0:640] = nn(gff[rr, :], w[id_])

            def one(r, total):
                r2 = rows_at(start + 16 * r, 16)
                v = pre[layer, r2, :]
                th = jnp.tanh(0.7978845608028654 * (v + 0.044715 * (v * v * v)))
                act[r2, :] = (0.5 * v * (1.0 + th)).astype(BF16)
                slope = 0.5 * (1.0 + th) + 0.5 * v * (1.0 - th * th) * (
                    0.7978845608028654 * (1.0 + 0.134145 * (v * v))
                )
                gp = (pool[rows_at(512 * s + 16 * r, 16), 0:640] * slope).astype(BF16)
                gpre[r2, :] = gp
                return total + fold(gp.astype(F32))

            add_sum(layer, 10 + c, lax.fori_loop(0, 8, one, jnp.zeros((8, 640), F32)))

        Gather(gff, 2, layer).run(act_back, layer < LAYERS - 1)
        when(layer == LAYERS - 1, lambda: pl.semaphore_wait(r_c, 3))
        sum1 = Reduce(2, layer, lambda start: nt(gpre[piece(start), :], w[iu]))
        sum1.run()

        def one_d(i, inner):
            w[id_, rows_at(128 * i, 128), :] = tn(gff[:, cols128(i)], act[...]).astype(BF16)
            return inner

        lax.fori_loop(0, 9, one_d, 0)
        when(layer == 0, lambda: g1(3))
        g0(id_, layer < LAYERS - 1)
        gather2 = Gather(gb, 3, layer)

        def middle(s, carry1):
            sum1.finish(s)

            def mid(r, sums):
                rr = rows_at(64 * s + 16 * r, 16)
                gf = sum1.total(s, 16 * r)
                n = own[layer, 1, rr, :]
                e = gf * (1.0 + mrow(layer, 4))
                iv = inv[layer, 1, rr, 0:1]
                ga = hb[rr, :] + iv * (
                    e
                    - jnp.mean(e, axis=-1, keepdims=True)
                    - n * jnp.mean(e * n, axis=-1, keepdims=True)
                )
                hb[rr, :] = ga
                gbv = (mrow(layer, 2) * ga).astype(BF16)
                gb[own_rows(s, 16 * r), :] = gbv
                return (
                    sums[0] + fold(gf),
                    sums[1] + fold(gf * n),
                    sums[2] + fold(ga * own[layer, 2, rr, :]),
                    sums[3] + fold(gbv.astype(F32)),
                )

            all_sums = lax.fori_loop(0, 4, mid, (zero8, zero8, zero8, zero8))
            for row, value in zip((3, 4, 2, 6), all_sums):
                add_sum(layer, row, value)
            gather2.begin(s)
            return carry1

        lax.fori_loop(0, 2, middle, 0)

        def one_u(i, inner):
            w[iu, rows_at(128 * i, 128), :] = tn(ffall[layer, :, cols128(i)], gpre[...]).astype(
                BF16
            )
            return inner

        lax.fori_loop(0, 9, one_u, 0)
        g1(id_)
        g0(iu, True)

        def att_back(s, start):
            rr = piece(start)
            doa[rr, :] = pltpu.roll(nn(gb[rr, :], w[ia, :, 384:640]), 224, 1).astype(BF16)

        gather2.run(att_back)
        dkv[...] = jnp.zeros_like(dkv)
        ot[...] = jnp.zeros_like(ot)

        def head(j, inner):
            h = lax.rem(j, 2)
            qh = j // 2
            q_rows = rows_at(512 * qh, 512)
            q_cols = pl.ds(pl.multiple_of(512 * qh, 512), 512)
            qm = jnp.where(head_mask(72 * h), qa[layer, q_rows, :].astype(F32), 0.0)
            dm = jnp.where(head_mask(16 + 72 * h), doa[q_rows, :].astype(F32), 0.0)
            pb[0:512, 0:256] = qm.astype(BF16)
            pb[0:512, 256:512] = dm.astype(BF16)
            log_row = lse[layer, j, 0:1, :]

            def first(kb, d8):
                rr = rows_at(256 * kb, 256)
                v = nt(qkv[layer, rr, 0:256], pb[0:512, 0:256]) * scale
                pr = jnp.exp(v - log_row)
                dp = nt(qkv[layer, rr, 128:384], pb[0:512, 256:512])
                pre[layer, rr, 0:512] = pr
                pool[rr, 0:512] = dp
                dkv[rr, 128:384] = dkv[rr, 128:384] + nn(pr.astype(BF16), pb[0:512, 256:512])
                return d8 + fold(pr * dp)

            d8 = lax.fori_loop(0, 4, first, jnp.zeros((8, 512), F32))
            delta = jnp.sum(d8, axis=0, keepdims=True)

            def second(kb, inner2):
                rr = rows_at(256 * kb, 256)
                ds = (pre[layer, rr, 0:512] * (pool[rr, 0:512] - delta)).astype(BF16)
                pb[rows_at(512 + 256 * kb, 256), :] = ds
                dkv[rr, 0:256] = dkv[rr, 0:256] + nn(ds, pb[0:512, 0:256]) * scale
                return inner2

            lax.fori_loop(0, 4, second, 0)
            otw[...] = tn(qkv[layer, :, 0:256], pb[512:1536, :]) * scale
            ot[pl.ds(pl.multiple_of(32 + 72 * h, 8), 72), q_cols] = otw[
                pl.ds(pl.multiple_of(72 * h, 8), 72), :
            ]
            return inner

        lax.fori_loop(0, 4, head, 0)

        def put(b, total):
            rr = pool_rows(b)
            dq = ot[:, cols128(b)].T
            kv = dkv[rr, :]
            both = jnp.concatenate(
                (kv[:, 0:256], kv[:, 256:384] + dq[:, 0:128], dq[:, 128:256]), axis=1
            ).astype(BF16)
            dqkv[rr, :] = both
            return total + fold(both.astype(F32))

        add_sum(layer, 8 + c, lax.fori_loop(0, 8, put, jnp.zeros((8, 512), F32)))

        def pending():
            g2(5)
            g2(4)

        when(layer == 0, pending)
        sum2 = Reduce(3, layer, lambda start: nt(dqkv[piece(start), :], w[ia, :, 0:512]))
        sum2.run()

        def one_a(i, inner):
            rr = rows_at(128 * i, 128)
            r1 = tn(mixed[layer, :, cols128(i)], dqkv[...])
            r3 = tn(gb[:, cols128(i)], att[layer])
            w[ia, rr, 0:384] = r1[:, 0:384].astype(BF16)
            w[ia, rr, 384:512] = (r1[:, 384:512] + r3[:, 0:128]).astype(BF16)
            w[ia, rr, 512:640] = r3[:, 128:256].astype(BF16)
            return inner

        lax.fori_loop(0, 9, one_a, 0)
        g1(iu)
        g0(ia, True)

        def final(s, carry1):
            sum2.finish(s)

            def last(r, sums):
                rr = rows_at(64 * s + 16 * r, 16)
                gm = sum2.total(s, 16 * r)
                n = own[layer, 0, rr, :]
                e = gm * (1.0 + mrow(layer, 1))
                iv = inv[layer, 0, rr, 0:1]
                hb[rr, :] = hb[rr, :] + iv * (
                    e
                    - jnp.mean(e, axis=-1, keepdims=True)
                    - n * jnp.mean(e * n, axis=-1, keepdims=True)
                )
                return (sums[0] + fold(gm), sums[1] + fold(gm * n))

            all_sums = lax.fori_loop(0, 4, last, (zero8, zero8))
            for row, value in zip((0, 1), all_sums):
                add_sum(layer, row, value)
            when(more, lambda: grad_in_ff(layer - 1, s, True))
            return carry1

        lax.fori_loop(0, 2, final, 0)
        return carry

    sm[...] = jnp.zeros_like(sm)
    for s in range(2):
        grad_in_ff(LAYERS - 1, s, False)
    lax.fori_loop(0, LAYERS, backward, 0)
    g1(0)
    when(jnp.logical_not(is_mid), lambda: pl.semaphore_wait(g_c, 1))
    small()
    g2(3)
    g2(2)
    g2(1)
    small_end()
    g2(0)
    for i in range(6):
        g3(i)


def sum_kernel(zs_n, part_ref, out_ref, got, send_sem, recv_sem):
    z = lax.axis_index("shard")
    c = lax.axis_index("context")
    t = lax.axis_index("tensor")
    others = [lax.rem(z + d, zs_n) for d in range(1, zs_n)]
    barrier = pltpu.get_barrier_semaphore()
    for zz in others:
        pl.semaphore_signal(barrier, inc=1, device_id=(zz, c, t), device_id_type=MESH)
    pl.semaphore_wait(barrier, zs_n - 1)

    def copy(d, slot, zz):
        return pltpu.make_async_remote_copy(
            src_ref=part_ref,
            dst_ref=got.at[slot],
            send_sem=send_sem.at[d],
            recv_sem=recv_sem.at[slot],
            device_id=(zz, c, t),
            device_id_type=MESH,
        )

    for d, zz in enumerate(others):
        copy(d, z, zz).start()
    got[z] = part_ref[...]
    for d, zz in enumerate(others):
        copy(d, zz, zz).wait_recv()
        copy(d, z, zz).wait_send()
    total = got[0]
    for zz in range(1, zs_n):
        total = total + got[zz]
    out_ref[...] = total


def sum_shards(zs_n, part):
    vm = pl.BlockSpec(memory_space=pltpu.VMEM)
    dma = pltpu.SemaphoreType.DMA
    return pl.pallas_call(
        functools.partial(sum_kernel, zs_n),
        name="sum_shards",
        out_shape=jax.ShapeDtypeStruct(part.shape, F32),
        in_specs=[vm],
        out_specs=vm,
        scratch_shapes=[
            pltpu.VMEM((zs_n,) + part.shape, F32),
            dma((zs_n - 1,)),
            dma((zs_n,)),
        ],
        compiler_params=pltpu.CompilerParams(collective_id=1, has_side_effects=True),
    )(part)


def run_stage(zs_n, x_in, cot, modin, bias, block_a, block_u, block_d):
    vm = pl.BlockSpec(memory_space=pltpu.VMEM)
    anyspace = pl.BlockSpec(memory_space=pl.ANY)
    dma = pltpu.SemaphoreType.DMA
    sds = jax.ShapeDtypeStruct
    scratch = [
        pltpu.VMEM((6, D, 640), BF16),
        pltpu.VMEM((2, 1024, D), BF16),
        pltpu.VMEM((2, 1024, 512), BF16),
        pltpu.VMEM((2, 1024, 256), BF16),
        pltpu.VMEM((2, 1024, 256), BF16),
        pltpu.VMEM((2, 1024, D), BF16),
        pltpu.VMEM((2, 1024, 640), F32),
        pltpu.VMEM((1024, 640), BF16),
        pltpu.VMEM((2, 4, 128, D), F32),
        pltpu.VMEM((2, 2, 128, 128), F32),
        pltpu.VMEM((2, 4, 8, 512), F32),
        pltpu.VMEM((zs_n, 16, 384), F32),
        pltpu.VMEM((2, 8, D), F32),
        pltpu.VMEM((128, D), F32),
        pltpu.VMEM((1024, D), F32),
        pltpu.VMEM((2, 4, 64, D), F32),
        pltpu.VMEM((2, 64, D), BF16),
        pltpu.VMEM((2, 64, D), BF16),
        pltpu.VMEM((2, 64, D), BF16),
        pltpu.VMEM((2, 64, D), BF16),
        pltpu.VMEM((2, 64, D), BF16),
        pltpu.VMEM((2, 64, D), BF16),
        pltpu.VMEM((1024, D), BF16),
        pltpu.VMEM((1024, 640), BF16),
        pltpu.VMEM((1024, D), BF16),
        pltpu.VMEM((1024, 256), BF16),
        pltpu.VMEM((1024, 512), BF16),
        pltpu.VMEM((1024, 384), F32),
        pltpu.VMEM((1536, 512), BF16),
        pltpu.VMEM((256, 512), F32),
        pltpu.VMEM((256, 1024), F32),
        pltpu.VMEM((6, zs_n - 1, 288, 640), BF16),
        pltpu.VMEM((288, 640), BF16),
        pltpu.VMEM((2, 16, D), F32),
        pltpu.VMEM((3, 2, 16, D), F32),
        dma((zs_n - 1,)),
        dma((zs_n,)),
        dma((6, 4)),
        dma((6, zs_n)),
        dma((6,)),
        dma((4, 2, 2, 9)),
        dma((4, 2, 2, 9)),
        dma((4, 2, 2, 10)),
        dma((4, 2, 2, 10)),
        dma((6, zs_n)),
        dma((6, zs_n)),
        dma((6,)),
        dma((6,)),
        dma((6,)),
        pltpu.SemaphoreType.REGULAR,
        pltpu.SemaphoreType.REGULAR,
        dma((3 + zs_n,)),
        dma((3 + zs_n,)),
    ]
    return pl.pallas_call(
        functools.partial(stage_kernel, zs_n),
        name="two_blocks",
        out_shape=(
            sds((128, D), BF16),
            sds((128, D), F32),
            sds((6, 2, 288, 640), BF16),
            sds((zs_n, 2, 16, D), F32),
        ),
        in_specs=[vm, vm, vm, vm, anyspace, anyspace, anyspace],
        out_specs=(vm, vm, anyspace, vm),
        scratch_shapes=scratch,
        compiler_params=pltpu.CompilerParams(
            collective_id=0, has_side_effects=True, vmem_limit_bytes=67043328
        ),
    )(x_in, cot, modin, bias, block_a, block_u, block_d)


def fast_body(
    zs_n,
    x_in,
    cond,
    w_ada,
    b_ada,
    w_qkv,
    b_qv,
    w_proj,
    b_proj,
    up_weight,
    up_bias_vector,
    down_weight,
    down_bias_vector,
    cotangent,
):
    z = lax.axis_index("shard")
    c = lax.axis_index("context")
    cols = w_ada.shape[3]
    part = w_qkv.shape[3] // 2
    units = up_weight.shape[2] // 2
    cond_low = jax.nn.silu(cond).astype(BF16)
    mod_terms = (
        jnp.einsum("sd,ldkc->lskc", cond_low, w_ada, preferred_element_type=F32)
        + b_ada.astype(F32)[:, None]
    ).astype(BF16)
    modin = jnp.pad(
        mod_terms.astype(F32).transpose(1, 0, 2, 3), ((0, 0), (0, 0), (0, 2), (0, 384 - cols))
    ).reshape(zs_n, 16, 384)

    def mine(array, size, axis):
        return lax.dynamic_slice_in_dim(array, c * size, size, axis)

    def wide(array, size):
        return jnp.pad(array, ((0, 0),) * (array.ndim - 1) + ((0, size - array.shape[-1]),))

    heads = mine(w_qkv, part, 3)
    block_a = wide(
        jnp.concatenate(
            (
                heads[:, 1],
                heads[:, 2],
                heads[:, 0],
                mine(w_proj, part, 1).transpose(0, 2, 1),
            ),
            axis=2,
        ),
        640,
    )
    block_u = wide(mine(up_weight, units, 2), 640)
    block_d = wide(mine(down_weight, units, 1).transpose(0, 2, 1), 640)
    b_heads = mine(b_qv, part, 2).astype(F32)
    b_qkv = jnp.concatenate((jnp.zeros((LAYERS, part), F32), b_heads[:, 1], b_heads[:, 0]), axis=1)
    bias = jnp.stack(
        (
            wide(b_qkv, D),
            b_proj.astype(F32),
            wide(mine(up_bias_vector, units, 1).astype(F32), D),
            down_bias_vector.astype(F32),
        ),
        axis=1,
    )
    out, grad_in, gw, small = run_stage(
        zs_n, x_in[:, 0], cotangent[:, 0], modin, bias, block_a, block_u, block_d
    )
    grad_mod = small[:, :, 0:6, :].astype(BF16)
    mod_cols = lax.dynamic_slice_in_dim(grad_mod, z * cols, cols, 3)
    grad_w_ada = jnp.einsum("sd,slkc->ldkc", cond_low, mod_cols, preferred_element_type=F32)
    grad_b_ada = jnp.sum(mod_cols.astype(F32), axis=0)
    cond_part = jnp.einsum("slkc,ldkc->sd", mod_cols, w_ada, preferred_element_type=F32)
    cond_total = sum_shards(zs_n, cond_part)
    silu_value, silu_back = jax.vjp(jax.nn.silu, cond)
    grad_cond = silu_back(cond_total)[0]
    sums = jnp.sum(small[:, :, 6:12, :], axis=0)

    def halves(row, start, size):
        return jnp.concatenate(
            (sums[:, row, start : start + size], sums[:, row + 1, start : start + size]), axis=1
        )

    gw = gw.reshape(LAYERS, 3, 2, cols, 640)

    def both(m, start, size):
        return jnp.concatenate(
            (gw[:, m, 0, :, start : start + size], gw[:, m, 1, :, start : start + size]), axis=2
        ).astype(F32)

    return (
        out[:, None],
        grad_in[:, None],
        grad_cond,
        grad_w_ada,
        grad_b_ada,
        jnp.stack((both(0, 2 * part, part), both(0, 0, part), both(0, part, part)), axis=1),
        jnp.stack((halves(2, 2 * part, part), halves(2, part, part)), axis=1),
        both(0, 3 * part, part).transpose(0, 2, 1),
        sums[:, 0],
        both(1, 0, units),
        halves(4, 0, units),
        both(2, 0, units).transpose(0, 2, 1),
        sums[:, 1],
    )


def solution(mesh):
    shape = mesh.shape
    program = body
    if shape["context"] == 2 and shape["tensor"] == 4 and shape["shard"] == 4:
        program = functools.partial(fast_body, shape["shard"])
    return jax.shard_map(
        program,
        mesh=mesh,
        in_specs=(
            P(("context", "tensor"), "shard", None),
            P(),
            P(None, None, None, "shard"),
            P(None, None, "shard"),
            P(None, None, "shard", "tensor"),
            P(None, None, "tensor"),
            P(None, "tensor", "shard"),
            P(),
            P(None, "shard", "tensor"),
            P(None, "tensor"),
            P(None, "tensor", "shard"),
            P(),
            P(("context", "tensor"), "shard", None),
        ),
        out_specs=(
            P(("context", "tensor"), "shard", None),
            P(("context", "tensor"), "shard", None),
            P(),
            P(None, None, None, "shard"),
            P(None, None, "shard"),
            P(None, None, "shard", "tensor"),
            P(None, None, "tensor"),
            P(None, "tensor", "shard"),
            P(),
            P(None, "shard", "tensor"),
            P(None, "tensor"),
            P(None, "tensor", "shard"),
            P(),
        ),
        check_vma=False,
    )
```

```python
import functools

import jax
import jax.numpy as jnp
from jax import lax
from jax.experimental import pallas as pl
from jax.experimental.pallas import tpu as pltpu
from jax.sharding import PartitionSpec as P

D = 1152
HD = 72
FF = 4608
LAYERS = 2


epsilon = 1e-06


def normalize(values):
    center = values - jnp.mean(values, axis=-1, keepdims=True)
    inverse = lax.rsqrt(jnp.mean(center * center, axis=-1, keepdims=True) + epsilon)
    return (center * inverse, inverse)


def normalize_back(grad_normed, normed, inverse):
    mean_grad = jnp.mean(grad_normed, axis=-1, keepdims=True)
    mean_proj = jnp.mean(grad_normed * normed, axis=-1, keepdims=True)
    return inverse * (grad_normed - mean_grad - normed * mean_proj)


def gelu_tanh(values):
    return jax.nn.gelu(values, approximate=True)


def to_heads(tokens):
    return tokens.reshape(tokens.shape[0], tokens.shape[1], -1, HD).transpose(1, 2, 0, 3)


def from_heads(blocks):
    return blocks.transpose(2, 0, 1, 3).reshape(blocks.shape[2], blocks.shape[0], -1)


def over_heads(head_fn, arrays):
    return lax.map(lambda seq_items: lax.map(head_fn, seq_items), arrays)


def score_block(query_head, key_head):
    return jnp.einsum(
        "qe,ke->qk", query_head, key_head, preferred_element_type=jnp.float32
    ) * HD ** (-0.5)


def forward_head(head_parts):
    query_head, key_head, value_head = head_parts
    scores = score_block(query_head, key_head)
    maxima = jnp.max(scores, axis=-1, keepdims=True)
    exp_scores = jnp.exp(scores - maxima)
    row_total = jnp.sum(exp_scores, axis=-1, keepdims=True)
    prob_low = (exp_scores / row_total).astype(jnp.bfloat16)
    result = jnp.dot(prob_low, value_head, preferred_element_type=jnp.float32).astype(jnp.bfloat16)
    return (result, (maxima + jnp.log(row_total))[:, 0])


def full_grads(head_parts):
    query_head, key_head, value_head, grad_head, log_head = head_parts
    prob_full = jnp.exp(score_block(query_head, key_head) - log_head[:, None])
    grad_prob = jnp.einsum("qe,ke->qk", grad_head, value_head, preferred_element_type=jnp.float32)
    row_delta = jnp.sum(prob_full * grad_prob, axis=-1, keepdims=True)
    grad_score = (prob_full * (grad_prob - row_delta)).astype(jnp.bfloat16)
    grad_query = jnp.dot(grad_score, key_head, preferred_element_type=jnp.float32) * HD ** (-0.5)
    grad_key = jnp.einsum(
        "qk,qe->ke", grad_score, query_head, preferred_element_type=jnp.float32
    ) * HD ** (-0.5)
    grad_value = jnp.einsum(
        "qk,qe->ke", prob_full.astype(jnp.bfloat16), grad_head, preferred_element_type=jnp.float32
    )
    return (grad_query, grad_key, grad_value)


def fetch_weights(qkv_part, proj_part, up_part, down_part, mod_part):
    return (
        lax.all_gather(qkv_part, "shard", axis=2, tiled=True),
        lax.all_gather(proj_part, "shard", axis=2, tiled=True),
        lax.all_gather(up_part, "shard", axis=1, tiled=True),
        lax.all_gather(down_part, "shard", axis=2, tiled=True),
        lax.all_gather(mod_part, "shard", axis=3, tiled=True),
    )


def layer_forward(hidden_state, weights, modulation, biases):
    full_qkv, full_proj, full_up, full_down, mod_unused = weights
    bias_qv, bias_proj, bias_up, bias_down = biases
    normed1, inverse1 = normalize(hidden_state)
    mix_in = (normed1 * (1.0 + modulation[:, 1]) + modulation[:, 0]).astype(jnp.bfloat16)
    mixed_all = lax.all_gather(mix_in, "tensor", axis=0, tiled=True)
    projected = jnp.einsum("tbd,kde->tbke", mixed_all, full_qkv, preferred_element_type=jnp.float32)
    queries = (projected[:, :, 0] + bias_qv[0]).astype(jnp.bfloat16)
    keys_own = projected[:, :, 1].astype(jnp.bfloat16)
    values_own = (projected[:, :, 2] + bias_qv[1]).astype(jnp.bfloat16)
    keys_all, values_all = (
        lax.all_gather(keys_own, "context", axis=0, tiled=True),
        lax.all_gather(values_own, "context", axis=0, tiled=True),
    )
    head_out, log_sums = over_heads(
        forward_head, (to_heads(queries), to_heads(keys_all), to_heads(values_all))
    )
    attended = from_heads(head_out)
    row_block = attended
    branch = (
        lax.psum_scatter(
            jnp.einsum("tbe,ed->tbd", row_block, full_proj, preferred_element_type=jnp.float32),
            "tensor",
            scatter_dimension=0,
            tiled=True,
        )
        + bias_proj
    )
    after_attn = hidden_state + modulation[:, 2] * branch
    normed2, inverse2 = normalize(after_attn)
    feedforward_input = (normed2 * (1.0 + modulation[:, 4]) + modulation[:, 3]).astype(jnp.bfloat16)
    ff_all = lax.all_gather(feedforward_input, "tensor", axis=0, tiled=True)
    preactivation_value = (
        jnp.einsum("tbd,df->tbf", ff_all, full_up, preferred_element_type=jnp.float32) + bias_up
    )
    activation_value = gelu_tanh(preactivation_value).astype(jnp.bfloat16)
    row_block = activation_value
    feedforward_output = (
        lax.psum_scatter(
            jnp.einsum(
                "tbf,fd->tbd", row_block, full_down, preferred_element_type=jnp.float32
            ).astype(jnp.bfloat16),
            "tensor",
            scatter_dimension=0,
            tiled=True,
        ).astype(jnp.float32)
        + bias_down
    )
    result = after_attn + modulation[:, 5] * feedforward_output
    stash = (
        normed1,
        inverse1,
        mixed_all,
        queries,
        keys_all,
        values_all,
        attended,
        log_sums,
        branch,
        normed2,
        inverse2,
        ff_all,
        preactivation_value,
        activation_value,
        feedforward_output,
    )
    return (result, stash)


def layer_backward(grad_hidden, weights, modulation, stash):
    full_qkv, full_proj, full_up, full_down, mod_unused = weights
    (
        normed1,
        inverse1,
        mixed_all,
        queries,
        keys_all,
        values_all,
        attended,
        log_sums,
        branch,
        normed2,
        inverse2,
        ff_all,
        preactivation_value,
        activation_value,
        feedforward_output,
    ) = stash
    grad_ff = (modulation[:, 5] * grad_hidden).astype(jnp.bfloat16)
    grad_gate2 = jnp.sum(grad_hidden * feedforward_output, axis=0)
    bias_down = jnp.sum(grad_ff.astype(jnp.float32), axis=(0, 1))
    grad_ff_all = lax.all_gather(grad_ff, "tensor", axis=0, tiled=True)
    grad_w_down = jnp.einsum(
        "tbf,tbd->fd", activation_value, grad_ff_all, preferred_element_type=jnp.float32
    )
    grad_activ = jnp.einsum(
        "tbd,fd->tbf", grad_ff_all, full_down, preferred_element_type=jnp.float32
    )
    gelu_value, gelu_back = jax.vjp(gelu_tanh, preactivation_value)
    grad_pre = gelu_back(grad_activ)[0].astype(jnp.bfloat16)
    bias_up = jnp.sum(grad_pre.astype(jnp.float32), axis=(0, 1))
    grad_w_up = jnp.einsum("tbd,tbf->df", ff_all, grad_pre, preferred_element_type=jnp.float32)
    row_block = grad_pre
    grad_ffin = lax.psum_scatter(
        jnp.einsum("tbf,df->tbd", row_block, full_up, preferred_element_type=jnp.float32).astype(
            jnp.bfloat16
        ),
        "tensor",
        scatter_dimension=0,
        tiled=True,
    ).astype(jnp.float32)
    grad_shift2 = jnp.sum(grad_ffin, axis=0)
    grad_scale2 = jnp.sum(grad_ffin * normed2, axis=0)
    grad_after = grad_hidden + normalize_back(
        grad_ffin * (1.0 + modulation[:, 4]), normed2, inverse2
    )
    grad_branch = (modulation[:, 2] * grad_after).astype(jnp.bfloat16)
    grad_gate1 = jnp.sum(grad_after * branch, axis=0)
    bias_proj = jnp.sum(grad_branch.astype(jnp.float32), axis=(0, 1))
    grad_branch_all = lax.all_gather(grad_branch, "tensor", axis=0, tiled=True)
    grad_w_proj = jnp.einsum(
        "tbe,tbd->ed", attended, grad_branch_all, preferred_element_type=jnp.float32
    )
    grad_attended = jnp.einsum(
        "tbd,ed->tbe", grad_branch_all, full_proj, preferred_element_type=jnp.float32
    ).astype(jnp.bfloat16)
    head_inputs = (
        to_heads(queries),
        to_heads(keys_all),
        to_heads(values_all),
        to_heads(grad_attended),
        log_sums,
    )
    grad_q_heads, grad_k_heads, grad_v_heads = over_heads(full_grads, head_inputs)
    grad_queries = from_heads(grad_q_heads).astype(jnp.bfloat16)
    grad_keys, grad_values = (
        lax.psum_scatter(
            from_heads(grad_k_heads).astype(jnp.bfloat16),
            "context",
            scatter_dimension=0,
            tiled=True,
        ).astype(jnp.float32),
        lax.psum_scatter(
            from_heads(grad_v_heads).astype(jnp.bfloat16),
            "context",
            scatter_dimension=0,
            tiled=True,
        ).astype(jnp.float32),
    )
    grad_keys = grad_keys.astype(jnp.bfloat16)
    grad_values = grad_values.astype(jnp.bfloat16)
    grad_qkv = jnp.stack((grad_queries, grad_keys, grad_values), axis=2)
    bias_qv = jnp.stack(
        (
            jnp.sum(grad_queries.astype(jnp.float32), axis=(0, 1)),
            jnp.sum(grad_values.astype(jnp.float32), axis=(0, 1)),
        )
    )
    grad_w_qkv = jnp.einsum(
        "tbd,tbke->kde", mixed_all, grad_qkv, preferred_element_type=jnp.float32
    )
    row_block = grad_qkv
    grad_mixin = lax.psum_scatter(
        jnp.einsum("tbke,kde->tbd", row_block, full_qkv, preferred_element_type=jnp.float32).astype(
            jnp.bfloat16
        ),
        "tensor",
        scatter_dimension=0,
        tiled=True,
    ).astype(jnp.float32)
    grad_shift1 = jnp.sum(grad_mixin, axis=0)
    grad_scale1 = jnp.sum(grad_mixin * normed1, axis=0)
    grad_input = grad_after + normalize_back(
        grad_mixin * (1.0 + modulation[:, 1]), normed1, inverse1
    )
    grad_mod_own = jnp.stack(
        (grad_shift1, grad_scale1, grad_gate1, grad_shift2, grad_scale2, grad_gate2), axis=1
    )
    return (
        grad_input,
        (grad_w_qkv, grad_w_proj, grad_w_up, grad_w_down),
        (grad_mod_own, bias_qv, bias_proj, bias_up, bias_down),
    )


def body(
    x_in,
    cond,
    w_ada,
    b_ada,
    w_qkv,
    b_qv,
    w_proj,
    b_proj,
    up_weight,
    up_bias_vector,
    down_weight,
    down_bias_vector,
    cotangent,
):
    shard_index = lax.axis_index("shard")
    tensor_index = lax.axis_index("tensor")
    context_index = lax.axis_index("context")
    own_latents = x_in.shape[1]
    all_latents = cond.shape[0]
    shard_cols = w_ada.shape[3]
    head_cols = w_qkv.shape[3]
    hidden_cols = up_weight.shape[2]
    condition_reduced = jax.nn.silu(cond).astype(jnp.bfloat16)
    mod_terms = (
        jnp.einsum("sd,ldkc->lskc", condition_reduced, w_ada, preferred_element_type=jnp.float32)
        + b_ada.astype(jnp.float32)[:, None]
    ).astype(jnp.bfloat16)
    hidden_state = x_in.astype(jnp.float32)
    layer_state = []
    for layer_number_index in range(LAYERS):
        sliced = fetch_weights(
            w_qkv[layer_number_index : layer_number_index + 1],
            w_proj[layer_number_index : layer_number_index + 1],
            up_weight[layer_number_index : layer_number_index + 1],
            down_weight[layer_number_index : layer_number_index + 1],
            mod_terms[layer_number_index : layer_number_index + 1],
        )
        weights = tuple((member_entry[0] for member_entry in sliced))
        modulation = lax.dynamic_slice_in_dim(
            weights[4], shard_index * own_latents, own_latents, 0
        ).astype(jnp.float32)
        biases = (
            b_qv[layer_number_index].astype(jnp.float32),
            b_proj[layer_number_index].astype(jnp.float32),
            up_bias_vector[layer_number_index].astype(jnp.float32),
            down_bias_vector[layer_number_index].astype(jnp.float32),
        )
        hidden_state, stash = layer_forward(hidden_state, weights, modulation, biases)
        layer_state.append((weights, modulation, stash))
    output = hidden_state.astype(jnp.bfloat16)
    grad_hidden = cotangent.astype(jnp.float32)
    cond_total = jnp.zeros(cond.shape, jnp.float32)
    results = [None] * LAYERS
    context_mask = (context_index == 0).astype(jnp.float32)
    for layer_number_index in reversed(range(LAYERS)):
        weights, modulation, stash = layer_state[layer_number_index]
        grad_hidden, matrix_grads, small_terms = layer_backward(
            grad_hidden, weights, modulation, stash
        )
        grad_mod_own, bias_qv, bias_proj, bias_up, bias_down = small_terms
        grad_mod_pad = lax.dynamic_update_slice_in_dim(
            jnp.zeros((all_latents, 6, D), jnp.float32), grad_mod_own, shard_index * own_latents, 0
        )
        bias_qv_pad = lax.dynamic_update_slice_in_dim(
            jnp.zeros((2, D), jnp.float32), bias_qv, tensor_index * head_cols, 1
        )
        bias_up_pad = lax.dynamic_update_slice_in_dim(
            jnp.zeros((FF,), jnp.float32), bias_up, tensor_index * hidden_cols, 0
        )
        mod_sum, proj_sum, down_sum, qv_sum, up_sum = lax.psum(
            (grad_mod_pad, bias_proj, bias_down, bias_qv_pad, bias_up_pad),
            ("shard", "context", "tensor"),
        )
        mod_cols = lax.dynamic_slice_in_dim(
            mod_sum.astype(jnp.bfloat16), shard_index * shard_cols, shard_cols, 2
        )
        grad_w_ada = jnp.einsum(
            "sd,skc->dkc", condition_reduced, mod_cols, preferred_element_type=jnp.float32
        )
        grad_b_ada = jnp.sum(mod_cols.astype(jnp.float32), axis=0)
        cond_part = (
            jnp.einsum(
                "skc,dkc->sd",
                mod_cols,
                w_ada[layer_number_index],
                preferred_element_type=jnp.float32,
            )
            * context_mask
        )
        grad_w_qkv, grad_w_proj, grad_w_up, grad_w_down = matrix_grads
        qkv_all, proj_all, up_all, down_all, cond_sum = (
            lax.psum(grad_w_qkv.astype(jnp.bfloat16), ("shard", "context")).astype(jnp.float32),
            lax.psum(grad_w_proj.astype(jnp.bfloat16), ("shard", "context")).astype(jnp.float32),
            lax.psum(grad_w_up.astype(jnp.bfloat16), ("shard", "context")).astype(jnp.float32),
            lax.psum(grad_w_down.astype(jnp.bfloat16), ("shard", "context")).astype(jnp.float32),
            lax.psum(cond_part.astype(jnp.bfloat16), ("shard", "context")).astype(jnp.float32),
        )
        qkv_own = lax.dynamic_slice_in_dim(qkv_all, shard_index * shard_cols, shard_cols, 1)
        proj_own = lax.dynamic_slice_in_dim(proj_all, shard_index * shard_cols, shard_cols, 1)
        up_own = lax.dynamic_slice_in_dim(up_all, shard_index * shard_cols, shard_cols, 0)
        down_own = lax.dynamic_slice_in_dim(down_all, shard_index * shard_cols, shard_cols, 1)
        cond_total = cond_total + cond_sum
        results[layer_number_index] = (
            grad_w_ada,
            grad_b_ada,
            qkv_own,
            lax.dynamic_slice_in_dim(qv_sum, tensor_index * head_cols, head_cols, 1),
            proj_own,
            proj_sum,
            up_own,
            lax.dynamic_slice_in_dim(up_sum, tensor_index * hidden_cols, hidden_cols, 0),
            down_own,
            down_sum,
        )
    silu_value, silu_back = jax.vjp(jax.nn.silu, cond)
    grad_cond = silu_back(cond_total)[0]
    stacked = tuple(
        (
            jnp.stack(
                [results[layer_number_index][member_entry] for layer_number_index in range(LAYERS)]
            )
            for member_entry in range(10)
        )
    )
    return (
        output,
        grad_hidden,
        grad_cond,
        stacked[0],
        stacked[1],
        stacked[2],
        stacked[3],
        stacked[4],
        stacked[5],
        stacked[6],
        stacked[7],
        stacked[8],
        stacked[9],
    )


MESH = pl.DeviceIdType.MESH
F32 = jnp.float32
BF16 = jnp.bfloat16


def nt(a, b):
    return lax.dot_general(a, b, (((1,), (1,)), ((), ())), preferred_element_type=F32)


def nn(a, b):
    return jnp.dot(a, b, preferred_element_type=F32)


def tn(a, b):
    return lax.dot_general(a, b, (((0,), (0,)), ((), ())), preferred_element_type=F32)


def fold(v):
    return jnp.sum(v.reshape(v.shape[0] // 8, 8, v.shape[1]), axis=0)


def rows_at(start, size, multiple=16):
    return pl.ds(pl.multiple_of(start, multiple), size)


def stage_kernel(
    zs_n,
    x_ref,
    cot_ref,
    modin_ref,
    bada_ref,
    bqv_ref,
    bproj_ref,
    bup_ref,
    bdown_ref,
    sa_ref,
    su_ref,
    sd_ref,
    out_ref,
    gin_ref,
    gw_ref,
    small_ref,
    w,
    mixed,
    qkv,
    qa,
    att,
    ffall,
    pre,
    act,
    own,
    inv,
    lse,
    bias_ref,
    mods,
    modr,
    modv,
    af,
    pool,
    ra,
    ysend,
    yrecv,
    xsend,
    xrecv,
    dsend,
    drecv,
    gff,
    gpre,
    gb,
    doa,
    dqkv,
    dkv,
    pb,
    otw,
    ot,
    rz,
    rzr,
    sm,
    smr,
    m_s,
    m_r,
    wz_s,
    wz_r,
    w_l,
    ap_s,
    ap_r,
    rp_s,
    rp_r,
    gz_s,
    gz_r,
    gf_s,
    gf_r,
    g_l,
    g_c,
    r_c,
    sm_s,
    sm_r,
):
    z = lax.axis_index("shard")
    c = lax.axis_index("context")
    t = lax.axis_index("tensor")
    y = t // 2
    k = t - 2 * y
    tp = t + 1 - 2 * k
    t_far = t + 2 - 4 * y
    tp_far = tp + 2 - 4 * y
    dev_p = (z, c, tp)
    dev_y = (z, c, t_far)
    dev_x = (z, 1 - c, t)
    zo = [lax.rem(z + d, zs_n) for d in range(1, zs_n)]
    scale = HD ** (-0.5)
    hb = gin_ref

    def rc(src, dst, ss, rs, dev):
        return pltpu.make_async_remote_copy(
            src_ref=src, dst_ref=dst, send_sem=ss, recv_sem=rs, device_id=dev, device_id_type=MESH
        )

    barrier = pltpu.get_barrier_semaphore()
    for dev in [dev_p, dev_y, dev_x] + [(zz, c, t) for zz in zo]:
        pl.semaphore_signal(barrier, inc=1, device_id=dev, device_id_type=MESH)
    pl.semaphore_wait(barrier, 2 + zs_n)

    def mod_copy(d, to, frm):
        return rc(mods.at[to], modr.at[frm], m_s.at[d], m_r.at[frm], (to, c, t))

    mods[...] = jnp.zeros_like(mods)
    for layer in range(LAYERS):
        for kind in range(6):
            row = 8 * layer + kind
            both = modin_ref[layer, kind] + bada_ref[layer, kind : kind + 1, :].astype(F32)
            both = both.astype(BF16).astype(F32)
            for zz in range(zs_n):
                mods[zz, row : row + 1, 0:288] = both[zz : zz + 1, :]
    for d, zz in enumerate(zo):
        mod_copy(d, zz, z).start()

    def own_half(value, size):
        return jnp.where(c == 0, value[:, 0:size], value[:, size : 2 * size])

    bias_ref[...] = jnp.zeros_like(bias_ref)
    for layer in range(LAYERS):
        b_heads = bqv_ref[layer].astype(F32)
        bias_ref[layer, 0:1, 144:288] = own_half(b_heads[1:2], 144)
        bias_ref[layer, 0:1, 288:432] = own_half(b_heads[0:1], 144)
        bias_ref[layer, 1:2, :] = bproj_ref[layer : layer + 1, :].astype(F32)
        bias_ref[layer, 2:3, 0:576] = own_half(bup_ref[layer : layer + 1, :].astype(F32), 576)
        bias_ref[layer, 3:4, :] = bdown_ref[layer : layer + 1, :].astype(F32)

    shards = (sa_ref, su_ref, sd_ref)
    z_far = z + 2 - 4 * (z // 2)
    z_end = 3 * (z // 2)
    is_mid = (z == 1) | (z == 2)

    def w_rows(zz):
        return rows_at(288 * zz, 288)

    def w_send(layer, m, slot, zz):
        i = 3 * layer + m
        return rc(
            shards[m].at[layer], w.at[i, w_rows(z)], wz_s.at[i, slot], wz_r.at[i, z], (zz, c, t)
        )

    def w_local(layer, m):
        i = 3 * layer + m
        return pltpu.make_async_copy(shards[m].at[layer], w.at[i, w_rows(z)], w_l.at[i])

    def w0(layer, m):
        w_local(layer, m).start()
        w_send(layer, m, 0, z_far).start()

        @pl.when(z < zs_n - 1)
        def _():
            w_send(layer, m, 1, z + 1).start()

        @pl.when(z > 0)
        def _():
            w_send(layer, m, 2, z - 1).start()

    def w_take(i, zz):
        part = w.at[i, w_rows(zz)]
        return rc(part, part, wz_s.at[i, 3], wz_r.at[i, zz], (z_end, c, t))

    def relay(i):
        @pl.when(is_mid)
        def _():
            w_take(i, z_far).wait_recv()
            w_take(i, z_far).start()

    def w2(i):
        for zz in zo:

            @pl.when(jnp.logical_not(is_mid & (zz == z_far)))
            def _():
                w_take(i, zz).wait_recv()

        part = w.at[i, w_rows(z)]
        pltpu.make_async_copy(part, part, w_l.at[i]).wait()

    def w_drain(layer, m):
        w_send(layer, m, 0, z_far).wait_send()

        @pl.when(z < zs_n - 1)
        def _():
            w_send(layer, m, 1, z + 1).wait_send()

        @pl.when(z > 0)
        def _():
            w_send(layer, m, 2, z - 1).wait_send()

        @pl.when(is_mid)
        def _():
            w_take(3 * layer + m, z_far).wait_send()

    w0(0, 0)
    w0(0, 1)


    modr[z] = mods[z]
    for zz in zo:
        mod_copy(0, zz, zz).wait_recv()
    for d in range(zs_n - 1):
        mod_copy(d, zo[d], z).wait_send()
    for layer in range(LAYERS):
        for zz in range(zs_n):
            modv[layer, 0:6, 288 * zz : 288 * (zz + 1)] = modr[zz, 8 * layer : 8 * layer + 6, 0:288]

    def mrow(layer, kind):
        return modv[layer, kind : kind + 1, :]

    def when(condition, action):
        @pl.when(condition)
        def _():
            action()

    def rows_of(s, block, offset=0, size=64):
        return rows_at(512 * s + 64 * block + offset, size)

    b_own, b_p = 4 * c + t, 4 * c + tp
    b_y, b_yp = 4 * c + t_far, 4 * c + tp_far
    b_x, b_xp = 4 * (1 - c) + t, 4 * (1 - c) + tp
    b_d, b_dp = 4 * (1 - c) + t_far, 4 * (1 - c) + tp_far
    sends = {
        0: (b_own, 0, 64, dev_p),
        1: (b_own, 0, 64, dev_y),
        2: (b_own, 0, 64, dev_x),
        3: (b_y, 0, 32, dev_x),
        4: (b_x, 32, 32, dev_y),
        5: (b_y, 0, 64, dev_p),
        6: (b_x, 0, 64, dev_p),
        7: (b_d, 0, 32, dev_p),
        8: (b_d, 32, 32, dev_p),
    }
    recvs = {
        0: (b_p, 0, 64),
        1: (b_y, 0, 64),
        2: (b_x, 0, 64),
        3: (b_d, 0, 32),
        4: (b_d, 32, 32),
        5: (b_yp, 0, 64),
        6: (b_xp, 0, 64),
        7: (b_dp, 0, 32),
        8: (b_dp, 32, 32),
    }

    class Gather:
        def __init__(self, buf, phase, layer):
            self.buf, self.phase, self.layer = buf, phase, layer

        def copy(self, s, index, block, offset, size, dev):
            part = self.buf.at[rows_of(s, block, offset, size)]
            at = (self.phase, self.layer, s, index)
            return rc(part, part, ap_s.at[at], ap_r.at[at], dev)

        def send(self, s, *indices):
            for index in indices:
                self.copy(s, index, *sends[index]).start()

        def wait(self, s, *indices):
            for index in indices:
                self.copy(s, index, *recvs[index], dev_p).wait_recv()

        def begin(self, s):
            self.send(s, 1, 2, 0)

        def hand_on(self, s):
            self.wait(s, 1)
            self.send(s, 3, 5)
            self.wait(s, 2)
            self.send(s, 4, 6)

        def hand_last(self, s):
            self.wait(s, 3)
            self.send(s, 7)
            self.wait(s, 4)
            self.send(s, 8)

        def drain(self):
            for s in range(2):
                for index, entry in sends.items():
                    self.copy(s, index, *entry).wait_send()

        def alone(self):
            for s in range(2):
                self.hand_on(s)
            for s in range(2):
                self.hand_last(s)
            for s in range(2):
                self.wait(s, 0, 5, 6, 7, 8)

        def run(self, compute, live=True):
            def step(n, carry):
                s, f = lax.rem(n, 2), n // 2

                def comm(*a):
                    first = a[0]
                    when((n == first) & live, lambda: a[1]())

                comm(0, lambda: self.wait(0, 0))
                comm(1, lambda: self.wait(1, 0))
                comm(2, lambda: (self.hand_on(0), self.wait(0, 5)))
                comm(3, lambda: (self.hand_on(1), self.wait(1, 5)))
                comm(4, lambda: self.wait(0, 6))
                comm(5, lambda: (self.wait(1, 6), self.hand_last(0)))
                comm(6, lambda: (self.wait(0, 7, 8), self.hand_last(1)))
                comm(7, lambda: self.wait(1, 7, 8))
                chip = 2 * lax.rem(c + f // 2, 2) + lax.rem(y + lax.rem(f, 2), 2)
                compute(s, 512 * s + 128 * chip)
                return carry

            lax.fori_loop(0, 8, step, 0)
            when(jnp.logical_and(live, True), self.drain)

    def pool_rows(i):
        return rows_at(128 * i, 128)

    def add_rows(count, fn):
        def one(r, inner):
            fn(16 * r)
            return inner

        lax.fori_loop(0, count // 16, one, 0)

    class Reduce:
        def __init__(self, phase, layer, compute):
            self.phase, self.layer, self.compute = phase, layer, compute

        def sem(self, s, index):
            at = (self.phase, self.layer, s, index)
            return rp_s.at[at], rp_r.at[at]

        def to_p(self, s, q):
            there = pool.at[rows_at(512 * s + 128 * q + 64 * (1 - k), 64)]
            return rc(there, ra.at[s, q], *self.sem(s, q), dev_p)

        def part(self, s, index, src, dst, offset, dev):
            return rc(
                src.at[s, pl.ds(offset, 32)],
                dst.at[s, pl.ds(offset, 32)],
                *self.sem(s, index),
                dev,
            )

        def leg(self, s, index):
            src, dst, offset, dev = {
                4: (dsend, drecv, 0, dev_x),
                5: (dsend, drecv, 32, dev_y),
                6: (xsend, xrecv, 0, dev_x),
                7: (ysend, yrecv, 32, dev_y),
                8: (xsend, xrecv, 32, dev_x),
                9: (ysend, yrecv, 0, dev_y),
            }[index]
            return self.part(s, index, src, dst, offset, dev)

        def pair(self, s, q, row):
            mine = pool[rows_at(512 * s + 128 * q + 64 * k + row, 16), :]
            return mine + ra[s, q, rows_at(row, 16), :]

        def step(self, s, q, both):
            chip = 2 * lax.rem(c + 1 - q // 2, 2) + lax.rem(y + 1 - lax.rem(q, 2), 2)
            pool[rows_at(512 * s + 128 * q, 128), :] = self.compute(512 * s + 128 * chip)
            self.to_p(s, q).start()
            def diagonal():
                self.to_p(s, 0).wait_recv()

                def fn(row):
                    dsend[s, rows_at(row, 16), :] = self.pair(s, 0, row).astype(BF16)

                add_rows(64, fn)
                self.leg(s, 4).start()
                self.leg(s, 5).start()

            def across_x():
                self.to_p(s, 1).wait_recv()

                def fn(row):
                    xsend[s, rows_at(row, 16), :] = self.pair(s, 1, row).astype(BF16)

                add_rows(32, fn)
                self.leg(s, 6).start()

            def across_y():
                self.to_p(s, 2).wait_recv()

                def fn(row):
                    ysend[s, rows_at(32 + row, 16), :] = self.pair(s, 2, 32 + row).astype(BF16)

                add_rows(32, fn)
                self.leg(s, 7).start()

            when(q == 1, diagonal)
            when(q == 2, across_x)

            def last():
                across_y()
                if both:
                    self.hand_on(s)

            when(q == 3, last)

        def hand_on(self, s):
            self.leg(s, 5).wait_recv()

            def fx(row):
                rr = rows_at(32 + row, 16)
                xsend[s, rr, :] = (
                    self.pair(s, 1, 32 + row) + drecv[s, rr, :].astype(F32)
                ).astype(BF16)

            add_rows(32, fx)
            self.leg(s, 8).start()
            self.leg(s, 4).wait_recv()

            def fy(row):
                rr = rows_at(row, 16)
                ysend[s, rr, :] = (self.pair(s, 2, row) + drecv[s, rr, :].astype(F32)).astype(BF16)

            add_rows(32, fy)
            self.leg(s, 9).start()

        def run(self):
            def one(n, carry):
                self.step(lax.rem(n, 2), n // 2, True)
                return carry

            lax.fori_loop(0, 8, one, 0)

        def finish(self, s):
            self.to_p(s, 3).wait_recv()
            for index in (6, 7, 8, 9):
                self.leg(s, index).wait_recv()
            for q in range(4):
                self.to_p(s, q).wait_send()
            for index in range(4, 10):
                self.leg(s, index).wait_send()

        def total(self, s, row):
            rr = rows_at(row, 16)
            return (
                self.pair(s, 3, row) + xrecv[s, rr, :].astype(F32) + yrecv[s, rr, :].astype(F32)
            )

    def spread(column):
        return jnp.broadcast_to(column, (column.shape[0], 128))

    def layer_norm(v):
        center = v - jnp.mean(v, axis=-1, keepdims=True)
        r = lax.rsqrt(jnp.mean(center * center, axis=-1, keepdims=True) + epsilon)
        return center * r, r

    def head_mask(lo):
        lane = lax.broadcasted_iota(jnp.int32, (512, 256), 1)
        return (lane >= lo) & (lane < lo + HD)

    def own_rows(s, row):
        return rows_at(512 * s + 64 * b_own + row, 16)

    def cols128(b):
        return pl.ds(pl.multiple_of(128 * b, 128), 128)

    def piece(start):
        return rows_at(start, 128)

    def norm_in(layer, s):
        def ln1(r, inner):
            rr = rows_at(64 * s + 16 * r, 16)
            n, iv = layer_norm(hb[rr, :])
            own[layer, 0, rr, :] = n
            inv[layer, 0, rr, :] = spread(iv)
            mixed[layer, own_rows(s, 16 * r), :] = (
                n * (1.0 + mrow(layer, 1)) + mrow(layer, 0)
            ).astype(BF16)
            return inner

        lax.fori_loop(0, 4, ln1, 0)
        Gather(mixed.at[layer], 0, layer).begin(s)

    def forward(layer, carry):
        ia, iu, id_ = 3 * layer, 3 * layer + 1, 3 * layer + 2
        more = layer < LAYERS - 1

        def project(start):
            rr = piece(start)
            qkv[layer, rr, :] = (
                nn(mixed[layer, rr, :], w[ia, :, 0:512]) + bias_ref[layer, 0:1, 0:512]
            ).astype(BF16)
            v = qkv[layer, rr, 256:512].astype(F32)
            qa[layer, rr, :] = pltpu.roll(v, 224, 1).astype(BF16)

        w2(ia)
        Gather(mixed.at[layer], 0, layer).run(lambda s, start: project(start), layer > 0)
        relay(iu)
        when(more, lambda: w0(layer + 1, 0))
        ot[...] = jnp.zeros_like(ot)
        sum1 = Reduce(
            0, layer, lambda start: nt(att[layer, piece(start), :], w[ia, :, 384:640])
        )

        def half(qh, carry1):
            q_rows = rows_at(512 * qh, 512)
            q_cols = pl.ds(pl.multiple_of(512 * qh, 512), 512)

            def head(h, inner):
                when((qh == 1) & (h == 1), lambda: sum1.hand_on(0))
                qm = jnp.where(head_mask(72 * h), qa[layer, q_rows, :].astype(F32), 0.0)
                pb[0:512, 0:256] = qm.astype(BF16)

                def scores(kb, m8):
                    rr = rows_at(256 * kb, 256)
                    v = nt(qkv[layer, rr, 0:256], pb[0:512, 0:256]) * scale
                    pre[layer, rr, 0:512] = v
                    return jnp.maximum(m8, jnp.max(v.reshape(32, 8, 512), axis=0))

                m8 = lax.fori_loop(0, 4, scores, jnp.full((8, 512), -jnp.inf, F32))
                mx = jnp.max(m8, axis=0, keepdims=True)

                def exps(kb, l8):
                    rr = rows_at(128 * kb, 128)
                    e = jnp.exp(pre[layer, rr, 0:512] - mx)
                    pre[layer, rr, 0:512] = e
                    return l8 + fold(e)

                l8 = lax.fori_loop(0, 8, exps, jnp.zeros((8, 512), F32))
                row_sum = jnp.sum(l8, axis=0, keepdims=True)
                lse[layer, 2 * qh + h, 0:1, :] = mx + jnp.log(row_sum)
                inverse = 1.0 / row_sum

                def probs(kb, inner2):
                    rr = rows_at(128 * kb, 128)
                    pb[rows_at(512 + 128 * kb, 128), :] = (pre[layer, rr, 0:512] * inverse).astype(BF16)
                    return inner2

                lax.fori_loop(0, 8, probs, 0)
                otw[...] = tn(qkv[layer, :, 128:384], pb[512:1536, :])
                ot[pl.ds(pl.multiple_of(48 + 72 * h, 8), 72), q_cols] = otw[
                    pl.ds(pl.multiple_of(16 + 72 * h, 8), 72), :
                ]
                return inner

            lax.fori_loop(0, 2, head, 0)

            def put_att(b, inner):
                here = 4 * qh + b
                att[layer, pool_rows(here), :] = ot[:, cols128(here)].T.astype(BF16)
                return inner

            lax.fori_loop(0, 4, put_att, 0)

            def reduce_step(q, inner):
                sum1.step(qh, q, False)
                return inner

            lax.fori_loop(0, 4, reduce_step, 0)
            return carry1

        lax.fori_loop(0, 2, half, 0)
        sum1.hand_on(1)
        gather2 = Gather(ffall.at[layer], 1, layer)

        def norm_mid(s, carry1):
            sum1.finish(s)

            def ln2(r, inner):
                rr = rows_at(64 * s + 16 * r, 16)
                br = sum1.total(s, 16 * r) + bias_ref[layer, 1:2, :]
                own[layer, 2, rr, :] = br
                v = hb[rr, :] + mrow(layer, 2) * br
                af[rr, :] = v
                n, iv = layer_norm(v)
                own[layer, 1, rr, :] = n
                inv[layer, 1, rr, :] = spread(iv)
                ffall[layer, own_rows(s, 16 * r), :] = (
                    n * (1.0 + mrow(layer, 4)) + mrow(layer, 3)
                ).astype(BF16)
                return inner

            lax.fori_loop(0, 4, ln2, 0)
            gather2.begin(s)
            return carry1

        lax.fori_loop(0, 2, norm_mid, 0)
        relay(id_)
        when(more, lambda: w0(layer + 1, 1))
        w2(iu)

        def up(s, start):
            rr = piece(start)
            pre[layer, rr, :] = nn(ffall[layer, rr, :], w[iu]) + bias_ref[layer, 2:3, 0:640]

            def gelu(r, inner):
                r2 = rows_at(start + 16 * r, 16)
                act[r2, :] = jax.nn.gelu(pre[layer, r2, :], approximate=True).astype(BF16)
                return inner

            lax.fori_loop(0, 8, gelu, 0)

        gather2.run(up)
        w2(id_)
        sum2 = Reduce(1, layer, lambda start: nt(act[piece(start), :], w[id_]))
        sum2.run()

        def hand():
            relay(id_ + 1)
            w0(layer + 1, 2)

        when(more, hand)

        def finish(s, carry1):
            sum2.finish(s)

            def one(r, inner):
                rr = rows_at(64 * s + 16 * r, 16)
                fo = sum2.total(s, 16 * r) + bias_ref[layer, 3:4, :]
                own[layer, 3, rr, :] = fo
                hb[rr, :] = af[rr, :] + mrow(layer, 5) * fo
                return inner

            lax.fori_loop(0, 4, one, 0)
            when(more, lambda: norm_in(layer + 1, s))
            return carry1

        lax.fori_loop(0, 2, finish, 0)
        return carry

    hb[...] = x_ref[...].astype(F32)
    for s in range(2):
        norm_in(0, s)
    first_gather = Gather(mixed.at[0], 0, 0)
    last_gather = Gather(gff, 2, LAYERS - 1)
    for s in range(2):
        for r in range(4):
            g_in = cot_ref[64 * s + 16 * r : 64 * s + 16 * r + 16, :].astype(F32)
            gff[own_rows(s, 16 * r), :] = (mrow(LAYERS - 1, 5) * g_in).astype(BF16)
        last_gather.begin(s)
    first_gather.alone()
    relay(0)
    w0(0, 2)
    last_gather.alone()
    first_gather.drain()
    last_gather.drain()
    lax.fori_loop(0, LAYERS, forward, 0)

    for dev in (dev_p, dev_y, dev_x):
        pl.semaphore_signal(r_c, inc=1, device_id=dev, device_id_type=MESH)
    out_ref[...] = hb[...].astype(BF16)
    for layer in range(LAYERS):
        for m in range(3):
            w_drain(layer, m)
    hb[...] = cot_ref[...].astype(F32)

    def clear(d):
        rz[:, d] = jnp.zeros((6, 288, 640), BF16)

    when(z == 0, lambda: clear(0))
    when(z == 3, lambda: clear(2))

    def g_rows(zz, h):
        return rows_at(288 * zz + 144 * h, 144)

    def g_copy(i, d, zz, h):
        got = rz.at[i, d, pl.ds(144 * h, 144)]
        return rc(
            w.at[i, g_rows(zz, h)], got, gz_s.at[i, d, h], gz_r.at[i, d, h], (zz, c, t)
        )

    def g_relay(i, h):
        got = rzr.at[pl.ds(144 * h, 144)]
        return rc(
            w.at[i, g_rows(3 - z, h)], got, gz_s.at[i, 3, h], gz_r.at[i, 3, h], (1 + z // 2, c, t)
        )

    is_end = jnp.logical_not(is_mid)

    def g_each(i, h, act_on):
        when(z == 0, lambda: act_on(g_copy(i, 0, 1, h)))
        when(z == 3, lambda: act_on(g_copy(i, 2, 2, h)))
        when(is_end, lambda: act_on(g_copy(i, 1, z_far, h)))

    def g_start(copy):
        copy.start()

    def g0(i):
        for h in range(2):
            g_each(i, h, g_start)

            def from_mid(h=h):
                g_copy(i, 0, z + 1, h).start()
                g_copy(i, 2, z - 1, h).start()

            when(is_mid, from_mid)

    def g0_relay(i, credit):
        when(is_end & jnp.logical_and(credit, True), lambda: pl.semaphore_wait(g_c, 1))
        for h in range(2):
            when(is_end, lambda h=h: g_relay(i, h).start())

    def g1(i):
        def at_mid():
            for h in range(2):
                g_relay(i, h).wait_recv()

                def add(row, h=h):
                    rr = rows_at(288 * z_far + 144 * h + row, 16)
                    w[i, rr, :] = (
                        w[i, rr, :].astype(F32) + rzr[rows_at(144 * h + row, 16), :].astype(F32)
                    ).astype(BF16)

                add_rows(144, add)
                g_copy(i, 1, z_far, h).start()
            pl.semaphore_signal(g_c, inc=1, device_id=(z_end, c, t), device_id_type=MESH)

        when(is_mid, at_mid)

    def g_send(i, h):
        there = gw_ref.at[i, c, pl.ds(144 * h, 144)]
        return rc(w.at[i, g_rows(z, h)], there, gf_s.at[i, h], gf_r.at[i, h], dev_x)

    def g_keep(i, h):
        there = gw_ref.at[i, c, pl.ds(144 * h, 144)]
        return pltpu.make_async_copy(w.at[i, g_rows(z, h)], there, g_l.at[i, h])

    def g2(i):
        for h in range(2):

            def got(d, h=h):
                part = rz.at[i, d, pl.ds(144 * h, 144)]
                return rc(part, part, gz_s.at[i, d, h], gz_r.at[i, d, h], dev_x)

            when(z != 0, lambda: got(0).wait_recv())
            when(z != 3, lambda: got(2).wait_recv())
            got(1).wait_recv()

            def add(row, h=h):
                rr = rows_at(288 * z + 144 * h + row, 16)
                total = w[i, rr, :].astype(F32)
                for d in range(3):
                    total = total + rz[i, d, rows_at(144 * h + row, 16), :].astype(F32)
                w[i, rr, :] = total.astype(BF16)

            add_rows(144, add)
            g_send(i, h).start()
            g_keep(i, h).start()

    def g3(i):
        def done(copy):
            copy.wait_send()

        for h in range(2):
            other = gw_ref.at[i, 1 - c, pl.ds(144 * h, 144)]
            rc(other, other, gf_s.at[i, h], gf_r.at[i, h], dev_x).wait_recv()
            g_send(i, h).wait_send()
            g_keep(i, h).wait()

            def from_mid(h=h):
                for d, zz in ((0, z + 1), (1, z_far), (2, z - 1)):
                    g_copy(i, d, zz, h).wait_send()

            when(is_mid, from_mid)
            when(is_end, lambda h=h: g_relay(i, h).wait_send())
            g_each(i, h, done)

    def small():
        for index, size, dev in ((0, 8, dev_p), (1, 8, dev_y), (2, 16, dev_x)):
            step = rc(
                sm.at[:, 0:size],
                smr.at[index, :, 0:size],
                sm_s.at[index],
                sm_r.at[index],
                dev,
            )
            step.start()
            step.wait_send()
            step.wait_recv()
            sm[:, 0:size, :] = sm[:, 0:size, :] + smr[index, :, 0:size, :]
        small_ref[z] = sm[...]
        for d, zz in enumerate(zo):
            rc(sm, small_ref.at[z], sm_s.at[3 + d], sm_r.at[3 + z], (zz, c, t)).start()

    def small_end():
        for d, zz in enumerate(zo):
            end = rc(sm, small_ref.at[zz], sm_s.at[3 + d], sm_r.at[3 + zz], (zz, c, t))
            end.wait_recv()
            end.wait_send()

    zero8 = jnp.zeros((8, D), F32)

    def add_sum(layer, row, v8):
        here = (layer, pl.ds(row, 1), slice(0, v8.shape[1]))
        sm[here] = sm[here] + jnp.sum(v8, axis=0, keepdims=True)

    def grad_in_ff(layer, s, live):
        def start(r, sums):
            rr = rows_at(64 * s + 16 * r, 16)
            g = hb[rr, :]
            gf = (mrow(layer, 5) * g).astype(BF16)
            gff[own_rows(s, 16 * r), :] = gf
            return (sums[0] + fold(g * own[layer, 3, rr, :]), sums[1] + fold(gf.astype(F32)))

        s_gate2, s_bdown = lax.fori_loop(0, 4, start, (zero8, zero8))
        add_sum(layer, 5, s_gate2)
        add_sum(layer, 7, s_bdown)
        if live:
            Gather(gff, 2, layer).begin(s)

    def backward(step_index, carry):
        layer = LAYERS - 1 - step_index
        ia, iu, id_ = 3 * layer, 3 * layer + 1, 3 * layer + 2
        more = layer > 0

        def act_back(s, start):
            rr = piece(start)
            temp = rows_at(512 * s, 128)
            pool[temp, 0:640] = nn(gff[rr, :], w[id_])

            def one(r, total):
                r2 = rows_at(start + 16 * r, 16)
                v = pre[layer, r2, :]
                th = jnp.tanh(0.7978845608028654 * (v + 0.044715 * (v * v * v)))
                act[r2, :] = (0.5 * v * (1.0 + th)).astype(BF16)
                slope = 0.5 * (1.0 + th) + 0.5 * v * (1.0 - th * th) * (
                    0.7978845608028654 * (1.0 + 0.134145 * (v * v))
                )
                gp = (pool[rows_at(512 * s + 16 * r, 16), 0:640] * slope).astype(BF16)
                gpre[r2, :] = gp
                return total + fold(gp.astype(F32))

            add_sum(layer, 10 + c, lax.fori_loop(0, 8, one, jnp.zeros((8, 640), F32)))

        Gather(gff, 2, layer).run(act_back, layer < LAYERS - 1)
        when(layer == 0, lambda: g1(3))
        when(layer == LAYERS - 1, lambda: pl.semaphore_wait(r_c, 3))
        sum1 = Reduce(2, layer, lambda start: nt(gpre[piece(start), :], w[iu]))
        sum1.run()

        def one_d(i, inner):
            w[id_, rows_at(128 * i, 128), :] = tn(gff[:, cols128(i)], act[...]).astype(BF16)
            return inner

        lax.fori_loop(0, 9, one_d, 0)
        g0_relay(id_, layer < LAYERS - 1)
        g0(id_)
        gather2 = Gather(gb, 3, layer)

        def middle(s, carry1):
            sum1.finish(s)

            def mid(r, sums):
                rr = rows_at(64 * s + 16 * r, 16)
                gf = sum1.total(s, 16 * r)
                n = own[layer, 1, rr, :]
                e = gf * (1.0 + mrow(layer, 4))
                iv = inv[layer, 1, rr, 0:1]
                ga = hb[rr, :] + iv * (
                    e
                    - jnp.mean(e, axis=-1, keepdims=True)
                    - n * jnp.mean(e * n, axis=-1, keepdims=True)
                )
                hb[rr, :] = ga
                gbv = (mrow(layer, 2) * ga).astype(BF16)
                gb[own_rows(s, 16 * r), :] = gbv
                return (
                    sums[0] + fold(gf),
                    sums[1] + fold(gf * n),
                    sums[2] + fold(ga * own[layer, 2, rr, :]),
                    sums[3] + fold(gbv.astype(F32)),
                )

            all_sums = lax.fori_loop(0, 4, mid, (zero8, zero8, zero8, zero8))
            for row, value in zip((3, 4, 2, 6), all_sums):
                add_sum(layer, row, value)
            gather2.begin(s)
            return carry1

        lax.fori_loop(0, 2, middle, 0)

        def one_u(i, inner):
            w[iu, rows_at(128 * i, 128), :] = tn(ffall[layer, :, cols128(i)], gpre[...]).astype(
                BF16
            )
            return inner

        lax.fori_loop(0, 9, one_u, 0)
        g1(id_)
        g0(iu)

        def att_back(s, start):
            rr = piece(start)
            doa[rr, :] = pltpu.roll(nn(gb[rr, :], w[ia, :, 384:640]), 224, 1).astype(BF16)

        gather2.run(att_back)
        g0_relay(iu, True)

        def pending():
            g2(5)
            g2(4)

        when(layer == 0, pending)
        dkv[...] = jnp.zeros_like(dkv)
        ot[...] = jnp.zeros_like(ot)

        def head(j, inner):
            h = lax.rem(j, 2)
            qh = j // 2
            q_rows = rows_at(512 * qh, 512)
            q_cols = pl.ds(pl.multiple_of(512 * qh, 512), 512)
            qm = jnp.where(head_mask(72 * h), qa[layer, q_rows, :].astype(F32), 0.0)
            dm = jnp.where(head_mask(16 + 72 * h), doa[q_rows, :].astype(F32), 0.0)
            pb[0:512, 0:256] = qm.astype(BF16)
            pb[0:512, 256:512] = dm.astype(BF16)
            log_row = lse[layer, j, 0:1, :]

            def first(kb, d8):
                rr = rows_at(256 * kb, 256)
                v = nt(qkv[layer, rr, 0:256], pb[0:512, 0:256]) * scale
                pr = jnp.exp(v - log_row)
                dp = nt(qkv[layer, rr, 128:384], pb[0:512, 256:512])
                pre[layer, rr, 0:512] = pr
                pool[rr, 0:512] = dp
                dkv[rr, 128:384] = dkv[rr, 128:384] + nn(pr.astype(BF16), pb[0:512, 256:512])
                return d8 + fold(pr * dp)

            d8 = lax.fori_loop(0, 4, first, jnp.zeros((8, 512), F32))
            delta = jnp.sum(d8, axis=0, keepdims=True)

            def second(kb, inner2):
                rr = rows_at(256 * kb, 256)
                ds = (pre[layer, rr, 0:512] * (pool[rr, 0:512] - delta)).astype(BF16)
                pb[rows_at(512 + 256 * kb, 256), :] = ds
                dkv[rr, 0:256] = dkv[rr, 0:256] + nn(ds, pb[0:512, 0:256]) * scale
                return inner2

            lax.fori_loop(0, 4, second, 0)
            otw[...] = tn(qkv[layer, :, 0:256], pb[512:1536, :]) * scale
            ot[pl.ds(pl.multiple_of(32 + 72 * h, 8), 72), q_cols] = otw[
                pl.ds(pl.multiple_of(72 * h, 8), 72), :
            ]
            return inner

        lax.fori_loop(0, 4, head, 0)

        def put(b, total):
            rr = pool_rows(b)
            dq = ot[:, cols128(b)].T
            kv = dkv[rr, :]
            both = jnp.concatenate(
                (kv[:, 0:256], kv[:, 256:384] + dq[:, 0:128], dq[:, 128:256]), axis=1
            ).astype(BF16)
            dqkv[rr, :] = both
            return total + fold(both.astype(F32))

        add_sum(layer, 8 + c, lax.fori_loop(0, 8, put, jnp.zeros((8, 512), F32)))

        g1(iu)
        sum2 = Reduce(3, layer, lambda start: nt(dqkv[piece(start), :], w[ia, :, 0:512]))
        sum2.run()

        def one_a(i, inner):
            rr = rows_at(128 * i, 128)
            r1 = tn(mixed[layer, :, cols128(i)], dqkv[...])
            r3 = tn(gb[:, cols128(i)], att[layer])
            w[ia, rr, 0:384] = r1[:, 0:384].astype(BF16)
            w[ia, rr, 384:512] = (r1[:, 384:512] + r3[:, 0:128]).astype(BF16)
            w[ia, rr, 512:640] = r3[:, 128:256].astype(BF16)
            return inner

        lax.fori_loop(0, 9, one_a, 0)
        g0_relay(ia, True)
        g0(ia)
        when(layer == 0, lambda: g2(3))

        def final(s, carry1):
            sum2.finish(s)

            def last(r, sums):
                rr = rows_at(64 * s + 16 * r, 16)
                gm = sum2.total(s, 16 * r)
                n = own[layer, 0, rr, :]
                e = gm * (1.0 + mrow(layer, 1))
                iv = inv[layer, 0, rr, 0:1]
                hb[rr, :] = hb[rr, :] + iv * (
                    e
                    - jnp.mean(e, axis=-1, keepdims=True)
                    - n * jnp.mean(e * n, axis=-1, keepdims=True)
                )
                return (sums[0] + fold(gm), sums[1] + fold(gm * n))

            all_sums = lax.fori_loop(0, 4, last, (zero8, zero8))
            for row, value in zip((0, 1), all_sums):
                add_sum(layer, row, value)
            when(more, lambda: grad_in_ff(layer - 1, s, True))
            return carry1

        lax.fori_loop(0, 2, final, 0)
        return carry

    sm[...] = jnp.zeros_like(sm)
    for s in range(2):
        grad_in_ff(LAYERS - 1, s, False)
    lax.fori_loop(0, LAYERS, backward, 0)
    g1(0)
    when(jnp.logical_not(is_mid), lambda: pl.semaphore_wait(g_c, 1))
    small()
    g2(2)
    g2(1)
    small_end()
    g2(0)
    for i in range(6):
        g3(i)


def sum_kernel(zs_n, part_ref, out_ref, got, send_sem, recv_sem):
    z = lax.axis_index("shard")
    c = lax.axis_index("context")
    t = lax.axis_index("tensor")
    others = [lax.rem(z + d, zs_n) for d in range(1, zs_n)]
    barrier = pltpu.get_barrier_semaphore()
    for zz in others:
        pl.semaphore_signal(barrier, inc=1, device_id=(zz, c, t), device_id_type=MESH)
    pl.semaphore_wait(barrier, zs_n - 1)

    def copy(d, slot, zz):
        return pltpu.make_async_remote_copy(
            src_ref=part_ref,
            dst_ref=got.at[slot],
            send_sem=send_sem.at[d],
            recv_sem=recv_sem.at[slot],
            device_id=(zz, c, t),
            device_id_type=MESH,
        )

    for d, zz in enumerate(others):
        copy(d, z, zz).start()
    got[z] = part_ref[...]
    for d, zz in enumerate(others):
        copy(d, zz, zz).wait_recv()
        copy(d, z, zz).wait_send()
    total = got[0]
    for zz in range(1, zs_n):
        total = total + got[zz]
    out_ref[...] = total


def sum_shards(zs_n, part):
    vm = pl.BlockSpec(memory_space=pltpu.VMEM)
    dma = pltpu.SemaphoreType.DMA
    return pl.pallas_call(
        functools.partial(sum_kernel, zs_n),
        name="sum_shards",
        out_shape=jax.ShapeDtypeStruct(part.shape, F32),
        in_specs=[vm],
        out_specs=vm,
        scratch_shapes=[
            pltpu.VMEM((zs_n,) + part.shape, F32),
            dma((zs_n - 1,)),
            dma((zs_n,)),
        ],
        compiler_params=pltpu.CompilerParams(collective_id=1, has_side_effects=True),
    )(part)


def run_stage(zs_n, *args):
    vm = pl.BlockSpec(memory_space=pltpu.VMEM)
    anyspace = pl.BlockSpec(memory_space=pl.ANY)
    dma = pltpu.SemaphoreType.DMA
    sds = jax.ShapeDtypeStruct
    scratch = [
        pltpu.VMEM((6, D, 640), BF16),
        pltpu.VMEM((2, 1024, D), BF16),
        pltpu.VMEM((2, 1024, 512), BF16),
        pltpu.VMEM((2, 1024, 256), BF16),
        pltpu.VMEM((2, 1024, 256), BF16),
        pltpu.VMEM((2, 1024, D), BF16),
        pltpu.VMEM((2, 1024, 640), F32),
        pltpu.VMEM((1024, 640), BF16),
        pltpu.VMEM((2, 4, 128, D), F32),
        pltpu.VMEM((2, 2, 128, 128), F32),
        pltpu.VMEM((2, 4, 8, 512), F32),
        pltpu.VMEM((2, 4, D), F32),
        pltpu.VMEM((zs_n, 16, 384), F32),
        pltpu.VMEM((zs_n, 16, 384), F32),
        pltpu.VMEM((2, 8, D), F32),
        pltpu.VMEM((128, D), F32),
        pltpu.VMEM((1024, D), F32),
        pltpu.VMEM((2, 4, 64, D), F32),
        pltpu.VMEM((2, 64, D), BF16),
        pltpu.VMEM((2, 64, D), BF16),
        pltpu.VMEM((2, 64, D), BF16),
        pltpu.VMEM((2, 64, D), BF16),
        pltpu.VMEM((2, 64, D), BF16),
        pltpu.VMEM((2, 64, D), BF16),
        pltpu.VMEM((1024, D), BF16),
        pltpu.VMEM((1024, 640), BF16),
        pltpu.VMEM((1024, D), BF16),
        pltpu.VMEM((1024, 256), BF16),
        pltpu.VMEM((1024, 512), BF16),
        pltpu.VMEM((1024, 384), F32),
        pltpu.VMEM((1536, 512), BF16),
        pltpu.VMEM((256, 512), F32),
        pltpu.VMEM((256, 1024), F32),
        pltpu.VMEM((6, zs_n - 1, 288, 640), BF16),
        pltpu.VMEM((288, 640), BF16),
        pltpu.VMEM((2, 16, D), F32),
        pltpu.VMEM((3, 2, 16, D), F32),
        dma((zs_n - 1,)),
        dma((zs_n,)),
        dma((6, 4)),
        dma((6, zs_n)),
        dma((6,)),
        dma((4, 2, 2, 9)),
        dma((4, 2, 2, 9)),
        dma((4, 2, 2, 10)),
        dma((4, 2, 2, 10)),
        dma((6, zs_n, 2)),
        dma((6, zs_n, 2)),
        dma((6, 2)),
        dma((6, 2)),
        dma((6, 2)),
        pltpu.SemaphoreType.REGULAR,
        pltpu.SemaphoreType.REGULAR,
        dma((3 + zs_n,)),
        dma((3 + zs_n,)),
    ]
    return pl.pallas_call(
        functools.partial(stage_kernel, zs_n),
        name="two_blocks",
        out_shape=(
            sds((128, D), BF16),
            sds((128, D), F32),
            sds((6, 2, 288, 640), BF16),
            sds((zs_n, 2, 16, D), F32),
        ),
        in_specs=[vm] * 8 + [anyspace] * 3,
        out_specs=(vm, vm, anyspace, vm),
        scratch_shapes=scratch,
        compiler_params=pltpu.CompilerParams(
            collective_id=0, has_side_effects=True, vmem_limit_bytes=67043328
        ),
    )(*args)


def fast_body(
    zs_n,
    x_in,
    cond,
    w_ada,
    b_ada,
    w_qkv,
    b_qv,
    w_proj,
    b_proj,
    up_weight,
    up_bias_vector,
    down_weight,
    down_bias_vector,
    cotangent,
):
    z = lax.axis_index("shard")
    c = lax.axis_index("context")
    cols = w_ada.shape[3]
    part = w_qkv.shape[3] // 2
    units = up_weight.shape[2] // 2
    cond_low = jax.nn.silu(cond).astype(BF16)
    modin = jnp.einsum("sd,ldkc->lksc", cond_low, w_ada, preferred_element_type=F32)

    def mine(array, size, axis):
        low = lax.slice_in_dim(array, 0, size, axis=axis)
        high = lax.slice_in_dim(array, size, 2 * size, axis=axis)
        return jnp.where(c == 0, low, high)

    def wide(array, size):
        return jnp.pad(array, ((0, 0),) * (array.ndim - 1) + ((0, size - array.shape[-1]),))

    heads = mine(w_qkv, part, 3)
    block_a = wide(
        jnp.concatenate(
            (
                heads[:, 1],
                heads[:, 2],
                heads[:, 0],
                mine(w_proj, part, 1).transpose(0, 2, 1),
            ),
            axis=2,
        ),
        640,
    )
    block_u = wide(mine(up_weight, units, 2), 640)
    block_d = wide(mine(down_weight, units, 1).transpose(0, 2, 1), 640)
    out, grad_in, gw, small = run_stage(
        zs_n,
        x_in[:, 0],
        cotangent[:, 0],
        modin,
        b_ada,
        b_qv,
        b_proj,
        up_bias_vector,
        down_bias_vector,
        block_a,
        block_u,
        block_d,
    )
    grad_mod = small[:, :, 0:6, :].astype(BF16)
    mod_cols = lax.dynamic_slice_in_dim(grad_mod, z * cols, cols, 3)
    grad_w_ada = jnp.einsum("sd,slkc->ldkc", cond_low, mod_cols, preferred_element_type=F32)
    grad_b_ada = jnp.sum(mod_cols.astype(F32), axis=0)
    cond_part = jnp.einsum("slkc,ldkc->sd", mod_cols, w_ada, preferred_element_type=F32)
    cond_total = sum_shards(zs_n, cond_part)
    silu_value, silu_back = jax.vjp(jax.nn.silu, cond)
    grad_cond = silu_back(cond_total)[0]
    sums = jnp.sum(small[:, :, 6:12, :], axis=0)

    def halves(row, start, size):
        return jnp.concatenate(
            (sums[:, row, start : start + size], sums[:, row + 1, start : start + size]), axis=1
        )

    gw = gw.reshape(LAYERS, 3, 2, cols, 640)

    def both(m, start, size):
        return jnp.concatenate(
            (gw[:, m, 0, :, start : start + size], gw[:, m, 1, :, start : start + size]), axis=2
        ).astype(F32)

    return (
        out[:, None],
        grad_in[:, None],
        grad_cond,
        grad_w_ada,
        grad_b_ada,
        jnp.stack((both(0, 2 * part, part), both(0, 0, part), both(0, part, part)), axis=1),
        jnp.stack((halves(2, 2 * part, part), halves(2, part, part)), axis=1),
        both(0, 3 * part, part).transpose(0, 2, 1),
        sums[:, 0],
        both(1, 0, units),
        halves(4, 0, units),
        both(2, 0, units).transpose(0, 2, 1),
        sums[:, 1],
    )


def solution(mesh):
    shape = mesh.shape
    program = body
    if shape["context"] == 2 and shape["tensor"] == 4 and shape["shard"] == 4:
        program = functools.partial(fast_body, shape["shard"])
    return jax.shard_map(
        program,
        mesh=mesh,
        in_specs=(
            P(("context", "tensor"), "shard", None),
            P(),
            P(None, None, None, "shard"),
            P(None, None, "shard"),
            P(None, None, "shard", "tensor"),
            P(None, None, "tensor"),
            P(None, "tensor", "shard"),
            P(),
            P(None, "shard", "tensor"),
            P(None, "tensor"),
            P(None, "tensor", "shard"),
            P(),
            P(("context", "tensor"), "shard", None),
        ),
        out_specs=(
            P(("context", "tensor"), "shard", None),
            P(("context", "tensor"), "shard", None),
            P(),
            P(None, None, None, "shard"),
            P(None, None, "shard"),
            P(None, None, "shard", "tensor"),
            P(None, None, "tensor"),
            P(None, "tensor", "shard"),
            P(),
            P(None, "shard", "tensor"),
            P(None, "tensor"),
            P(None, "tensor", "shard"),
            P(),
        ),
        check_vma=False,
    )
```

```python
import functools

import jax
import jax.numpy as jnp
from jax import lax
from jax.experimental import pallas as pl
from jax.experimental.pallas import tpu as pltpu
from jax.sharding import PartitionSpec as P

D = 1152
HD = 72
FF = 4608
LAYERS = 2


epsilon = 1e-06


def normalize(values):
    center = values - jnp.mean(values, axis=-1, keepdims=True)
    inverse = lax.rsqrt(jnp.mean(center * center, axis=-1, keepdims=True) + epsilon)
    return (center * inverse, inverse)


def normalize_back(grad_normed, normed, inverse):
    mean_grad = jnp.mean(grad_normed, axis=-1, keepdims=True)
    mean_proj = jnp.mean(grad_normed * normed, axis=-1, keepdims=True)
    return inverse * (grad_normed - mean_grad - normed * mean_proj)


def gelu_tanh(values):
    return jax.nn.gelu(values, approximate=True)


def to_heads(tokens):
    return tokens.reshape(tokens.shape[0], tokens.shape[1], -1, HD).transpose(1, 2, 0, 3)


def from_heads(blocks):
    return blocks.transpose(2, 0, 1, 3).reshape(blocks.shape[2], blocks.shape[0], -1)


def over_heads(head_fn, arrays):
    return lax.map(lambda seq_items: lax.map(head_fn, seq_items), arrays)


def score_block(query_head, key_head):
    return jnp.einsum(
        "qe,ke->qk", query_head, key_head, preferred_element_type=jnp.float32
    ) * HD ** (-0.5)


def forward_head(head_parts):
    query_head, key_head, value_head = head_parts
    scores = score_block(query_head, key_head)
    maxima = jnp.max(scores, axis=-1, keepdims=True)
    exp_scores = jnp.exp(scores - maxima)
    row_total = jnp.sum(exp_scores, axis=-1, keepdims=True)
    prob_low = (exp_scores / row_total).astype(jnp.bfloat16)
    result = jnp.dot(prob_low, value_head, preferred_element_type=jnp.float32).astype(jnp.bfloat16)
    return (result, (maxima + jnp.log(row_total))[:, 0])


def full_grads(head_parts):
    query_head, key_head, value_head, grad_head, log_head = head_parts
    prob_full = jnp.exp(score_block(query_head, key_head) - log_head[:, None])
    grad_prob = jnp.einsum("qe,ke->qk", grad_head, value_head, preferred_element_type=jnp.float32)
    row_delta = jnp.sum(prob_full * grad_prob, axis=-1, keepdims=True)
    grad_score = (prob_full * (grad_prob - row_delta)).astype(jnp.bfloat16)
    grad_query = jnp.dot(grad_score, key_head, preferred_element_type=jnp.float32) * HD ** (-0.5)
    grad_key = jnp.einsum(
        "qk,qe->ke", grad_score, query_head, preferred_element_type=jnp.float32
    ) * HD ** (-0.5)
    grad_value = jnp.einsum(
        "qk,qe->ke", prob_full.astype(jnp.bfloat16), grad_head, preferred_element_type=jnp.float32
    )
    return (grad_query, grad_key, grad_value)


def fetch_weights(qkv_part, proj_part, up_part, down_part, mod_part):
    return (
        lax.all_gather(qkv_part, "shard", axis=2, tiled=True),
        lax.all_gather(proj_part, "shard", axis=2, tiled=True),
        lax.all_gather(up_part, "shard", axis=1, tiled=True),
        lax.all_gather(down_part, "shard", axis=2, tiled=True),
        lax.all_gather(mod_part, "shard", axis=3, tiled=True),
    )


def layer_forward(hidden_state, weights, modulation, biases):
    full_qkv, full_proj, full_up, full_down, mod_unused = weights
    bias_qv, bias_proj, bias_up, bias_down = biases
    normed1, inverse1 = normalize(hidden_state)
    mix_in = (normed1 * (1.0 + modulation[:, 1]) + modulation[:, 0]).astype(jnp.bfloat16)
    mixed_all = lax.all_gather(mix_in, "tensor", axis=0, tiled=True)
    projected = jnp.einsum("tbd,kde->tbke", mixed_all, full_qkv, preferred_element_type=jnp.float32)
    queries = (projected[:, :, 0] + bias_qv[0]).astype(jnp.bfloat16)
    keys_own = projected[:, :, 1].astype(jnp.bfloat16)
    values_own = (projected[:, :, 2] + bias_qv[1]).astype(jnp.bfloat16)
    keys_all, values_all = (
        lax.all_gather(keys_own, "context", axis=0, tiled=True),
        lax.all_gather(values_own, "context", axis=0, tiled=True),
    )
    head_out, log_sums = over_heads(
        forward_head, (to_heads(queries), to_heads(keys_all), to_heads(values_all))
    )
    attended = from_heads(head_out)
    row_block = attended
    branch = (
        lax.psum_scatter(
            jnp.einsum("tbe,ed->tbd", row_block, full_proj, preferred_element_type=jnp.float32),
            "tensor",
            scatter_dimension=0,
            tiled=True,
        )
        + bias_proj
    )
    after_attn = hidden_state + modulation[:, 2] * branch
    normed2, inverse2 = normalize(after_attn)
    feedforward_input = (normed2 * (1.0 + modulation[:, 4]) + modulation[:, 3]).astype(jnp.bfloat16)
    ff_all = lax.all_gather(feedforward_input, "tensor", axis=0, tiled=True)
    preactivation_value = (
        jnp.einsum("tbd,df->tbf", ff_all, full_up, preferred_element_type=jnp.float32) + bias_up
    )
    activation_value = gelu_tanh(preactivation_value).astype(jnp.bfloat16)
    row_block = activation_value
    feedforward_output = (
        lax.psum_scatter(
            jnp.einsum(
                "tbf,fd->tbd", row_block, full_down, preferred_element_type=jnp.float32
            ).astype(jnp.bfloat16),
            "tensor",
            scatter_dimension=0,
            tiled=True,
        ).astype(jnp.float32)
        + bias_down
    )
    result = after_attn + modulation[:, 5] * feedforward_output
    stash = (
        normed1,
        inverse1,
        mixed_all,
        queries,
        keys_all,
        values_all,
        attended,
        log_sums,
        branch,
        normed2,
        inverse2,
        ff_all,
        preactivation_value,
        activation_value,
        feedforward_output,
    )
    return (result, stash)


def layer_backward(grad_hidden, weights, modulation, stash):
    full_qkv, full_proj, full_up, full_down, mod_unused = weights
    (
        normed1,
        inverse1,
        mixed_all,
        queries,
        keys_all,
        values_all,
        attended,
        log_sums,
        branch,
        normed2,
        inverse2,
        ff_all,
        preactivation_value,
        activation_value,
        feedforward_output,
    ) = stash
    grad_ff = (modulation[:, 5] * grad_hidden).astype(jnp.bfloat16)
    grad_gate2 = jnp.sum(grad_hidden * feedforward_output, axis=0)
    bias_down = jnp.sum(grad_ff.astype(jnp.float32), axis=(0, 1))
    grad_ff_all = lax.all_gather(grad_ff, "tensor", axis=0, tiled=True)
    grad_w_down = jnp.einsum(
        "tbf,tbd->fd", activation_value, grad_ff_all, preferred_element_type=jnp.float32
    )
    grad_activ = jnp.einsum(
        "tbd,fd->tbf", grad_ff_all, full_down, preferred_element_type=jnp.float32
    )
    gelu_value, gelu_back = jax.vjp(gelu_tanh, preactivation_value)
    grad_pre = gelu_back(grad_activ)[0].astype(jnp.bfloat16)
    bias_up = jnp.sum(grad_pre.astype(jnp.float32), axis=(0, 1))
    grad_w_up = jnp.einsum("tbd,tbf->df", ff_all, grad_pre, preferred_element_type=jnp.float32)
    row_block = grad_pre
    grad_ffin = lax.psum_scatter(
        jnp.einsum("tbf,df->tbd", row_block, full_up, preferred_element_type=jnp.float32).astype(
            jnp.bfloat16
        ),
        "tensor",
        scatter_dimension=0,
        tiled=True,
    ).astype(jnp.float32)
    grad_shift2 = jnp.sum(grad_ffin, axis=0)
    grad_scale2 = jnp.sum(grad_ffin * normed2, axis=0)
    grad_after = grad_hidden + normalize_back(
        grad_ffin * (1.0 + modulation[:, 4]), normed2, inverse2
    )
    grad_branch = (modulation[:, 2] * grad_after).astype(jnp.bfloat16)
    grad_gate1 = jnp.sum(grad_after * branch, axis=0)
    bias_proj = jnp.sum(grad_branch.astype(jnp.float32), axis=(0, 1))
    grad_branch_all = lax.all_gather(grad_branch, "tensor", axis=0, tiled=True)
    grad_w_proj = jnp.einsum(
        "tbe,tbd->ed", attended, grad_branch_all, preferred_element_type=jnp.float32
    )
    grad_attended = jnp.einsum(
        "tbd,ed->tbe", grad_branch_all, full_proj, preferred_element_type=jnp.float32
    ).astype(jnp.bfloat16)
    head_inputs = (
        to_heads(queries),
        to_heads(keys_all),
        to_heads(values_all),
        to_heads(grad_attended),
        log_sums,
    )
    grad_q_heads, grad_k_heads, grad_v_heads = over_heads(full_grads, head_inputs)
    grad_queries = from_heads(grad_q_heads).astype(jnp.bfloat16)
    grad_keys, grad_values = (
        lax.psum_scatter(
            from_heads(grad_k_heads).astype(jnp.bfloat16),
            "context",
            scatter_dimension=0,
            tiled=True,
        ).astype(jnp.float32),
        lax.psum_scatter(
            from_heads(grad_v_heads).astype(jnp.bfloat16),
            "context",
            scatter_dimension=0,
            tiled=True,
        ).astype(jnp.float32),
    )
    grad_keys = grad_keys.astype(jnp.bfloat16)
    grad_values = grad_values.astype(jnp.bfloat16)
    grad_qkv = jnp.stack((grad_queries, grad_keys, grad_values), axis=2)
    bias_qv = jnp.stack(
        (
            jnp.sum(grad_queries.astype(jnp.float32), axis=(0, 1)),
            jnp.sum(grad_values.astype(jnp.float32), axis=(0, 1)),
        )
    )
    grad_w_qkv = jnp.einsum(
        "tbd,tbke->kde", mixed_all, grad_qkv, preferred_element_type=jnp.float32
    )
    row_block = grad_qkv
    grad_mixin = lax.psum_scatter(
        jnp.einsum("tbke,kde->tbd", row_block, full_qkv, preferred_element_type=jnp.float32).astype(
            jnp.bfloat16
        ),
        "tensor",
        scatter_dimension=0,
        tiled=True,
    ).astype(jnp.float32)
    grad_shift1 = jnp.sum(grad_mixin, axis=0)
    grad_scale1 = jnp.sum(grad_mixin * normed1, axis=0)
    grad_input = grad_after + normalize_back(
        grad_mixin * (1.0 + modulation[:, 1]), normed1, inverse1
    )
    grad_mod_own = jnp.stack(
        (grad_shift1, grad_scale1, grad_gate1, grad_shift2, grad_scale2, grad_gate2), axis=1
    )
    return (
        grad_input,
        (grad_w_qkv, grad_w_proj, grad_w_up, grad_w_down),
        (grad_mod_own, bias_qv, bias_proj, bias_up, bias_down),
    )


def body(
    x_in,
    cond,
    w_ada,
    b_ada,
    w_qkv,
    b_qv,
    w_proj,
    b_proj,
    up_weight,
    up_bias_vector,
    down_weight,
    down_bias_vector,
    cotangent,
):
    shard_index = lax.axis_index("shard")
    tensor_index = lax.axis_index("tensor")
    context_index = lax.axis_index("context")
    own_latents = x_in.shape[1]
    all_latents = cond.shape[0]
    shard_cols = w_ada.shape[3]
    head_cols = w_qkv.shape[3]
    hidden_cols = up_weight.shape[2]
    condition_reduced = jax.nn.silu(cond).astype(jnp.bfloat16)
    mod_terms = (
        jnp.einsum("sd,ldkc->lskc", condition_reduced, w_ada, preferred_element_type=jnp.float32)
        + b_ada.astype(jnp.float32)[:, None]
    ).astype(jnp.bfloat16)
    hidden_state = x_in.astype(jnp.float32)
    layer_state = []
    for layer_number_index in range(LAYERS):
        sliced = fetch_weights(
            w_qkv[layer_number_index : layer_number_index + 1],
            w_proj[layer_number_index : layer_number_index + 1],
            up_weight[layer_number_index : layer_number_index + 1],
            down_weight[layer_number_index : layer_number_index + 1],
            mod_terms[layer_number_index : layer_number_index + 1],
        )
        weights = tuple((member_entry[0] for member_entry in sliced))
        modulation = lax.dynamic_slice_in_dim(
            weights[4], shard_index * own_latents, own_latents, 0
        ).astype(jnp.float32)
        biases = (
            b_qv[layer_number_index].astype(jnp.float32),
            b_proj[layer_number_index].astype(jnp.float32),
            up_bias_vector[layer_number_index].astype(jnp.float32),
            down_bias_vector[layer_number_index].astype(jnp.float32),
        )
        hidden_state, stash = layer_forward(hidden_state, weights, modulation, biases)
        layer_state.append((weights, modulation, stash))
    output = hidden_state.astype(jnp.bfloat16)
    grad_hidden = cotangent.astype(jnp.float32)
    cond_total = jnp.zeros(cond.shape, jnp.float32)
    results = [None] * LAYERS
    context_mask = (context_index == 0).astype(jnp.float32)
    for layer_number_index in reversed(range(LAYERS)):
        weights, modulation, stash = layer_state[layer_number_index]
        grad_hidden, matrix_grads, small_terms = layer_backward(
            grad_hidden, weights, modulation, stash
        )
        grad_mod_own, bias_qv, bias_proj, bias_up, bias_down = small_terms
        grad_mod_pad = lax.dynamic_update_slice_in_dim(
            jnp.zeros((all_latents, 6, D), jnp.float32), grad_mod_own, shard_index * own_latents, 0
        )
        bias_qv_pad = lax.dynamic_update_slice_in_dim(
            jnp.zeros((2, D), jnp.float32), bias_qv, tensor_index * head_cols, 1
        )
        bias_up_pad = lax.dynamic_update_slice_in_dim(
            jnp.zeros((FF,), jnp.float32), bias_up, tensor_index * hidden_cols, 0
        )
        mod_sum, proj_sum, down_sum, qv_sum, up_sum = lax.psum(
            (grad_mod_pad, bias_proj, bias_down, bias_qv_pad, bias_up_pad),
            ("shard", "context", "tensor"),
        )
        mod_cols = lax.dynamic_slice_in_dim(
            mod_sum.astype(jnp.bfloat16), shard_index * shard_cols, shard_cols, 2
        )
        grad_w_ada = jnp.einsum(
            "sd,skc->dkc", condition_reduced, mod_cols, preferred_element_type=jnp.float32
        )
        grad_b_ada = jnp.sum(mod_cols.astype(jnp.float32), axis=0)
        cond_part = (
            jnp.einsum(
                "skc,dkc->sd",
                mod_cols,
                w_ada[layer_number_index],
                preferred_element_type=jnp.float32,
            )
            * context_mask
        )
        grad_w_qkv, grad_w_proj, grad_w_up, grad_w_down = matrix_grads
        qkv_all, proj_all, up_all, down_all, cond_sum = (
            lax.psum(grad_w_qkv.astype(jnp.bfloat16), ("shard", "context")).astype(jnp.float32),
            lax.psum(grad_w_proj.astype(jnp.bfloat16), ("shard", "context")).astype(jnp.float32),
            lax.psum(grad_w_up.astype(jnp.bfloat16), ("shard", "context")).astype(jnp.float32),
            lax.psum(grad_w_down.astype(jnp.bfloat16), ("shard", "context")).astype(jnp.float32),
            lax.psum(cond_part.astype(jnp.bfloat16), ("shard", "context")).astype(jnp.float32),
        )
        qkv_own = lax.dynamic_slice_in_dim(qkv_all, shard_index * shard_cols, shard_cols, 1)
        proj_own = lax.dynamic_slice_in_dim(proj_all, shard_index * shard_cols, shard_cols, 1)
        up_own = lax.dynamic_slice_in_dim(up_all, shard_index * shard_cols, shard_cols, 0)
        down_own = lax.dynamic_slice_in_dim(down_all, shard_index * shard_cols, shard_cols, 1)
        cond_total = cond_total + cond_sum
        results[layer_number_index] = (
            grad_w_ada,
            grad_b_ada,
            qkv_own,
            lax.dynamic_slice_in_dim(qv_sum, tensor_index * head_cols, head_cols, 1),
            proj_own,
            proj_sum,
            up_own,
            lax.dynamic_slice_in_dim(up_sum, tensor_index * hidden_cols, hidden_cols, 0),
            down_own,
            down_sum,
        )
    silu_value, silu_back = jax.vjp(jax.nn.silu, cond)
    grad_cond = silu_back(cond_total)[0]
    stacked = tuple(
        (
            jnp.stack(
                [results[layer_number_index][member_entry] for layer_number_index in range(LAYERS)]
            )
            for member_entry in range(10)
        )
    )
    return (
        output,
        grad_hidden,
        grad_cond,
        stacked[0],
        stacked[1],
        stacked[2],
        stacked[3],
        stacked[4],
        stacked[5],
        stacked[6],
        stacked[7],
        stacked[8],
        stacked[9],
    )


MESH = pl.DeviceIdType.MESH
F32 = jnp.float32
BF16 = jnp.bfloat16


def nt(a, b):
    return lax.dot_general(a, b, (((1,), (1,)), ((), ())), preferred_element_type=F32)


def nn(a, b):
    return jnp.dot(a, b, preferred_element_type=F32)


def tn(a, b):
    return lax.dot_general(a, b, (((0,), (0,)), ((), ())), preferred_element_type=F32)


def fold(v):
    return jnp.sum(v.reshape(v.shape[0] // 8, 8, v.shape[1]), axis=0)


def rows_at(start, size, multiple=16):
    return pl.ds(pl.multiple_of(start, multiple), size)


def stage_kernel(
    zs_n,
    x_ref,
    cot_ref,
    modin_ref,
    bada_ref,
    bqv_ref,
    bproj_ref,
    bup_ref,
    bdown_ref,
    sa_ref,
    su_ref,
    sd_ref,
    out_ref,
    gin_ref,
    gw_ref,
    small_ref,
    w,
    mixed,
    qkv,
    qa,
    att,
    ffall,
    pre,
    act,
    own,
    inv,
    lse,
    bias_ref,
    mods,
    modr,
    modv,
    af,
    pool,
    ra,
    ysend,
    yrecv,
    xsend,
    xrecv,
    dsend,
    drecv,
    gff,
    gpre,
    gb,
    doa,
    dqkv,
    dkv,
    pb,
    otw,
    ot,
    rz,
    rzr,
    sm,
    smr,
    m_s,
    m_r,
    wz_s,
    wz_r,
    w_l,
    ap_s,
    ap_r,
    rp_s,
    rp_r,
    gz_s,
    gz_r,
    gf_s,
    gf_r,
    g_l,
    g_c,
    r_c,
    sm_s,
    sm_r,
):
    z = lax.axis_index("shard")
    c = lax.axis_index("context")
    t = lax.axis_index("tensor")
    y = t // 2
    k = t - 2 * y
    tp = t + 1 - 2 * k
    t_far = t + 2 - 4 * y
    tp_far = tp + 2 - 4 * y
    dev_p = (z, c, tp)
    dev_y = (z, c, t_far)
    dev_x = (z, 1 - c, t)
    zo = [lax.rem(z + d, zs_n) for d in range(1, zs_n)]
    scale = HD ** (-0.5)
    hb = gin_ref

    def rc(src, dst, ss, rs, dev):
        return pltpu.make_async_remote_copy(
            src_ref=src, dst_ref=dst, send_sem=ss, recv_sem=rs, device_id=dev, device_id_type=MESH
        )

    barrier = pltpu.get_barrier_semaphore()
    for dev in [dev_p, dev_y, dev_x] + [(zz, c, t) for zz in zo]:
        pl.semaphore_signal(barrier, inc=1, device_id=dev, device_id_type=MESH)
    pl.semaphore_wait(barrier, 2 + zs_n)

    def mod_copy(d, to, frm):
        return rc(mods.at[to], modr.at[frm], m_s.at[d], m_r.at[frm], (to, c, t))

    mods[...] = jnp.zeros_like(mods)
    for layer in range(LAYERS):
        for kind in range(6):
            row = 8 * layer + kind
            both = modin_ref[layer, kind] + bada_ref[layer, kind : kind + 1, :].astype(F32)
            both = both.astype(BF16).astype(F32)
            for zz in range(zs_n):
                mods[zz, row : row + 1, 0:288] = both[zz : zz + 1, :]
    for d, zz in enumerate(zo):
        mod_copy(d, zz, z).start()

    def own_half(value, size):
        return jnp.where(c == 0, value[:, 0:size], value[:, size : 2 * size])

    bias_ref[...] = jnp.zeros_like(bias_ref)
    for layer in range(LAYERS):
        b_heads = bqv_ref[layer].astype(F32)
        bias_ref[layer, 0:1, 144:288] = own_half(b_heads[1:2], 144)
        bias_ref[layer, 0:1, 288:432] = own_half(b_heads[0:1], 144)
        bias_ref[layer, 1:2, :] = bproj_ref[layer : layer + 1, :].astype(F32)
        bias_ref[layer, 2:3, 0:576] = own_half(bup_ref[layer : layer + 1, :].astype(F32), 576)
        bias_ref[layer, 3:4, :] = bdown_ref[layer : layer + 1, :].astype(F32)

    shards = (sa_ref, su_ref, sd_ref)
    z_far = z + 2 - 4 * (z // 2)
    z_end = 3 * (z // 2)
    is_mid = (z == 1) | (z == 2)

    def w_rows(zz):
        return rows_at(288 * zz, 288)

    def w_send(layer, m, slot, zz):
        i = 3 * layer + m
        return rc(
            shards[m].at[layer], w.at[i, w_rows(z)], wz_s.at[i, slot], wz_r.at[i, z], (zz, c, t)
        )

    def w_local(layer, m):
        i = 3 * layer + m
        return pltpu.make_async_copy(shards[m].at[layer], w.at[i, w_rows(z)], w_l.at[i])

    def w0(layer, m):
        w_local(layer, m).start()
        w_send(layer, m, 0, z_far).start()

        @pl.when(z < zs_n - 1)
        def _():
            w_send(layer, m, 1, z + 1).start()

        @pl.when(z > 0)
        def _():
            w_send(layer, m, 2, z - 1).start()

    def w_take(i, zz):
        part = w.at[i, w_rows(zz)]
        return rc(part, part, wz_s.at[i, 3], wz_r.at[i, zz], (z_end, c, t))

    def relay(i):
        @pl.when(is_mid)
        def _():
            w_take(i, z_far).wait_recv()
            w_take(i, z_far).start()

    def w2(i):
        for zz in zo:

            @pl.when(jnp.logical_not(is_mid & (zz == z_far)))
            def _():
                w_take(i, zz).wait_recv()

        part = w.at[i, w_rows(z)]
        pltpu.make_async_copy(part, part, w_l.at[i]).wait()

    def w_drain(layer, m):
        w_send(layer, m, 0, z_far).wait_send()

        @pl.when(z < zs_n - 1)
        def _():
            w_send(layer, m, 1, z + 1).wait_send()

        @pl.when(z > 0)
        def _():
            w_send(layer, m, 2, z - 1).wait_send()

        @pl.when(is_mid)
        def _():
            w_take(3 * layer + m, z_far).wait_send()

    w0(0, 0)


    modr[z] = mods[z]
    for zz in zo:
        mod_copy(0, zz, zz).wait_recv()
    for d in range(zs_n - 1):
        mod_copy(d, zo[d], z).wait_send()
    for layer in range(LAYERS):
        for zz in range(zs_n):
            modv[layer, 0:6, 288 * zz : 288 * (zz + 1)] = modr[zz, 8 * layer : 8 * layer + 6, 0:288]

    def mrow(layer, kind):
        return modv[layer, kind : kind + 1, :]

    def when(condition, action):
        @pl.when(condition)
        def _():
            action()

    def rows_of(s, block, offset=0, size=64):
        return rows_at(512 * s + 64 * block + offset, size)

    b_own, b_p = 4 * c + t, 4 * c + tp
    b_y, b_yp = 4 * c + t_far, 4 * c + tp_far
    b_x, b_xp = 4 * (1 - c) + t, 4 * (1 - c) + tp
    b_d, b_dp = 4 * (1 - c) + t_far, 4 * (1 - c) + tp_far
    sends = {
        0: (b_own, 0, 64, dev_p),
        1: (b_own, 0, 64, dev_y),
        2: (b_own, 0, 64, dev_x),
        3: (b_y, 0, 32, dev_x),
        4: (b_x, 32, 32, dev_y),
        5: (b_y, 0, 64, dev_p),
        6: (b_x, 0, 64, dev_p),
        7: (b_d, 0, 32, dev_p),
        8: (b_d, 32, 32, dev_p),
    }
    recvs = {
        0: (b_p, 0, 64),
        1: (b_y, 0, 64),
        2: (b_x, 0, 64),
        3: (b_d, 0, 32),
        4: (b_d, 32, 32),
        5: (b_yp, 0, 64),
        6: (b_xp, 0, 64),
        7: (b_dp, 0, 32),
        8: (b_dp, 32, 32),
    }

    class Gather:
        def __init__(self, buf, phase, layer):
            self.buf, self.phase, self.layer = buf, phase, layer

        def copy(self, s, index, block, offset, size, dev):
            part = self.buf.at[rows_of(s, block, offset, size)]
            at = (self.phase, self.layer, s, index)
            return rc(part, part, ap_s.at[at], ap_r.at[at], dev)

        def send(self, s, *indices):
            for index in indices:
                self.copy(s, index, *sends[index]).start()

        def wait(self, s, *indices):
            for index in indices:
                self.copy(s, index, *recvs[index], dev_p).wait_recv()

        def begin(self, s):
            self.send(s, 1, 2, 0)

        def hand_on(self, s):
            self.wait(s, 1)
            self.send(s, 3, 5)
            self.wait(s, 2)
            self.send(s, 4, 6)

        def hand_last(self, s):
            self.wait(s, 3)
            self.send(s, 7)
            self.wait(s, 4)
            self.send(s, 8)

        def drain(self):
            for s in range(2):
                for index, entry in sends.items():
                    self.copy(s, index, *entry).wait_send()

        def alone(self):
            for s in range(2):
                self.hand_on(s)
            for s in range(2):
                self.hand_last(s)
            for s in range(2):
                self.wait(s, 0, 5, 6, 7, 8)

        def run(self, compute, live=True):
            def step(n, carry):
                s, f = lax.rem(n, 2), n // 2

                def comm(*a):
                    first = a[0]
                    when((n == first) & live, lambda: a[1]())

                comm(0, lambda: self.wait(0, 0))
                comm(1, lambda: self.wait(1, 0))
                comm(2, lambda: (self.hand_on(0), self.wait(0, 5)))
                comm(3, lambda: (self.hand_on(1), self.wait(1, 5)))
                comm(4, lambda: self.wait(0, 6))
                comm(5, lambda: (self.wait(1, 6), self.hand_last(0)))
                comm(6, lambda: (self.wait(0, 7, 8), self.hand_last(1)))
                comm(7, lambda: self.wait(1, 7, 8))
                chip = 2 * lax.rem(c + f // 2, 2) + lax.rem(y + lax.rem(f, 2), 2)
                compute(s, 512 * s + 128 * chip)
                return carry

            lax.fori_loop(0, 8, step, 0)
            when(jnp.logical_and(live, True), self.drain)

    def pool_rows(i):
        return rows_at(128 * i, 128)

    def add_rows(count, fn):
        def one(r, inner):
            fn(16 * r)
            return inner

        lax.fori_loop(0, count // 16, one, 0)

    class Reduce:
        def __init__(self, phase, layer, compute):
            self.phase, self.layer, self.compute = phase, layer, compute

        def sem(self, s, index):
            at = (self.phase, self.layer, s, index)
            return rp_s.at[at], rp_r.at[at]

        def to_p(self, s, q):
            there = pool.at[rows_at(512 * s + 128 * q + 64 * (1 - k), 64)]
            return rc(there, ra.at[s, q], *self.sem(s, q), dev_p)

        def part(self, s, index, src, dst, offset, dev):
            return rc(
                src.at[s, pl.ds(offset, 32)],
                dst.at[s, pl.ds(offset, 32)],
                *self.sem(s, index),
                dev,
            )

        def leg(self, s, index):
            src, dst, offset, dev = {
                4: (dsend, drecv, 0, dev_x),
                5: (dsend, drecv, 32, dev_y),
                6: (xsend, xrecv, 0, dev_x),
                7: (ysend, yrecv, 32, dev_y),
                8: (xsend, xrecv, 32, dev_x),
                9: (ysend, yrecv, 0, dev_y),
            }[index]
            return self.part(s, index, src, dst, offset, dev)

        def pair(self, s, q, row):
            mine = pool[rows_at(512 * s + 128 * q + 64 * k + row, 16), :]
            return mine + ra[s, q, rows_at(row, 16), :]

        def step(self, s, q, both):
            chip = 2 * lax.rem(c + 1 - q // 2, 2) + lax.rem(y + 1 - lax.rem(q, 2), 2)
            pool[rows_at(512 * s + 128 * q, 128), :] = self.compute(512 * s + 128 * chip)
            self.to_p(s, q).start()
            def diagonal():
                self.to_p(s, 0).wait_recv()

                def fn(row):
                    dsend[s, rows_at(row, 16), :] = self.pair(s, 0, row).astype(BF16)

                add_rows(64, fn)
                self.leg(s, 4).start()
                self.leg(s, 5).start()

            def across_x():
                self.to_p(s, 1).wait_recv()

                def fn(row):
                    xsend[s, rows_at(row, 16), :] = self.pair(s, 1, row).astype(BF16)

                add_rows(32, fn)
                self.leg(s, 6).start()

            def across_y():
                self.to_p(s, 2).wait_recv()

                def fn(row):
                    ysend[s, rows_at(32 + row, 16), :] = self.pair(s, 2, 32 + row).astype(BF16)

                add_rows(32, fn)
                self.leg(s, 7).start()

            when(q == 1, diagonal)
            when(q == 2, across_x)

            def last():
                across_y()
                if both:
                    self.hand_on(s)

            when(q == 3, last)

        def hand_on(self, s):
            self.leg(s, 5).wait_recv()

            def fx(row):
                rr = rows_at(32 + row, 16)
                xsend[s, rr, :] = (
                    self.pair(s, 1, 32 + row) + drecv[s, rr, :].astype(F32)
                ).astype(BF16)

            add_rows(32, fx)
            self.leg(s, 8).start()
            self.leg(s, 4).wait_recv()

            def fy(row):
                rr = rows_at(row, 16)
                ysend[s, rr, :] = (self.pair(s, 2, row) + drecv[s, rr, :].astype(F32)).astype(BF16)

            add_rows(32, fy)
            self.leg(s, 9).start()

        def run(self):
            def one(n, carry):
                self.step(lax.rem(n, 2), n // 2, True)
                return carry

            lax.fori_loop(0, 8, one, 0)

        def finish(self, s):
            self.to_p(s, 3).wait_recv()
            for index in (6, 7, 8, 9):
                self.leg(s, index).wait_recv()
            for q in range(4):
                self.to_p(s, q).wait_send()
            for index in range(4, 10):
                self.leg(s, index).wait_send()

        def total(self, s, row):
            rr = rows_at(row, 16)
            return (
                self.pair(s, 3, row) + xrecv[s, rr, :].astype(F32) + yrecv[s, rr, :].astype(F32)
            )

    def spread(column):
        return jnp.broadcast_to(column, (column.shape[0], 128))

    def layer_norm(v):
        center = v - jnp.mean(v, axis=-1, keepdims=True)
        r = lax.rsqrt(jnp.mean(center * center, axis=-1, keepdims=True) + epsilon)
        return center * r, r

    def head_mask(lo):
        lane = lax.broadcasted_iota(jnp.int32, (512, 256), 1)
        return (lane >= lo) & (lane < lo + HD)

    def own_rows(s, row):
        return rows_at(512 * s + 64 * b_own + row, 16)

    def cols128(b):
        return pl.ds(pl.multiple_of(128 * b, 128), 128)

    def piece(start):
        return rows_at(start, 128)

    def norm_in(layer, s):
        def ln1(r, inner):
            rr = rows_at(64 * s + 16 * r, 16)
            n, iv = layer_norm(hb[rr, :])
            own[layer, 0, rr, :] = n
            inv[layer, 0, rr, :] = spread(iv)
            mixed[layer, own_rows(s, 16 * r), :] = (
                n * (1.0 + mrow(layer, 1)) + mrow(layer, 0)
            ).astype(BF16)
            return inner

        lax.fori_loop(0, 4, ln1, 0)
        Gather(mixed.at[layer], 0, layer).begin(s)

    def forward(layer, carry):
        ia, iu, id_ = 3 * layer, 3 * layer + 1, 3 * layer + 2
        more = layer < LAYERS - 1

        def project(start):
            rr = piece(start)
            qkv[layer, rr, :] = (
                nn(mixed[layer, rr, :], w[ia, :, 0:512]) + bias_ref[layer, 0:1, 0:512]
            ).astype(BF16)
            v = qkv[layer, rr, 256:512].astype(F32)
            qa[layer, rr, :] = pltpu.roll(v, 224, 1).astype(BF16)

        w2(ia)
        Gather(mixed.at[layer], 0, layer).run(lambda s, start: project(start), layer > 0)
        relay(iu)
        when(jnp.logical_not(more), lambda: w0(LAYERS - 1, 2))
        ot[...] = jnp.zeros_like(ot)
        sum1 = Reduce(
            0, layer, lambda start: nt(att[layer, piece(start), :], w[ia, :, 384:640])
        )

        def half(qh, carry1):
            q_rows = rows_at(512 * qh, 512)
            q_cols = pl.ds(pl.multiple_of(512 * qh, 512), 512)

            def head(h, inner):
                when((qh == 1) & (h == 1), lambda: sum1.hand_on(0))
                qm = jnp.where(head_mask(72 * h), qa[layer, q_rows, :].astype(F32), 0.0)
                pb[0:512, 0:256] = qm.astype(BF16)

                def scores(kb, m8):
                    rr = rows_at(256 * kb, 256)
                    v = nt(qkv[layer, rr, 0:256], pb[0:512, 0:256]) * scale
                    pre[layer, rr, 0:512] = v
                    return jnp.maximum(m8, jnp.max(v.reshape(32, 8, 512), axis=0))

                m8 = lax.fori_loop(0, 4, scores, jnp.full((8, 512), -jnp.inf, F32))
                mx = jnp.max(m8, axis=0, keepdims=True)

                def exps(kb, l8):
                    rr = rows_at(128 * kb, 128)
                    e = jnp.exp(pre[layer, rr, 0:512] - mx)
                    pre[layer, rr, 0:512] = e
                    return l8 + fold(e)

                l8 = lax.fori_loop(0, 8, exps, jnp.zeros((8, 512), F32))
                row_sum = jnp.sum(l8, axis=0, keepdims=True)
                lse[layer, 2 * qh + h, 0:1, :] = mx + jnp.log(row_sum)
                inverse = 1.0 / row_sum

                def probs(kb, inner2):
                    rr = rows_at(128 * kb, 128)
                    pb[rows_at(512 + 128 * kb, 128), :] = (pre[layer, rr, 0:512] * inverse).astype(BF16)
                    return inner2

                lax.fori_loop(0, 8, probs, 0)
                otw[...] = tn(qkv[layer, :, 128:384], pb[512:1536, :])
                ot[pl.ds(pl.multiple_of(48 + 72 * h, 8), 72), q_cols] = otw[
                    pl.ds(pl.multiple_of(16 + 72 * h, 8), 72), :
                ]
                return inner

            lax.fori_loop(0, 2, head, 0)

            def put_att(b, inner):
                here = 4 * qh + b
                att[layer, pool_rows(here), :] = ot[:, cols128(here)].T.astype(BF16)
                return inner

            lax.fori_loop(0, 4, put_att, 0)

            def reduce_step(q, inner):
                sum1.step(qh, q, False)
                return inner

            lax.fori_loop(0, 4, reduce_step, 0)
            return carry1

        lax.fori_loop(0, 2, half, 0)
        sum1.hand_on(1)
        gather2 = Gather(ffall.at[layer], 1, layer)

        def norm_mid(s, carry1):
            sum1.finish(s)

            def ln2(r, inner):
                rr = rows_at(64 * s + 16 * r, 16)
                br = sum1.total(s, 16 * r) + bias_ref[layer, 1:2, :]
                own[layer, 2, rr, :] = br
                v = hb[rr, :] + mrow(layer, 2) * br
                af[rr, :] = v
                n, iv = layer_norm(v)
                own[layer, 1, rr, :] = n
                inv[layer, 1, rr, :] = spread(iv)
                ffall[layer, own_rows(s, 16 * r), :] = (
                    n * (1.0 + mrow(layer, 4)) + mrow(layer, 3)
                ).astype(BF16)
                return inner

            lax.fori_loop(0, 4, ln2, 0)
            gather2.begin(s)
            return carry1

        lax.fori_loop(0, 2, norm_mid, 0)
        relay(id_)
        when(more, lambda: w0(layer + 1, 0))
        w2(iu)

        def up(s, start):
            rr = piece(start)
            pre[layer, rr, :] = nn(ffall[layer, rr, :], w[iu]) + bias_ref[layer, 2:3, 0:640]

            def gelu(r, inner):
                r2 = rows_at(start + 16 * r, 16)
                act[r2, :] = jax.nn.gelu(pre[layer, r2, :], approximate=True).astype(BF16)
                return inner

            lax.fori_loop(0, 8, gelu, 0)

        gather2.run(up)
        w2(id_)
        sum2 = Reduce(1, layer, lambda start: nt(act[piece(start), :], w[id_]))
        sum2.run()

        def hand():
            relay(id_ + 1)
            w0(layer + 1, 1)

        when(more, hand)

        def finish(s, carry1):
            sum2.finish(s)

            def one(r, inner):
                rr = rows_at(64 * s + 16 * r, 16)
                fo = sum2.total(s, 16 * r) + bias_ref[layer, 3:4, :]
                own[layer, 3, rr, :] = fo
                hb[rr, :] = af[rr, :] + mrow(layer, 5) * fo
                return inner

            lax.fori_loop(0, 4, one, 0)
            when(more, lambda: norm_in(layer + 1, s))
            return carry1

        lax.fori_loop(0, 2, finish, 0)
        return carry

    hb[...] = x_ref[...].astype(F32)
    for s in range(2):
        norm_in(0, s)
    first_gather = Gather(mixed.at[0], 0, 0)
    last_gather = Gather(gff, 2, LAYERS - 1)
    for s in range(2):
        for r in range(4):
            g_in = cot_ref[64 * s + 16 * r : 64 * s + 16 * r + 16, :].astype(F32)
            gff[own_rows(s, 16 * r), :] = (mrow(LAYERS - 1, 5) * g_in).astype(BF16)
        last_gather.begin(s)
    first_gather.alone()
    relay(0)
    w0(0, 1)
    w0(0, 2)
    last_gather.alone()
    first_gather.drain()
    last_gather.drain()
    lax.fori_loop(0, LAYERS, forward, 0)

    for dev in (dev_p, dev_y, dev_x):
        pl.semaphore_signal(r_c, inc=1, device_id=dev, device_id_type=MESH)
    out_ref[...] = hb[...].astype(BF16)
    for layer in range(LAYERS):
        for m in range(3):
            w_drain(layer, m)
    hb[...] = cot_ref[...].astype(F32)

    def clear(d):
        rz[:, d] = jnp.zeros((6, 288, 640), BF16)

    when(z == 0, lambda: clear(0))
    when(z == 3, lambda: clear(2))

    def g_rows(zz, h):
        return rows_at(288 * zz + 144 * h, 144)

    def g_copy(i, d, zz, h):
        got = rz.at[i, d, pl.ds(144 * h, 144)]
        return rc(
            w.at[i, g_rows(zz, h)], got, gz_s.at[i, d, h], gz_r.at[i, d, h], (zz, c, t)
        )

    def g_relay(i, h):
        got = rzr.at[pl.ds(144 * h, 144)]
        return rc(
            w.at[i, g_rows(3 - z, h)], got, gz_s.at[i, 3, h], gz_r.at[i, 3, h], (1 + z // 2, c, t)
        )

    is_end = jnp.logical_not(is_mid)

    def g_each(i, h, act_on):
        when(z == 0, lambda: act_on(g_copy(i, 0, 1, h)))
        when(z == 3, lambda: act_on(g_copy(i, 2, 2, h)))
        when(is_end, lambda: act_on(g_copy(i, 1, z_far, h)))

    def g_start(copy):
        copy.start()

    def g0(i):
        for h in range(2):
            g_each(i, h, g_start)

            def from_mid(h=h):
                g_copy(i, 0, z + 1, h).start()
                g_copy(i, 2, z - 1, h).start()

            when(is_mid, from_mid)

    def g0_relay(i, credit):
        when(is_end & jnp.logical_and(credit, True), lambda: pl.semaphore_wait(g_c, 1))
        for h in range(2):
            when(is_end, lambda h=h: g_relay(i, h).start())

    def g1(i):
        def at_mid():
            for h in range(2):
                g_relay(i, h).wait_recv()

                def add(row, h=h):
                    rr = rows_at(288 * z_far + 144 * h + row, 16)
                    w[i, rr, :] = (
                        w[i, rr, :].astype(F32) + rzr[rows_at(144 * h + row, 16), :].astype(F32)
                    ).astype(BF16)

                add_rows(144, add)
                g_copy(i, 1, z_far, h).start()
            pl.semaphore_signal(g_c, inc=1, device_id=(z_end, c, t), device_id_type=MESH)

        when(is_mid, at_mid)

    def g_send(i, h):
        there = gw_ref.at[i, c, pl.ds(144 * h, 144)]
        return rc(w.at[i, g_rows(z, h)], there, gf_s.at[i, h], gf_r.at[i, h], dev_x)

    def g_keep(i, h):
        there = gw_ref.at[i, c, pl.ds(144 * h, 144)]
        return pltpu.make_async_copy(w.at[i, g_rows(z, h)], there, g_l.at[i, h])

    def g2(i):
        for h in range(2):

            def got(d, h=h):
                part = rz.at[i, d, pl.ds(144 * h, 144)]
                return rc(part, part, gz_s.at[i, d, h], gz_r.at[i, d, h], dev_x)

            when(z != 0, lambda: got(0).wait_recv())
            when(z != 3, lambda: got(2).wait_recv())
            got(1).wait_recv()

            def add(row, h=h):
                rr = rows_at(288 * z + 144 * h + row, 16)
                total = w[i, rr, :].astype(F32)
                for d in range(3):
                    total = total + rz[i, d, rows_at(144 * h + row, 16), :].astype(F32)
                w[i, rr, :] = total.astype(BF16)

            add_rows(144, add)
            g_send(i, h).start()
            g_keep(i, h).start()

    def g3(i):
        def done(copy):
            copy.wait_send()

        for h in range(2):
            other = gw_ref.at[i, 1 - c, pl.ds(144 * h, 144)]
            rc(other, other, gf_s.at[i, h], gf_r.at[i, h], dev_x).wait_recv()
            g_send(i, h).wait_send()
            g_keep(i, h).wait()

            def from_mid(h=h):
                for d, zz in ((0, z + 1), (1, z_far), (2, z - 1)):
                    g_copy(i, d, zz, h).wait_send()

            when(is_mid, from_mid)
            when(is_end, lambda h=h: g_relay(i, h).wait_send())
            g_each(i, h, done)

    def small():
        for index, size, dev in ((0, 8, dev_p), (1, 8, dev_y), (2, 16, dev_x)):
            step = rc(
                sm.at[:, 0:size],
                smr.at[index, :, 0:size],
                sm_s.at[index],
                sm_r.at[index],
                dev,
            )
            step.start()
            step.wait_send()
            step.wait_recv()
            sm[:, 0:size, :] = sm[:, 0:size, :] + smr[index, :, 0:size, :]
        small_ref[z] = sm[...]
        for d, zz in enumerate(zo):
            rc(sm, small_ref.at[z], sm_s.at[3 + d], sm_r.at[3 + z], (zz, c, t)).start()

    def small_end():
        for d, zz in enumerate(zo):
            end = rc(sm, small_ref.at[zz], sm_s.at[3 + d], sm_r.at[3 + zz], (zz, c, t))
            end.wait_recv()
            end.wait_send()

    zero8 = jnp.zeros((8, D), F32)

    def add_sum(layer, row, v8):
        here = (layer, pl.ds(row, 1), slice(0, v8.shape[1]))
        sm[here] = sm[here] + jnp.sum(v8, axis=0, keepdims=True)

    def grad_in_ff(layer, s, live):
        def start(r, sums):
            rr = rows_at(64 * s + 16 * r, 16)
            g = hb[rr, :]
            gf = (mrow(layer, 5) * g).astype(BF16)
            gff[own_rows(s, 16 * r), :] = gf
            return (sums[0] + fold(g * own[layer, 3, rr, :]), sums[1] + fold(gf.astype(F32)))

        s_gate2, s_bdown = lax.fori_loop(0, 4, start, (zero8, zero8))
        add_sum(layer, 5, s_gate2)
        add_sum(layer, 7, s_bdown)
        if live:
            Gather(gff, 2, layer).begin(s)

    def backward(step_index, carry):
        layer = LAYERS - 1 - step_index
        ia, iu, id_ = 3 * layer, 3 * layer + 1, 3 * layer + 2
        more = layer > 0

        def act_back(s, start):
            rr = piece(start)
            temp = rows_at(512 * s, 128)
            pool[temp, 0:640] = nn(gff[rr, :], w[id_])

            def one(r, total):
                r2 = rows_at(start + 16 * r, 16)
                v = pre[layer, r2, :]
                th = jnp.tanh(0.7978845608028654 * (v + 0.044715 * (v * v * v)))
                act[r2, :] = (0.5 * v * (1.0 + th)).astype(BF16)
                slope = 0.5 * (1.0 + th) + 0.5 * v * (1.0 - th * th) * (
                    0.7978845608028654 * (1.0 + 0.134145 * (v * v))
                )
                gp = (pool[rows_at(512 * s + 16 * r, 16), 0:640] * slope).astype(BF16)
                gpre[r2, :] = gp
                return total + fold(gp.astype(F32))

            add_sum(layer, 10 + c, lax.fori_loop(0, 8, one, jnp.zeros((8, 640), F32)))

        Gather(gff, 2, layer).run(act_back, layer < LAYERS - 1)
        when(layer == 0, lambda: g1(3))
        when(layer == LAYERS - 1, lambda: pl.semaphore_wait(r_c, 3))
        sum1 = Reduce(2, layer, lambda start: nt(gpre[piece(start), :], w[iu]))
        sum1.run()

        def one_d(i, inner):
            w[id_, rows_at(128 * i, 128), :] = tn(gff[:, cols128(i)], act[...]).astype(BF16)
            return inner

        lax.fori_loop(0, 9, one_d, 0)
        g0_relay(id_, layer < LAYERS - 1)
        g0(id_)
        gather2 = Gather(gb, 3, layer)

        def middle(s, carry1):
            sum1.finish(s)

            def mid(r, sums):
                rr = rows_at(64 * s + 16 * r, 16)
                gf = sum1.total(s, 16 * r)
                n = own[layer, 1, rr, :]
                e = gf * (1.0 + mrow(layer, 4))
                iv = inv[layer, 1, rr, 0:1]
                ga = hb[rr, :] + iv * (
                    e
                    - jnp.mean(e, axis=-1, keepdims=True)
                    - n * jnp.mean(e * n, axis=-1, keepdims=True)
                )
                hb[rr, :] = ga
                gbv = (mrow(layer, 2) * ga).astype(BF16)
                gb[own_rows(s, 16 * r), :] = gbv
                return (
                    sums[0] + fold(gf),
                    sums[1] + fold(gf * n),
                    sums[2] + fold(ga * own[layer, 2, rr, :]),
                    sums[3] + fold(gbv.astype(F32)),
                )

            all_sums = lax.fori_loop(0, 4, mid, (zero8, zero8, zero8, zero8))
            for row, value in zip((3, 4, 2, 6), all_sums):
                add_sum(layer, row, value)
            gather2.begin(s)
            return carry1

        lax.fori_loop(0, 2, middle, 0)

        def one_u(i, inner):
            w[iu, rows_at(128 * i, 128), :] = tn(ffall[layer, :, cols128(i)], gpre[...]).astype(
                BF16
            )
            return inner

        lax.fori_loop(0, 9, one_u, 0)
        g1(id_)
        g0(iu)

        def att_back(s, start):
            rr = piece(start)
            doa[rr, :] = pltpu.roll(nn(gb[rr, :], w[ia, :, 384:640]), 224, 1).astype(BF16)

        gather2.run(att_back)
        g0_relay(iu, True)

        def pending():
            g2(5)
            g2(4)

        when(layer == 0, pending)
        dkv[...] = jnp.zeros_like(dkv)
        ot[...] = jnp.zeros_like(ot)

        def head(j, inner):
            h = lax.rem(j, 2)
            qh = j // 2
            q_rows = rows_at(512 * qh, 512)
            q_cols = pl.ds(pl.multiple_of(512 * qh, 512), 512)
            qm = jnp.where(head_mask(72 * h), qa[layer, q_rows, :].astype(F32), 0.0)
            dm = jnp.where(head_mask(16 + 72 * h), doa[q_rows, :].astype(F32), 0.0)
            pb[0:512, 0:256] = qm.astype(BF16)
            pb[0:512, 256:512] = dm.astype(BF16)
            log_row = lse[layer, j, 0:1, :]

            def first(kb, d8):
                rr = rows_at(256 * kb, 256)
                v = nt(qkv[layer, rr, 0:256], pb[0:512, 0:256]) * scale
                pr = jnp.exp(v - log_row)
                dp = nt(qkv[layer, rr, 128:384], pb[0:512, 256:512])
                pre[layer, rr, 0:512] = pr
                pool[rr, 0:512] = dp
                dkv[rr, 128:384] = dkv[rr, 128:384] + nn(pr.astype(BF16), pb[0:512, 256:512])
                return d8 + fold(pr * dp)

            d8 = lax.fori_loop(0, 4, first, jnp.zeros((8, 512), F32))
            delta = jnp.sum(d8, axis=0, keepdims=True)

            def second(kb, inner2):
                rr = rows_at(256 * kb, 256)
                ds = (pre[layer, rr, 0:512] * (pool[rr, 0:512] - delta)).astype(BF16)
                pb[rows_at(512 + 256 * kb, 256), :] = ds
                dkv[rr, 0:256] = dkv[rr, 0:256] + nn(ds, pb[0:512, 0:256]) * scale
                return inner2

            lax.fori_loop(0, 4, second, 0)
            otw[...] = tn(qkv[layer, :, 0:256], pb[512:1536, :]) * scale
            ot[pl.ds(pl.multiple_of(32 + 72 * h, 8), 72), q_cols] = otw[
                pl.ds(pl.multiple_of(72 * h, 8), 72), :
            ]
            return inner

        lax.fori_loop(0, 4, head, 0)

        def put(b, total):
            rr = pool_rows(b)
            dq = ot[:, cols128(b)].T
            kv = dkv[rr, :]
            both = jnp.concatenate(
                (kv[:, 0:256], kv[:, 256:384] + dq[:, 0:128], dq[:, 128:256]), axis=1
            ).astype(BF16)
            dqkv[rr, :] = both
            return total + fold(both.astype(F32))

        add_sum(layer, 8 + c, lax.fori_loop(0, 8, put, jnp.zeros((8, 512), F32)))

        g1(iu)
        sum2 = Reduce(3, layer, lambda start: nt(dqkv[piece(start), :], w[ia, :, 0:512]))
        sum2.run()

        def one_a(i, inner):
            rr = rows_at(128 * i, 128)
            r1 = tn(mixed[layer, :, cols128(i)], dqkv[...])
            r3 = tn(gb[:, cols128(i)], att[layer])
            w[ia, rr, 0:384] = r1[:, 0:384].astype(BF16)
            w[ia, rr, 384:512] = (r1[:, 384:512] + r3[:, 0:128]).astype(BF16)
            w[ia, rr, 512:640] = r3[:, 128:256].astype(BF16)
            return inner

        lax.fori_loop(0, 9, one_a, 0)
        g0_relay(ia, True)
        g0(ia)
        when(layer == 0, lambda: g2(3))

        def final(s, carry1):
            sum2.finish(s)

            def last(r, sums):
                rr = rows_at(64 * s + 16 * r, 16)
                gm = sum2.total(s, 16 * r)
                n = own[layer, 0, rr, :]
                e = gm * (1.0 + mrow(layer, 1))
                iv = inv[layer, 0, rr, 0:1]
                hb[rr, :] = hb[rr, :] + iv * (
                    e
                    - jnp.mean(e, axis=-1, keepdims=True)
                    - n * jnp.mean(e * n, axis=-1, keepdims=True)
                )
                return (sums[0] + fold(gm), sums[1] + fold(gm * n))

            all_sums = lax.fori_loop(0, 4, last, (zero8, zero8))
            for row, value in zip((0, 1), all_sums):
                add_sum(layer, row, value)
            when(more, lambda: grad_in_ff(layer - 1, s, True))
            return carry1

        lax.fori_loop(0, 2, final, 0)
        return carry

    sm[...] = jnp.zeros_like(sm)
    for s in range(2):
        grad_in_ff(LAYERS - 1, s, False)
    lax.fori_loop(0, LAYERS, backward, 0)
    g1(0)
    when(jnp.logical_not(is_mid), lambda: pl.semaphore_wait(g_c, 1))
    small()
    g2(2)
    g2(1)
    small_end()
    g2(0)
    for i in range(6):
        g3(i)


def sum_kernel(zs_n, part_ref, out_ref, got, send_sem, recv_sem):
    z = lax.axis_index("shard")
    c = lax.axis_index("context")
    t = lax.axis_index("tensor")
    others = [lax.rem(z + d, zs_n) for d in range(1, zs_n)]
    barrier = pltpu.get_barrier_semaphore()
    for zz in others:
        pl.semaphore_signal(barrier, inc=1, device_id=(zz, c, t), device_id_type=MESH)
    pl.semaphore_wait(barrier, zs_n - 1)

    def copy(d, slot, zz):
        return pltpu.make_async_remote_copy(
            src_ref=part_ref,
            dst_ref=got.at[slot],
            send_sem=send_sem.at[d],
            recv_sem=recv_sem.at[slot],
            device_id=(zz, c, t),
            device_id_type=MESH,
        )

    for d, zz in enumerate(others):
        copy(d, z, zz).start()
    got[z] = part_ref[...]
    for d, zz in enumerate(others):
        copy(d, zz, zz).wait_recv()
        copy(d, z, zz).wait_send()
    total = got[0]
    for zz in range(1, zs_n):
        total = total + got[zz]
    out_ref[...] = total


def sum_shards(zs_n, part):
    vm = pl.BlockSpec(memory_space=pltpu.VMEM)
    dma = pltpu.SemaphoreType.DMA
    return pl.pallas_call(
        functools.partial(sum_kernel, zs_n),
        name="sum_shards",
        out_shape=jax.ShapeDtypeStruct(part.shape, F32),
        in_specs=[vm],
        out_specs=vm,
        scratch_shapes=[
            pltpu.VMEM((zs_n,) + part.shape, F32),
            dma((zs_n - 1,)),
            dma((zs_n,)),
        ],
        compiler_params=pltpu.CompilerParams(collective_id=1, has_side_effects=True),
    )(part)


def run_stage(zs_n, *args):
    vm = pl.BlockSpec(memory_space=pltpu.VMEM)
    anyspace = pl.BlockSpec(memory_space=pl.ANY)
    dma = pltpu.SemaphoreType.DMA
    sds = jax.ShapeDtypeStruct
    scratch = [
        pltpu.VMEM((6, D, 640), BF16),
        pltpu.VMEM((2, 1024, D), BF16),
        pltpu.VMEM((2, 1024, 512), BF16),
        pltpu.VMEM((2, 1024, 256), BF16),
        pltpu.VMEM((2, 1024, 256), BF16),
        pltpu.VMEM((2, 1024, D), BF16),
        pltpu.VMEM((2, 1024, 640), F32),
        pltpu.VMEM((1024, 640), BF16),
        pltpu.VMEM((2, 4, 128, D), F32),
        pltpu.VMEM((2, 2, 128, 128), F32),
        pltpu.VMEM((2, 4, 8, 512), F32),
        pltpu.VMEM((2, 4, D), F32),
        pltpu.VMEM((zs_n, 16, 384), F32),
        pltpu.VMEM((zs_n, 16, 384), F32),
        pltpu.VMEM((2, 8, D), F32),
        pltpu.VMEM((128, D), F32),
        pltpu.VMEM((1024, D), F32),
        pltpu.VMEM((2, 4, 64, D), F32),
        pltpu.VMEM((2, 64, D), BF16),
        pltpu.VMEM((2, 64, D), BF16),
        pltpu.VMEM((2, 64, D), BF16),
        pltpu.VMEM((2, 64, D), BF16),
        pltpu.VMEM((2, 64, D), BF16),
        pltpu.VMEM((2, 64, D), BF16),
        pltpu.VMEM((1024, D), BF16),
        pltpu.VMEM((1024, 640), BF16),
        pltpu.VMEM((1024, D), BF16),
        pltpu.VMEM((1024, 256), BF16),
        pltpu.VMEM((1024, 512), BF16),
        pltpu.VMEM((1024, 384), F32),
        pltpu.VMEM((1536, 512), BF16),
        pltpu.VMEM((256, 512), F32),
        pltpu.VMEM((256, 1024), F32),
        pltpu.VMEM((6, zs_n - 1, 288, 640), BF16),
        pltpu.VMEM((288, 640), BF16),
        pltpu.VMEM((2, 16, D), F32),
        pltpu.VMEM((3, 2, 16, D), F32),
        dma((zs_n - 1,)),
        dma((zs_n,)),
        dma((6, 4)),
        dma((6, zs_n)),
        dma((6,)),
        dma((4, 2, 2, 9)),
        dma((4, 2, 2, 9)),
        dma((4, 2, 2, 10)),
        dma((4, 2, 2, 10)),
        dma((6, zs_n, 2)),
        dma((6, zs_n, 2)),
        dma((6, 2)),
        dma((6, 2)),
        dma((6, 2)),
        pltpu.SemaphoreType.REGULAR,
        pltpu.SemaphoreType.REGULAR,
        dma((3 + zs_n,)),
        dma((3 + zs_n,)),
    ]
    return pl.pallas_call(
        functools.partial(stage_kernel, zs_n),
        name="two_blocks",
        out_shape=(
            sds((128, D), BF16),
            sds((128, D), F32),
            sds((6, 2, 288, 640), BF16),
            sds((zs_n, 2, 16, D), F32),
        ),
        in_specs=[vm] * 8 + [anyspace] * 3,
        out_specs=(vm, vm, anyspace, vm),
        scratch_shapes=scratch,
        compiler_params=pltpu.CompilerParams(
            collective_id=0, has_side_effects=True, vmem_limit_bytes=67043328
        ),
    )(*args)


def fast_body(
    zs_n,
    x_in,
    cond,
    w_ada,
    b_ada,
    w_qkv,
    b_qv,
    w_proj,
    b_proj,
    up_weight,
    up_bias_vector,
    down_weight,
    down_bias_vector,
    cotangent,
):
    z = lax.axis_index("shard")
    c = lax.axis_index("context")
    cols = w_ada.shape[3]
    part = w_qkv.shape[3] // 2
    units = up_weight.shape[2] // 2
    cond_low = jax.nn.silu(cond).astype(BF16)
    modin = jnp.einsum("sd,ldkc->lksc", cond_low, w_ada, preferred_element_type=F32)

    def mine(array, size, axis):
        low = lax.slice_in_dim(array, 0, size, axis=axis)
        high = lax.slice_in_dim(array, size, 2 * size, axis=axis)
        return jnp.where(c == 0, low, high)

    def wide(array, size):
        return jnp.pad(array, ((0, 0),) * (array.ndim - 1) + ((0, size - array.shape[-1]),))

    heads = mine(w_qkv, part, 3)
    block_a = wide(
        jnp.concatenate(
            (
                heads[:, 1],
                heads[:, 2],
                heads[:, 0],
                mine(w_proj, part, 1).transpose(0, 2, 1),
            ),
            axis=2,
        ),
        640,
    )
    block_u = wide(mine(up_weight, units, 2), 640)
    block_d = wide(mine(down_weight, units, 1).transpose(0, 2, 1), 640)
    out, grad_in, gw, small = run_stage(
        zs_n,
        x_in[:, 0],
        cotangent[:, 0],
        modin,
        b_ada,
        b_qv,
        b_proj,
        up_bias_vector,
        down_bias_vector,
        block_a,
        block_u,
        block_d,
    )
    grad_mod = small[:, :, 0:6, :].astype(BF16)
    mod_cols = lax.dynamic_slice_in_dim(grad_mod, z * cols, cols, 3)
    grad_w_ada = jnp.einsum("sd,slkc->ldkc", cond_low, mod_cols, preferred_element_type=F32)
    grad_b_ada = jnp.sum(mod_cols.astype(F32), axis=0)
    cond_part = jnp.einsum("slkc,ldkc->sd", mod_cols, w_ada, preferred_element_type=F32)
    cond_total = sum_shards(zs_n, cond_part)
    silu_value, silu_back = jax.vjp(jax.nn.silu, cond)
    grad_cond = silu_back(cond_total)[0]
    sums = jnp.sum(small[:, :, 6:12, :], axis=0)

    def halves(row, start, size):
        return jnp.concatenate(
            (sums[:, row, start : start + size], sums[:, row + 1, start : start + size]), axis=1
        )

    gw = gw.reshape(LAYERS, 3, 2, cols, 640)

    def both(m, start, size):
        return jnp.concatenate(
            (gw[:, m, 0, :, start : start + size], gw[:, m, 1, :, start : start + size]), axis=2
        ).astype(F32)

    return (
        out[:, None],
        grad_in[:, None],
        grad_cond,
        grad_w_ada,
        grad_b_ada,
        jnp.stack((both(0, 2 * part, part), both(0, 0, part), both(0, part, part)), axis=1),
        jnp.stack((halves(2, 2 * part, part), halves(2, part, part)), axis=1),
        both(0, 3 * part, part).transpose(0, 2, 1),
        sums[:, 0],
        both(1, 0, units),
        halves(4, 0, units),
        both(2, 0, units).transpose(0, 2, 1),
        sums[:, 1],
    )


def solution(mesh):
    shape = mesh.shape
    program = body
    if shape["context"] == 2 and shape["tensor"] == 4 and shape["shard"] == 4:
        program = functools.partial(fast_body, shape["shard"])
    return jax.shard_map(
        program,
        mesh=mesh,
        in_specs=(
            P(("context", "tensor"), "shard", None),
            P(),
            P(None, None, None, "shard"),
            P(None, None, "shard"),
            P(None, None, "shard", "tensor"),
            P(None, None, "tensor"),
            P(None, "tensor", "shard"),
            P(),
            P(None, "shard", "tensor"),
            P(None, "tensor"),
            P(None, "tensor", "shard"),
            P(),
            P(("context", "tensor"), "shard", None),
        ),
        out_specs=(
            P(("context", "tensor"), "shard", None),
            P(("context", "tensor"), "shard", None),
            P(),
            P(None, None, None, "shard"),
            P(None, None, "shard"),
            P(None, None, "shard", "tensor"),
            P(None, None, "tensor"),
            P(None, "tensor", "shard"),
            P(),
            P(None, "shard", "tensor"),
            P(None, "tensor"),
            P(None, "tensor", "shard"),
            P(),
        ),
        check_vma=False,
    )
```
